128 devices in a mesh: lang: 16 (over y_lo, z, core), shard: 8 (over y_hi, x).
Axes of the slice: x: 4, y: 4 (y_hi: 2, y_lo: 2; y = y_hi * 2 + y_lo), z: 4, core: 2. Of those that a mesh axis runs over, the one named last changes fastest.
Arguments:
- queries: bfloat16 [16384, 768], P(('lang', 'shard')), may hold values from -6 to 6
- routes: int32 [16384, 1], P(('lang', 'shard')), may hold values from 0 to 15; in each aligned block of 128 rows (0 to 127, 128 to 255, ...) at most 20 rows name the same one
- corpus: bfloat16 [131072, 768], P(('lang', 'shard')), may hold values from -0.21875 to 0.21875
Outputs:
- top_scores: float32 [16384, 128], P(('lang', 'shard'))
The draws below stay inside these ranges and needn't reach their ends.
Inputs may be any that keep to these rules, and one draw needn't show every extreme that they name: `routes`: among the 128 queries of one device, each language is named at most 20 times; some language is named exactly 20 times.
All inputs are finite; a program needn't handle non-finite values.
Results may differ from the reference program's by a relative error of at most 0.0012.
Values may be sent and summed in bfloat16 or wider, within the bound.
No kernel may reach another device: no remote copies, remote signals or barrier semaphores. Data moves between devices by JAX's collectives and lax.ppermute only.
A program may use at most 64 MiB of HBM per device.

```python
import math
import jax
import jax.numpy as jnp
import numpy as np
from jax import lax

D = 768
Q_DEV = 128
PASS_DEV = 1024
CAP = 20
TOPK = 128
QUERIES = 16384
PASSAGES = 131072
N_LANG = 16
N_SHARD = 8


def block_levels(rng, extent, cuts, least, largest):
    def one(dim, shards_of):
        steps = jax.random.uniform(jax.random.fold_in(jax.random.fold_in(rng, 6), dim), (shards_of,), jnp.float32, least / len(cuts), largest / len(cuts))
        return jnp.repeat(jnp.exp(steps), extent[dim] // shards_of).reshape((-1,) + (1,) * (len(extent) - dim - 1))

    gain = one(*cuts[0])
    for cut in cuts[1:]:
        gain = gain * one(*cut)
    return gain


def deal_out(own_key, own, number, rows, count, top, most, slope):
    order = jax.random.permutation(own_key, count)
    heavy_load, ordinary = portions_of(count, rows * top, most, slope, True), portions_of(count, rows * top, most, slope, False)
    places = jnp.arange(count)

    def named(tallies, turn):
        used = int((tallies > 0).sum())
        fixed = max(1, used // 4)
        shifted = fixed + (places - fixed + turn * (used - fixed)) % max(1, count - fixed)
        return jnp.zeros((count,), jnp.int32).at[order[jnp.where(places < fixed, places, shifted)]].set(jnp.asarray(tallies, jnp.int32))

    tallies = jnp.where(number % 4 == 0, named(heavy_load, number // 4), named(ordinary, number - number // 4 - 1))
    mixed = jax.random.permutation(jax.random.fold_in(own, 3), count)
    giver, sink = mixed[0:count // 2 * 2:2], mixed[1:count // 2 * 2:2]
    margin = jnp.minimum(tallies[giver] - 1, most - tallies[sink]) // 2
    margin = jnp.where((giver == order[0]) | (sink == order[0]) | (tallies[sink] == 0), 0, jnp.maximum(margin, 0))
    shifted = jax.random.randint(jax.random.fold_in(own, 4), (count // 2,), 0, 1 << 20) % (margin + 1)
    tallies = tallies.at[giver].add(-shifted).at[sink].add(shifted)
    items = jnp.searchsorted(jnp.cumsum(tallies), jnp.arange(rows * top), side="right").astype(jnp.int32)
    grid = items.reshape(top, rows).T
    grid = grid[jax.random.permutation(jax.random.fold_in(own, 1), rows)]
    turn = jax.random.randint(jax.random.fold_in(own, 2), (rows, 1), 0, top)
    return jnp.take_along_axis(grid, (jnp.arange(top)[None, :] + turn) % top, axis=1)


def portions_of(number_of, total, bound, lean, full):
    weights = [(1 << 20) // math.isqrt(standing ** lean) + 1 for standing in range(1, number_of + 1)]
    largest = bound if full else min(bound, max(-(-total // number_of), total * weights[0] // sum(weights)))
    least = 1 if total - largest >= number_of - 1 else 0
    holding, surplus = [largest] + [least] * (number_of - 1), total - largest - least * (number_of - 1)
    while surplus > 0:
        movable = [i for i in range(1, number_of) if holding[i] < largest] or [i for i in range(1, number_of) if holding[i] < bound]
        mass, left = sum([weights[i] for i in movable]), surplus
        for i in movable:
            extra = min(bound - holding[i], max(1, left * weights[i] // mass), surplus)
            holding[i] = holding[i] + extra
            surplus = surplus - extra
    return np.array(holding)


def gaussian(rng, shape, deviation, reach, shards=(), held_as=jnp.bfloat16):
    drawn = deviation * jax.random.normal(rng, shape, jnp.float32)
    if shards:
        drawn = drawn * block_levels(rng, shape, shards, -0.22, 0.18)
    return jnp.clip(drawn, -reach, reach).astype(held_as)


def setup_inputs(seed: int = 0) -> dict:
    arg_keys = jax.random.split(jax.random.key(seed), 4)
    queries = gaussian(arg_keys[0], (QUERIES, D), 1.0, 6.0, ((0, 128),))
    routes_keys = jax.random.split(jax.random.fold_in(arg_keys[1], 1), QUERIES // Q_DEV)
    routes_turns = jax.random.permutation(jax.random.fold_in(arg_keys[1], 3), QUERIES // Q_DEV)
    routes = jax.vmap(lambda own, number: deal_out(jax.random.fold_in(arg_keys[1], 2), own, number, Q_DEV, N_LANG, 1, CAP, 2))(routes_keys, routes_turns).reshape((QUERIES, 1))
    corpus = gaussian(arg_keys[2], (PASSAGES, D), D ** -0.5, 0.21875, ((0, 128),))
    return dict(queries=queries, routes=routes, corpus=corpus)


epsilon = 1e-06

def reference(queries, routes, corpus):
    widened = queries.astype(jnp.float32)
    unit_query = (widened * lax.rsqrt(lax.optimization_barrier(jnp.mean(widened * widened, axis=1, keepdims=True)) + epsilon)).astype(jnp.bfloat16)
    devices_count = N_LANG * N_SHARD
    language = routes[:, 0].reshape(devices_count, Q_DEV).astype(jnp.int32)
    onehot = (language[:, :, None] == jnp.arange(N_LANG, dtype=jnp.int32)[None, None, :]).astype(jnp.int32)
    slot_index = (lax.optimization_barrier(jnp.sum(jnp.cumsum(onehot, axis=1) * onehot, axis=2)) - 1).astype(jnp.int32)
    device_index = jnp.broadcast_to(jnp.arange(devices_count, dtype=jnp.int32)[:, None], (devices_count, Q_DEV))
    padded = jnp.zeros((devices_count, N_LANG, CAP, D), jnp.bfloat16)
    padded = padded.at[device_index, language, slot_index].set(unit_query.reshape(devices_count, Q_DEV, D))
    blocks = jnp.transpose(padded, (1, 0, 2, 3)).reshape(N_LANG, devices_count * CAP, D)
    lang_corpus = corpus.reshape(N_LANG, N_SHARD * PASS_DEV, D)

    def score_language(inputs):
        block_rows, passages = inputs
        scores = jnp.dot(block_rows.astype(jnp.float32), passages.astype(jnp.float32).T, precision=lax.Precision.HIGHEST)
        return lax.top_k(scores, TOPK)[0]
    results = lax.map(score_language, (blocks, lang_corpus))
    results = results.reshape(N_LANG, devices_count, CAP, TOPK)
    picked = results[language, device_index, slot_index]
    return picked.reshape(devices_count * Q_DEV, TOPK)
```

```python
import functools

import jax
import jax.numpy as jnp
from jax import lax
from jax.experimental import pallas as pl
from jax.experimental.pallas import tpu as pltpu
from jax.sharding import PartitionSpec as P

CAP = 20
TOPK = 128
SLOTS = 320
MAIN = 256
TAIL = SLOTS - MAIN

epsilon = 1e-06


def batcher(n):
    pairs = []
    p = 1
    while p < n:
        k = p
        while k >= 1:
            for j in range(k % p, n - k, 2 * k):
                for i in range(min(k, n - j - k)):
                    if (i + j) // (2 * p) == (i + j + k) // (2 * p):
                        pairs.append((i + j, i + j + k))
            k //= 2
        p *= 2
    return pairs


SORT32 = batcher(32)


def wire(ref, base, i):
    return ref[pl.ds(pl.multiple_of((base + i) * 8, 8), 8), :]


def put(ref, base, i, value):
    ref[pl.ds(pl.multiple_of((base + i) * 8, 8), 8), :] = value


def sort32(ref, base):
    v = [wire(ref, base, i) for i in range(32)]
    for i, j in SORT32:
        v[i], v[j] = jnp.maximum(v[i], v[j]), jnp.minimum(v[i], v[j])
    for i in range(32):
        put(ref, base, i, v[i])


def clean(v):
    n = len(v)
    step = n // 2
    while step:
        for i in range(n):
            if not i & step:
                v[i], v[i + step] = jnp.maximum(v[i], v[i + step]), jnp.minimum(v[i], v[i + step])
        step //= 2
    return v


def clean_at(ref, base):
    v = clean([wire(ref, base, i) for i in range(32)])
    for i in range(32):
        put(ref, base, i, v[i])


def merge64(src, base, dst):
    for op, at in ((jnp.maximum, 0), (jnp.minimum, 32)):
        v = clean([op(wire(src, base, i), wire(src, base, 63 - i)) for i in range(32)])
        for i in range(32):
            put(dst, base + at, i, v[i])


def merge128(src, base, dst):
    for op, at in ((jnp.maximum, 0), (jnp.minimum, 64)):
        v = []
        for i in range(32):
            a = op(wire(src, base, i), wire(src, base, 127 - i))
            b = op(wire(src, base, i + 32), wire(src, base, 95 - i))
            v.append(jnp.maximum(a, b))
            put(dst, base + at + 32, i, jnp.minimum(a, b))
        v = clean(v)
        for i in range(32):
            put(dst, base + at, i, v[i])
        clean_at(dst, base + at + 32)


def merge_top(a, a_base, b, b_base, dst, dst_base, turn=0):
    def other(i):
        value = wire(b, b_base, 127 - i)
        return pltpu.roll(value, turn, 0) if turn else value

    v = []
    for i in range(32):
        c = [jnp.maximum(wire(a, a_base, i + 32 * k), other(i + 32 * k)) for k in range(4)]
        f0, g0 = jnp.maximum(c[0], c[2]), jnp.minimum(c[0], c[2])
        f1, g1 = jnp.maximum(c[1], c[3]), jnp.minimum(c[1], c[3])
        v.append(jnp.maximum(f0, f1))
        put(dst, dst_base + 32, i, jnp.minimum(f0, f1))
        put(dst, dst_base + 64, i, jnp.maximum(g0, g1))
        put(dst, dst_base + 96, i, jnp.minimum(g0, g1))
    v = clean(v)
    for i in range(32):
        put(dst, dst_base, i, v[i])

    def rest(k, carry):
        clean_at(dst, dst_base + 32 + 32 * k)
        return carry

    lax.fori_loop(0, 3, rest, 0)


def loop(n, body):
    def step(i, carry):
        body(i)
        return carry

    lax.fori_loop(0, n, step, 0)


def leaders_kernel(q0, q1, q2, q3, own, far, main_ref, tail_ref, q_all, s, u, w):
    for k, q in enumerate((q0, q1, q2, q3)):
        q_all[k * MAIN : (k + 1) * MAIN, :] = q[0:MAIN, :]
        q_all[4 * MAIN + k * TAIL : 4 * MAIN + (k + 1) * TAIL, :] = q[MAIN:SLOTS, :]

    def scored(corpus, g, dst):
        rows = q_all[pl.ds(pl.multiple_of(g * MAIN, MAIN), MAIN), :]
        for quarter in range(4):
            part = lax.dot_general(
                corpus[quarter * 256 : (quarter + 1) * 256, :],
                rows,
                (((1,), (1,)), ((), ())),
                preferred_element_type=jnp.float32,
            )
            for half in range(2):
                s[pl.ds(quarter * 2 + half, 256, stride=8), :] = part[:, half * 128 : (half + 1) * 128]
        loop(8, lambda i: sort32(s, i * 32))
        loop(4, lambda i: merge64(s, i * 64, u))
        loop(2, lambda i: merge128(u, i * 128, s))
        merge_top(s, 0, s, 128, dst, 0)

    def group(g):
        scored(own, g, w)
        scored(far, g, u)
        merge_top(w, 0, u, 0, s, 0)
        merge_top(s, 0, s, 0, u, 0, turn=4)
        merge_top(u, 0, u, 0, s, 0, turn=2)

        @pl.when(g < 4)
        def _():
            for half in range(2):
                main_ref[g, half] = s[pl.ds(half, 128, stride=8), :]

        @pl.when(g == 4)
        def _():
            for half in range(2):
                tail_ref[half] = s[pl.ds(half, 128, stride=8), :]

    loop(5, group)


def leaders(chunks, own, far):
    return pl.pallas_call(
        leaders_kernel,
        out_shape=(
            jax.ShapeDtypeStruct((4, 2, TOPK, 128), jnp.float32),
            jax.ShapeDtypeStruct((2, TOPK, 128), jnp.float32),
        ),
        in_specs=[pl.BlockSpec(memory_space=pltpu.VMEM)] * 6,
        out_specs=[pl.BlockSpec(memory_space=pltpu.VMEM)] * 2,
        scratch_shapes=[
            pltpu.VMEM((4 * SLOTS, 768), jnp.bfloat16),
            pltpu.VMEM((256 * 8, 128), jnp.float32),
            pltpu.VMEM((256 * 8, 128), jnp.float32),
            pltpu.VMEM((128 * 8, 128), jnp.float32),
        ],
        compiler_params=pltpu.CompilerParams(vmem_limit_bytes=40 << 20),
        name="leaders",
    )(*chunks, own, far)


def join_kernel(m0, m1, m2, m3, t0, t1, t2, t3, out, a, b, c):
    for ref, at, main, tail, shift in (
        (a, 0, m0, t0, 0),
        (b, 0, m1, t1, 64),
        (a, 4, m2, t2, 0),
        (b, 4, m3, t3, 64),
    ):
        for half in range(2):
            ref[pl.ds(at + half, TOPK, stride=8), :] = main[half]
        last = tail[...]
        ref[pl.ds(at + 2, TOPK, stride=8), :] = pltpu.roll(last, 64, 1) if shift else last
        ref[pl.ds(at + 3, TOPK, stride=8), :] = last
    merge_top(a, 0, b, 0, c, 0)
    merge_top(c, 0, c, 0, a, 0, turn=4)
    for half in range(2):
        out[half * 128 : (half + 1) * 128, :] = a[pl.ds(half, TOPK, stride=8), :].T
    out[MAIN:SLOTS, :] = a[pl.ds(2, TOPK, stride=8), :].T[0:TAIL, :]


def join(mains, tails):
    return pl.pallas_call(
        join_kernel,
        out_shape=jax.ShapeDtypeStruct((SLOTS, TOPK), jnp.float32),
        in_specs=[pl.BlockSpec(memory_space=pltpu.VMEM)] * 8,
        out_specs=pl.BlockSpec(memory_space=pltpu.VMEM),
        scratch_shapes=[pltpu.VMEM((128 * 8, 128), jnp.float32)] * 3,
        name="join",
    )(*mains, *tails)


def x_ring(step):
    return [(y * 4 + x, y * 4 + (x + step) % 4) for y in range(2) for x in range(4)]


def across(value):
    return lax.ppermute(value, "shard", [(i, (i + 4) % 8) for i in range(8)])


def shards(queries, routes, corpus):
    lang_count = lax.axis_size("lang")
    feature_count = queries.shape[1]
    capacity = CAP
    far = across(corpus)
    widened = queries.astype(jnp.float32)
    unit_query = (
        widened * lax.rsqrt(jnp.mean(widened * widened, axis=1, keepdims=True) + epsilon)
    ).astype(jnp.bfloat16)
    language = routes[:, 0]
    onehot = (language[:, None] == jnp.arange(lang_count, dtype=jnp.int32)[None, :]).astype(jnp.int32)
    slot_index = jnp.sum(jnp.cumsum(onehot, axis=0) * onehot, axis=1) - 1
    position = language * capacity + slot_index
    outbox = jnp.zeros((lang_count * capacity, feature_count), jnp.bfloat16).at[position].set(unit_query)
    mine = lax.all_to_all(outbox, "lang", split_axis=0, concat_axis=0, tiled=True)
    chunks = (mine,) + tuple(lax.ppermute(mine, "shard", x_ring(s)) for s in (1, -1, 2))
    main, tail = leaders(chunks, corpus, far)
    mains, tails = [main[0]], [tail[0]]
    for k, s in ((1, -1), (2, 1), (3, 2)):
        back = lax.ppermute(
            jnp.concatenate([main[k], tail[k // 2][None]], axis=0), "shard", x_ring(s)
        )
        mains.append(back[:2])
        tails.append(back[2])
    owned = join(mains, tails)
    returned = lax.all_to_all(owned, "lang", split_axis=0, concat_axis=0, tiled=True)
    return returned[position]


def solution(mesh):
    placed = (P(("lang", "shard"), None), P(("lang", "shard"), None), P(("lang", "shard"), None))
    return jax.shard_map(
        shards, mesh=mesh, in_specs=placed, out_specs=P(("lang", "shard"), None), check_vma=False
    )
```

```python
import functools

import jax
import jax.numpy as jnp
from jax import lax
from jax.experimental import pallas as pl
from jax.experimental.pallas import tpu as pltpu
from jax.sharding import PartitionSpec as P

TOPK = 128
LANGS = 16
CAP = 20
ROWS = 24
MAIN = 16
TAIL = CAP - MAIN
Q = 128
WIDTH = 768

epsilon = 1e-06


def batcher(n):
    pairs = []
    p = 1
    while p < n:
        k = p
        while k >= 1:
            for j in range(k % p, n - k, 2 * k):
                for i in range(min(k, n - j - k)):
                    if (i + j) // (2 * p) == (i + j + k) // (2 * p):
                        pairs.append((i + j, i + j + k))
            k //= 2
        p *= 2
    return pairs


SORT32 = batcher(32)


def wire(ref, base, i):
    return ref[pl.ds(pl.multiple_of((base + i) * 8, 8), 8), :]


def put(ref, base, i, value):
    ref[pl.ds(pl.multiple_of((base + i) * 8, 8), 8), :] = value


def sort32(ref, base):
    v = [wire(ref, base, i) for i in range(32)]
    for i, j in SORT32:
        v[i], v[j] = jnp.maximum(v[i], v[j]), jnp.minimum(v[i], v[j])
    for i in range(32):
        put(ref, base, i, v[i])


def clean(v):
    n = len(v)
    step = n // 2
    while step:
        for i in range(n):
            if not i & step:
                v[i], v[i + step] = jnp.maximum(v[i], v[i + step]), jnp.minimum(v[i], v[i + step])
        step //= 2
    return v


def clean_at(ref, base):
    v = clean([wire(ref, base, i) for i in range(32)])
    for i in range(32):
        put(ref, base, i, v[i])


def merge64(src, base, dst):
    for op, at in ((jnp.maximum, 0), (jnp.minimum, 32)):
        v = clean([op(wire(src, base, i), wire(src, base, 63 - i)) for i in range(32)])
        for i in range(32):
            put(dst, base + at, i, v[i])


def merge128(src, base, dst):
    for op, at in ((jnp.maximum, 0), (jnp.minimum, 64)):
        v = []
        for i in range(32):
            a = op(wire(src, base, i), wire(src, base, 127 - i))
            b = op(wire(src, base, i + 32), wire(src, base, 95 - i))
            v.append(jnp.maximum(a, b))
            put(dst, base + at + 32, i, jnp.minimum(a, b))
        v = clean(v)
        for i in range(32):
            put(dst, base + at, i, v[i])
        clean_at(dst, base + at + 32)


def merge_top(a, a_base, b, b_base, dst, dst_base, turn=0):
    def other(i):
        value = wire(b, b_base, 127 - i)
        return pltpu.roll(value, turn, 0) if turn else value

    v = []
    for i in range(32):
        c = [jnp.maximum(wire(a, a_base, i + 32 * k), other(i + 32 * k)) for k in range(4)]
        f0, g0 = jnp.maximum(c[0], c[2]), jnp.minimum(c[0], c[2])
        f1, g1 = jnp.maximum(c[1], c[3]), jnp.minimum(c[1], c[3])
        v.append(jnp.maximum(f0, f1))
        put(dst, dst_base + 32, i, jnp.minimum(f0, f1))
        put(dst, dst_base + 64, i, jnp.maximum(g0, g1))
        put(dst, dst_base + 96, i, jnp.minimum(g0, g1))
    v = clean(v)
    for i in range(32):
        put(dst, dst_base, i, v[i])

    def rest(k, carry):
        clean_at(dst, dst_base + 32 + 32 * k)
        return carry

    lax.fori_loop(0, 3, rest, 0)


def loop(n, body):
    def step(i, carry):
        body(i)
        return carry

    lax.fori_loop(0, n, step, 0)


def score(corpus, rows, s):
    for quarter in range(4):
        part = lax.dot_general(
            corpus[quarter * 256 : (quarter + 1) * 256, :],
            rows,
            (((1,), (1,)), ((), ())),
            preferred_element_type=jnp.float32,
        )
        for half in range(2):
            s[pl.ds(quarter * 2 + half, 256, stride=8), :] = part[:, half * 128 : (half + 1) * 128]


def order(s, u, dst):
    loop(8, lambda i: sort32(s, i * 32))
    loop(4, lambda i: merge64(s, i * 64, u))
    loop(2, lambda i: merge128(u, i * 128, s))
    merge_top(s, 0, s, 128, dst, 0)


def leaders(rows_of, groups, own, far, s, u, w, emit):
    def group(g):
        rows = rows_of(g)
        score(own, rows, s)
        order(s, u, w)
        score(far, rows, s)
        order(s, u, u)
        merge_top(w, 0, u, 0, s, 0)
        merge_top(s, 0, s, 0, u, 0, turn=4)
        merge_top(u, 0, u, 0, s, 0, turn=2)
        for half in range(2):
            emit(g, half, s[pl.ds(half, TOPK, stride=8), :].T)

    loop(groups, group)


def main_rows(chunk):
    return chunk[:, 0:MAIN, :].reshape(-1, WIDTH)


def early_kernel(count, *refs):
    chunks, (own, far, out, rows, s, u, w) = refs[:count], refs[count:]
    for k, chunk in enumerate(chunks):
        rows[k * 256 : (k + 1) * 256, :] = main_rows(chunk)

    def emit(g, half, value):
        out[g, half * Q : (half + 1) * Q, :] = value

    leaders(
        lambda g: rows[pl.ds(pl.multiple_of(g * 256, 256), 256), :], count, own, far, s, u, w, emit
    )


def late_kernel(at, mine, cx, cy, cd0, cd1, own, far, first, second, out, rows, tails, s, u, w):
    rows[0:128, :] = main_rows(cd0)
    rows[128:256, :] = main_rows(cd1)
    slot = lax.broadcasted_iota(jnp.int32, (64, LANGS * ROWS), 1)
    row = lax.broadcasted_iota(jnp.int32, (64, LANGS * ROWS), 0)
    picks = (slot == row // TAIL * ROWS + MAIN + row % TAIL).astype(jnp.float32).astype(jnp.bfloat16)
    half_picks = picks[0:32, 0 : 8 * ROWS]

    def tail_of(chunk, sel):
        flat = chunk[...].reshape(-1, WIDTH)
        return jnp.dot(sel, flat, preferred_element_type=jnp.float32).astype(jnp.bfloat16)

    for k, chunk in enumerate((mine, cx, cy)):
        rows[256 + k * 64 : 256 + (k + 1) * 64, :] = tail_of(chunk, picks)
    rows[448:480, :] = tail_of(cd0, half_picks)
    rows[480:512, :] = tail_of(cd1, half_picks)

    me = at[0]
    owner = (me, me ^ 1, me ^ 2, me ^ 3)

    def emit(g, half, value):
        tails[g, half] = value

    leaders(
        lambda g: rows[pl.ds(pl.multiple_of(g * 256, 256), 256), :], 2, own, far, s, u, w, emit
    )
    none = jnp.zeros((ROWS - CAP, TOPK), jnp.float32)
    for k in range(4):
        for lang in range(LANGS):
            if k == 3:
                main = tails[0, lang // 8, lang % 8 * MAIN : (lang % 8 + 1) * MAIN, :]
            else:
                main = (first.at[0] if k == 0 else second.at[k - 1])[lang * MAIN : (lang + 1) * MAIN, :]
            out[lang, owner[k], 0:MAIN, :] = main
            start = k % 2 * 64 + lang * TAIL
            out[lang, owner[k], MAIN:CAP, :] = tails[1, k // 2, start : start + TAIL, :]
            out[lang, owner[k], CAP:ROWS, :] = none


COST = 2 * 256 * 2048 * 768 * 8
VMEM = pl.BlockSpec(memory_space=pltpu.VMEM)
LIMIT = pltpu.CompilerParams(vmem_limit_bytes=40 << 20)


def work(groups):
    return [
        pltpu.VMEM((256 * 8, 128), jnp.float32),
        pltpu.VMEM((256 * 8, 128), jnp.float32),
        pltpu.VMEM((128 * 8, 128), jnp.float32),
    ]


def early(chunks, own, far):
    count = len(chunks)
    return pl.pallas_call(
        functools.partial(early_kernel, count),
        out_shape=jax.ShapeDtypeStruct((count, 256, TOPK), jnp.float32),
        in_specs=[VMEM] * (count + 2),
        out_specs=VMEM,
        scratch_shapes=[pltpu.VMEM((256 * count, WIDTH), jnp.bfloat16)] + work(count),
        compiler_params=LIMIT,
        cost_estimate=pl.CostEstimate(flops=COST * count, bytes_accessed=1 << 20, transcendentals=0),
        name="early",
    )(*chunks, own, far)


def late(at, mine, cx, cy, cd0, cd1, own, far, first, second):
    return pl.pallas_call(
        late_kernel,
        out_shape=jax.ShapeDtypeStruct((LANGS, 4, ROWS, TOPK), jnp.float32),
        in_specs=[pl.BlockSpec(memory_space=pltpu.SMEM)] + [VMEM] * 9,
        out_specs=VMEM,
        scratch_shapes=[
            pltpu.VMEM((512, WIDTH), jnp.bfloat16),
            pltpu.VMEM((2, 2, Q, TOPK), jnp.float32),
        ]
        + work(2),
        compiler_params=LIMIT,
        cost_estimate=pl.CostEstimate(flops=COST * 2, bytes_accessed=1 << 20, transcendentals=0),
        name="late",
    )(at, mine, cx, cy, cd0, cd1, own, far, first, second)


def outbox_kernel(queries, routes, out, slots):
    x = queries[...].astype(jnp.float32)
    unit = (x * lax.rsqrt(jnp.mean(x * x, axis=1, keepdims=True) + epsilon)).astype(jnp.bfloat16)
    along = jnp.broadcast_to(routes[...].astype(jnp.float32), (Q, Q))
    down = along.T
    before = lax.broadcasted_iota(jnp.int32, (Q, Q), 0) < lax.broadcasted_iota(jnp.int32, (Q, Q), 1)
    earlier = jnp.where(before & (along == down), 1.0, 0.0)
    rank = jnp.sum(earlier, axis=0, keepdims=True)
    place = routes[...] * ROWS + rank.astype(jnp.int32)
    slots[...] = place
    total = LANGS * ROWS
    hits = lax.broadcasted_iota(jnp.int32, (total, Q), 0) == jnp.broadcast_to(place, (total, Q))
    picks = jnp.where(hits, 1.0, 0.0).astype(jnp.bfloat16)
    box = jnp.dot(picks, unit, preferred_element_type=jnp.float32).astype(jnp.bfloat16)
    out[...] = box.reshape(LANGS, ROWS, WIDTH)


def outbox_of(queries, routes):
    return pl.pallas_call(
        outbox_kernel,
        out_shape=(
            jax.ShapeDtypeStruct((LANGS, ROWS, WIDTH), jnp.bfloat16),
            jax.ShapeDtypeStruct((1, Q), jnp.int32),
        ),
        in_specs=[VMEM] * 2,
        out_specs=(VMEM, VMEM),
        compiler_params=LIMIT,
        name="outbox",
    )(queries, routes)


def join_kernel(back, slots, out, a, b):
    total = LANGS * ROWS
    hits = lax.broadcasted_iota(jnp.int32, (total, Q), 0) == jnp.broadcast_to(slots[...], (total, Q))
    picks = jnp.where(hits, 1.0, 0.0)
    picks = jnp.concatenate([picks[i * Q : (i + 1) * Q, :].T for i in range(total // Q)], axis=1)
    picks = picks.astype(jnp.bfloat16)
    for k in range(4):
        left = back[:, k].reshape(total, TOPK)
        rows = jnp.zeros((Q, TOPK), jnp.float32)
        for _ in range(3):
            part = left.astype(jnp.bfloat16)
            left = left - part.astype(jnp.float32)
            rows = rows + jnp.dot(picks, part, preferred_element_type=jnp.float32)
        ranks = rows.T
        a[pl.ds(k, TOPK, stride=8), :] = ranks
        a[pl.ds(k + 4, TOPK, stride=8), :] = ranks
    merge_top(a, 0, a, 0, b, 0, turn=2)
    merge_top(b, 0, b, 0, a, 0, turn=1)
    out[...] = a[pl.ds(0, TOPK, stride=8), :].T


def join(back, slots):
    return pl.pallas_call(
        join_kernel,
        out_shape=jax.ShapeDtypeStruct((Q, TOPK), jnp.float32),
        in_specs=[VMEM] * 2,
        out_specs=VMEM,
        scratch_shapes=[pltpu.VMEM((128 * 8, 128), jnp.float32)] * 2,
        compiler_params=LIMIT,
        name="join",
    )(back, slots)


AXES = ("lang", "shard")


def moves(target):
    return [
        (lang * 8 + y * 4 + x, lang * 8 + ty * 4 + tx % 4)
        for lang in range(16)
        for y in range(2)
        for x in range(4)
        for ty, tx in (target(lang % 2, y, x),)
    ]


def pair(core, y, x):
    return y, x + (1 if (x + core) % 2 == 0 else -1)


def over_x(core, y, x):
    return y, x + 2


def over_y(core, y, x):
    return 1 - y, x


TEAMS = [
    [lang * 8 + y * 4 + odd + 2 * half for lang in range(16) for y in range(2) for half in range(2)]
    for odd in range(2)
]


def shards(queries, routes, corpus):
    far = lax.ppermute(corpus, AXES, moves(pair))
    outbox, slots = outbox_of(queries, routes.reshape(1, Q))
    mine = lax.all_to_all(outbox, "lang", split_axis=0, concat_axis=0, tiled=True)
    cx = lax.ppermute(mine, AXES, moves(over_x))
    cy = lax.ppermute(mine, AXES, moves(over_y))
    cd0 = lax.ppermute(cx[:8], AXES, moves(over_y))
    cd1 = lax.ppermute(cy[8:], AXES, moves(over_x))
    first = early((mine,), corpus, far)
    second = early((cx, cy), corpus, far)
    shard = lax.axis_index("shard")
    at = (shard // 4 * 2 + shard % 4 // 2).astype(jnp.int32).reshape(1)
    found = late(at, mine, cx, cy, cd0, cd1, corpus, far, first, second)
    back = lax.all_to_all(
        found.reshape(LANGS * 4, ROWS, TOPK), AXES, 0, 0, axis_index_groups=TEAMS, tiled=True
    )
    return join(back.reshape(LANGS, 4, ROWS, TOPK), slots)


def solution(mesh):
    placed = (P(AXES, None), P(AXES, None), P(AXES, None))
    return jax.shard_map(shards, mesh=mesh, in_specs=placed, out_specs=P(AXES, None), check_vma=False)
```

```python
import functools

import jax
import jax.numpy as jnp
from jax import lax
from jax.experimental import pallas as pl
from jax.experimental.pallas import tpu as pltpu
from jax.sharding import PartitionSpec as P

TOPK = 128
LANGS = 16
CAP = 20
ROWS = 24
MAIN = 16
TAIL = CAP - MAIN
Q = 128
WIDTH = 768

epsilon = 1e-06


def batcher(n):
    pairs = []
    p = 1
    while p < n:
        k = p
        while k >= 1:
            for j in range(k % p, n - k, 2 * k):
                for i in range(min(k, n - j - k)):
                    if (i + j) // (2 * p) == (i + j + k) // (2 * p):
                        pairs.append((i + j, i + j + k))
            k //= 2
        p *= 2
    return pairs


SORT32 = batcher(32)


def wire(ref, base, i):
    return ref[pl.ds(pl.multiple_of((base + i) * 8, 8), 8), :]


def put(ref, base, i, value):
    ref[pl.ds(pl.multiple_of((base + i) * 8, 8), 8), :] = value


def sort32(ref, base):
    v = [wire(ref, base, i) for i in range(32)]
    for i, j in SORT32:
        v[i], v[j] = jnp.maximum(v[i], v[j]), jnp.minimum(v[i], v[j])
    for i in range(32):
        put(ref, base, i, v[i])


def clean(v):
    n = len(v)
    step = n // 2
    while step:
        for i in range(n):
            if not i & step:
                v[i], v[i + step] = jnp.maximum(v[i], v[i + step]), jnp.minimum(v[i], v[i + step])
        step //= 2
    return v


def clean_at(ref, base):
    v = clean([wire(ref, base, i) for i in range(32)])
    for i in range(32):
        put(ref, base, i, v[i])


def merge64(src, base, dst):
    for op, at in ((jnp.maximum, 0), (jnp.minimum, 32)):
        v = clean([op(wire(src, base, i), wire(src, base, 63 - i)) for i in range(32)])
        for i in range(32):
            put(dst, base + at, i, v[i])


def merge128(src, base, dst):
    for op, at in ((jnp.maximum, 0), (jnp.minimum, 64)):
        v = []
        for i in range(32):
            a = op(wire(src, base, i), wire(src, base, 127 - i))
            b = op(wire(src, base, i + 32), wire(src, base, 95 - i))
            v.append(jnp.maximum(a, b))
            put(dst, base + at + 32, i, jnp.minimum(a, b))
        v = clean(v)
        for i in range(32):
            put(dst, base + at, i, v[i])
        clean_at(dst, base + at + 32)


def merge_top(a, a_base, b, b_base, dst, dst_base, turn=0):
    def other(i):
        value = wire(b, b_base, 127 - i)
        return pltpu.roll(value, turn, 0) if turn else value

    v = []
    for i in range(32):
        c = [jnp.maximum(wire(a, a_base, i + 32 * k), other(i + 32 * k)) for k in range(4)]
        f0, g0 = jnp.maximum(c[0], c[2]), jnp.minimum(c[0], c[2])
        f1, g1 = jnp.maximum(c[1], c[3]), jnp.minimum(c[1], c[3])
        v.append(jnp.maximum(f0, f1))
        put(dst, dst_base + 32, i, jnp.minimum(f0, f1))
        put(dst, dst_base + 64, i, jnp.maximum(g0, g1))
        put(dst, dst_base + 96, i, jnp.minimum(g0, g1))
    v = clean(v)
    for i in range(32):
        put(dst, dst_base, i, v[i])

    def rest(k, carry):
        clean_at(dst, dst_base + 32 + 32 * k)
        return carry

    lax.fori_loop(0, 3, rest, 0)


def loop(n, body):
    def step(i, carry):
        body(i)
        return carry

    lax.fori_loop(0, n, step, 0)


def score(corpus, rows, s):
    for quarter in range(4):
        part = lax.dot_general(
            corpus[quarter * 256 : (quarter + 1) * 256, :],
            rows,
            (((1,), (1,)), ((), ())),
            preferred_element_type=jnp.float32,
        )
        for half in range(2):
            s[pl.ds(quarter * 2 + half, 256, stride=8), :] = part[:, half * 128 : (half + 1) * 128]


def order(s, u, dst):
    loop(8, lambda i: sort32(s, i * 32))
    loop(4, lambda i: merge64(s, i * 64, u))
    loop(2, lambda i: merge128(u, i * 128, s))
    merge_top(s, 0, s, 128, dst, 0)


def leaders(rows_of, groups, own, far, s, u, w, emit):
    def group(g):
        rows = rows_of(g)
        score(own, rows, s)
        order(s, u, w)
        score(far, rows, s)
        order(s, u, u)
        merge_top(w, 0, u, 0, s, 0)
        merge_top(s, 0, s, 0, u, 0, turn=4)
        merge_top(u, 0, u, 0, s, 0, turn=2)
        for half in range(2):
            emit(g, half, s[pl.ds(half, TOPK, stride=8), :].T)

    loop(groups, group)


def main_rows(chunk):
    return chunk[:, 0:MAIN, :].reshape(-1, WIDTH)


def early_kernel(count, *refs):
    chunks, (own, far, out, rows, s, u, w) = refs[:count], refs[count:]
    for k, chunk in enumerate(chunks):
        rows[k * 256 : (k + 1) * 256, :] = main_rows(chunk)

    def emit(g, half, value):
        out[g, half * Q : (half + 1) * Q, :] = value

    leaders(
        lambda g: rows[pl.ds(pl.multiple_of(g * 256, 256), 256), :], count, own, far, s, u, w, emit
    )


STEPS = 800.0
FLOOR = 32.5
LN2 = 0.6931471805599453


def coded(v):
    level = jnp.round(jnp.log(jnp.abs(v)) * (STEPS / LN2) + STEPS * FLOOR)
    level = jnp.clip(level, 0.0, 32767.0)
    return jnp.where(v < 0, -level, level)


def decoded(c):
    level = jnp.abs(c)
    v = jnp.where(level > 0, jnp.exp(level * (LN2 / STEPS) - FLOOR * LN2), 0.0)
    return jnp.where(c < 0, -v, v)


def late_kernel(at, mine, cx, cy, cd0, cd1, own, far, first, second, out, rows, tails, box, s, u, w):
    rows[0:128, :] = main_rows(cd0)
    rows[128:256, :] = main_rows(cd1)
    slot = lax.broadcasted_iota(jnp.int32, (64, LANGS * ROWS), 1)
    row = lax.broadcasted_iota(jnp.int32, (64, LANGS * ROWS), 0)
    picks = (slot == row // TAIL * ROWS + MAIN + row % TAIL).astype(jnp.float32).astype(jnp.bfloat16)
    half_picks = picks[0:32, 0 : 8 * ROWS]

    def tail_of(chunk, sel):
        flat = chunk[...].reshape(-1, WIDTH)
        return jnp.dot(sel, flat, preferred_element_type=jnp.float32).astype(jnp.bfloat16)

    for k, chunk in enumerate((mine, cx, cy)):
        rows[256 + k * 64 : 256 + (k + 1) * 64, :] = tail_of(chunk, picks)
    rows[448:480, :] = tail_of(cd0, half_picks)
    rows[480:512, :] = tail_of(cd1, half_picks)

    me = at[0]
    owner = (me, me ^ 1, me ^ 2, me ^ 3)

    def emit(g, half, value):
        tails[g, half] = value

    leaders(
        lambda g: rows[pl.ds(pl.multiple_of(g * 256, 256), 256), :], 2, own, far, s, u, w, emit
    )
    none = jnp.zeros((ROWS - CAP, TOPK), jnp.float32)
    for k in range(4):
        for lang in range(LANGS):
            if k == 3:
                main = tails[0, lang // 8, lang % 8 * MAIN : (lang % 8 + 1) * MAIN, :]
            else:
                main = (first.at[0] if k == 0 else second.at[k - 1])[lang * MAIN : (lang + 1) * MAIN, :]
            box[k, 0:MAIN, :] = main
            start = k % 2 * 64 + lang * TAIL
            box[k, MAIN:CAP, :] = tails[1, k // 2, start : start + TAIL, :]
            box[k, CAP:ROWS, :] = none
            out[lang, owner[k]] = coded(box[k]).astype(jnp.int32).astype(jnp.int16)


COST = 2 * 256 * 2048 * 768 * 8
VMEM = pl.BlockSpec(memory_space=pltpu.VMEM)
LIMIT = pltpu.CompilerParams(vmem_limit_bytes=40 << 20)


def work(groups):
    return [
        pltpu.VMEM((256 * 8, 128), jnp.float32),
        pltpu.VMEM((256 * 8, 128), jnp.float32),
        pltpu.VMEM((128 * 8, 128), jnp.float32),
    ]


def early(chunks, own, far):
    count = len(chunks)
    return pl.pallas_call(
        functools.partial(early_kernel, count),
        out_shape=jax.ShapeDtypeStruct((count, 256, TOPK), jnp.float32),
        in_specs=[VMEM] * (count + 2),
        out_specs=VMEM,
        scratch_shapes=[pltpu.VMEM((256 * count, WIDTH), jnp.bfloat16)] + work(count),
        compiler_params=LIMIT,
        cost_estimate=pl.CostEstimate(flops=COST * count, bytes_accessed=1 << 20, transcendentals=0),
        name="early",
    )(*chunks, own, far)


def late(at, mine, cx, cy, cd0, cd1, own, far, first, second):
    return pl.pallas_call(
        late_kernel,
        out_shape=jax.ShapeDtypeStruct((LANGS, 4, ROWS, TOPK), jnp.int16),
        in_specs=[pl.BlockSpec(memory_space=pltpu.SMEM)] + [VMEM] * 9,
        out_specs=VMEM,
        scratch_shapes=[
            pltpu.VMEM((512, WIDTH), jnp.bfloat16),
            pltpu.VMEM((2, 2, Q, TOPK), jnp.float32),
            pltpu.VMEM((4, ROWS, TOPK), jnp.float32),
        ]
        + work(2),
        compiler_params=LIMIT,
        cost_estimate=pl.CostEstimate(flops=COST * 2, bytes_accessed=1 << 20, transcendentals=0),
        name="late",
    )(at, mine, cx, cy, cd0, cd1, own, far, first, second)


def outbox_kernel(queries, routes, out, slots):
    x = queries[...].astype(jnp.float32)
    unit = (x * lax.rsqrt(jnp.mean(x * x, axis=1, keepdims=True) + epsilon)).astype(jnp.bfloat16)
    along = jnp.broadcast_to(routes[...].astype(jnp.float32), (Q, Q))
    down = along.T
    before = lax.broadcasted_iota(jnp.int32, (Q, Q), 0) < lax.broadcasted_iota(jnp.int32, (Q, Q), 1)
    earlier = jnp.where(before & (along == down), 1.0, 0.0)
    rank = jnp.sum(earlier, axis=0, keepdims=True)
    place = routes[...] * ROWS + rank.astype(jnp.int32)
    slots[...] = place
    total = LANGS * ROWS
    hits = lax.broadcasted_iota(jnp.int32, (total, Q), 0) == jnp.broadcast_to(place, (total, Q))
    picks = jnp.where(hits, 1.0, 0.0).astype(jnp.bfloat16)
    box = jnp.dot(picks, unit, preferred_element_type=jnp.float32).astype(jnp.bfloat16)
    out[...] = box.reshape(LANGS, ROWS, WIDTH)


def outbox_of(queries, routes):
    return pl.pallas_call(
        outbox_kernel,
        out_shape=(
            jax.ShapeDtypeStruct((LANGS, ROWS, WIDTH), jnp.bfloat16),
            jax.ShapeDtypeStruct((1, Q), jnp.int32),
        ),
        in_specs=[VMEM] * 2,
        out_specs=(VMEM, VMEM),
        compiler_params=LIMIT,
        name="outbox",
    )(queries, routes)


def join_kernel(back, slots, out, a, b):
    total = LANGS * ROWS
    hits = lax.broadcasted_iota(jnp.int32, (total, Q), 0) == jnp.broadcast_to(slots[...], (total, Q))
    picks = jnp.where(hits, 1.0, 0.0)
    picks = jnp.concatenate([picks[i * Q : (i + 1) * Q, :].T for i in range(total // Q)], axis=1)
    picks = picks.astype(jnp.bfloat16)
    for k in range(4):
        code = back[:, k].astype(jnp.int32).astype(jnp.float32).reshape(total, TOPK)
        high = code.astype(jnp.bfloat16)
        low = (code - high.astype(jnp.float32)).astype(jnp.bfloat16)
        rows = jnp.dot(picks, high, preferred_element_type=jnp.float32) + jnp.dot(
            picks, low, preferred_element_type=jnp.float32
        )
        ranks = decoded(rows).T
        a[pl.ds(k, TOPK, stride=8), :] = ranks
        a[pl.ds(k + 4, TOPK, stride=8), :] = ranks
    merge_top(a, 0, a, 0, b, 0, turn=2)
    merge_top(b, 0, b, 0, a, 0, turn=1)
    out[...] = a[pl.ds(0, TOPK, stride=8), :].T


def join(back, slots):
    return pl.pallas_call(
        join_kernel,
        out_shape=jax.ShapeDtypeStruct((Q, TOPK), jnp.float32),
        in_specs=[VMEM] * 2,
        out_specs=VMEM,
        scratch_shapes=[pltpu.VMEM((128 * 8, 128), jnp.float32)] * 2,
        compiler_params=LIMIT,
        name="join",
    )(back, slots)


AXES = ("lang", "shard")


def moves(target):
    return [
        (lang * 8 + y * 4 + x, lang * 8 + ty * 4 + tx % 4)
        for lang in range(16)
        for y in range(2)
        for x in range(4)
        for ty, tx in (target(lang % 2, y, x),)
    ]


def pair(core, y, x):
    return y, x + (1 if (x + core) % 2 == 0 else -1)


def over_x(core, y, x):
    return y, x + 2


def over_y(core, y, x):
    return 1 - y, x


TEAMS = [
    [lang * 8 + y * 4 + odd + 2 * half for lang in range(16) for y in range(2) for half in range(2)]
    for odd in range(2)
]


def shards(queries, routes, corpus):
    far = lax.ppermute(corpus, AXES, moves(pair))
    outbox, slots = outbox_of(queries, routes.reshape(1, Q))
    mine = lax.all_to_all(outbox, "lang", split_axis=0, concat_axis=0, tiled=True)
    cx = lax.ppermute(mine, AXES, moves(over_x))
    cy = lax.ppermute(mine, AXES, moves(over_y))
    first = early((mine,), corpus, far)
    cx, cy, first = lax.optimization_barrier((cx, cy, first))
    cd0 = lax.ppermute(cx[:8], AXES, moves(over_y))
    cd1 = lax.ppermute(cy[8:], AXES, moves(over_x))
    second = early((cx, cy), corpus, far)
    shard = lax.axis_index("shard")
    at = (shard // 4 * 2 + shard % 4 // 2).astype(jnp.int32).reshape(1)
    found = late(at, mine, cx, cy, cd0, cd1, corpus, far, first, second)
    back = lax.all_to_all(
        found.reshape(LANGS * 4, ROWS, TOPK), AXES, 0, 0, axis_index_groups=TEAMS, tiled=True
    )
    return join(back.reshape(LANGS, 4, ROWS, TOPK), slots)


def solution(mesh):
    placed = (P(AXES, None), P(AXES, None), P(AXES, None))
    return jax.shard_map(shards, mesh=mesh, in_specs=placed, out_specs=P(AXES, None), check_vma=False)
```

```python
import functools

import jax
import jax.numpy as jnp
from jax import lax
from jax.experimental import pallas as pl
from jax.experimental.pallas import tpu as pltpu
from jax.sharding import PartitionSpec as P

TOPK = 128
LANGS = 16
CAP = 20
ROWS = 24
MAIN = 16
TAIL = CAP - MAIN
Q = 128
WIDTH = 768

epsilon = 1e-06


def batcher(n):
    pairs = []
    p = 1
    while p < n:
        k = p
        while k >= 1:
            for j in range(k % p, n - k, 2 * k):
                for i in range(min(k, n - j - k)):
                    if (i + j) // (2 * p) == (i + j + k) // (2 * p):
                        pairs.append((i + j, i + j + k))
            k //= 2
        p *= 2
    return pairs


SORT32 = batcher(32)


def wire(ref, base, i):
    return ref[pl.ds(pl.multiple_of((base + i) * 8, 8), 8), :]


def put(ref, base, i, value):
    ref[pl.ds(pl.multiple_of((base + i) * 8, 8), 8), :] = value


def sort32(ref, base):
    v = [wire(ref, base, i) for i in range(32)]
    for i, j in SORT32:
        v[i], v[j] = jnp.maximum(v[i], v[j]), jnp.minimum(v[i], v[j])
    for i in range(32):
        put(ref, base, i, v[i])


def clean(v):
    n = len(v)
    step = n // 2
    while step:
        for i in range(n):
            if not i & step:
                v[i], v[i + step] = jnp.maximum(v[i], v[i + step]), jnp.minimum(v[i], v[i + step])
        step //= 2
    return v


def clean_at(ref, base):
    v = clean([wire(ref, base, i) for i in range(32)])
    for i in range(32):
        put(ref, base, i, v[i])


def merge64(src, base, dst):
    for op, at in ((jnp.maximum, 0), (jnp.minimum, 32)):
        v = clean([op(wire(src, base, i), wire(src, base, 63 - i)) for i in range(32)])
        for i in range(32):
            put(dst, base + at, i, v[i])


def merge128(src, base, dst):
    for op, at in ((jnp.maximum, 0), (jnp.minimum, 64)):
        v = []
        for i in range(32):
            a = op(wire(src, base, i), wire(src, base, 127 - i))
            b = op(wire(src, base, i + 32), wire(src, base, 95 - i))
            v.append(jnp.maximum(a, b))
            put(dst, base + at + 32, i, jnp.minimum(a, b))
        v = clean(v)
        for i in range(32):
            put(dst, base + at, i, v[i])
        clean_at(dst, base + at + 32)


def merge_top(a, a_base, b, b_base, dst, dst_base, turn=0):
    def other(i):
        value = wire(b, b_base, 127 - i)
        return pltpu.roll(value, turn, 0) if turn else value

    v = []
    for i in range(32):
        c = [jnp.maximum(wire(a, a_base, i + 32 * k), other(i + 32 * k)) for k in range(4)]
        f0, g0 = jnp.maximum(c[0], c[2]), jnp.minimum(c[0], c[2])
        f1, g1 = jnp.maximum(c[1], c[3]), jnp.minimum(c[1], c[3])
        v.append(jnp.maximum(f0, f1))
        put(dst, dst_base + 32, i, jnp.minimum(f0, f1))
        put(dst, dst_base + 64, i, jnp.maximum(g0, g1))
        put(dst, dst_base + 96, i, jnp.minimum(g0, g1))
    v = clean(v)
    for i in range(32):
        put(dst, dst_base, i, v[i])

    def rest(k, carry):
        clean_at(dst, dst_base + 32 + 32 * k)
        return carry

    lax.fori_loop(0, 3, rest, 0)


def loop(n, body):
    def step(i, carry):
        body(i)
        return carry

    lax.fori_loop(0, n, step, 0)


def score(corpus, rows, s):
    for quarter in range(4):
        part = lax.dot_general(
            corpus[quarter * 256 : (quarter + 1) * 256, :],
            rows,
            (((1,), (1,)), ((), ())),
            preferred_element_type=jnp.float32,
        )
        for half in range(2):
            s[pl.ds(quarter * 2 + half, 256, stride=8), :] = part[:, half * 128 : (half + 1) * 128]


def order(s, u, dst):
    loop(8, lambda i: sort32(s, i * 32))
    loop(4, lambda i: merge64(s, i * 64, u))
    loop(2, lambda i: merge128(u, i * 128, s))
    merge_top(s, 0, s, 128, dst, 0)


def leaders(rows_of, groups, own, far, s, u, w, emit):
    def group(g):
        rows = rows_of(g)
        score(own, rows, s)
        order(s, u, w)
        score(far, rows, s)
        order(s, u, u)
        merge_top(w, 0, u, 0, s, 0)
        merge_top(s, 0, s, 0, u, 0, turn=4)
        merge_top(u, 0, u, 0, s, 0, turn=2)
        for half in range(2):
            emit(g, half, s[pl.ds(half, TOPK, stride=8), :].T)

    loop(groups, group)


def main_rows(chunk):
    return chunk[:, 0:MAIN, :].reshape(-1, WIDTH)


def first_kernel(chunk, own, far, out, both, rows, s, u, w):
    rows[...] = main_rows(chunk)
    both[0] = own[...]
    both[1] = far[...]

    def emit(g, half, value):
        out[half * Q : (half + 1) * Q, :] = value

    leaders(lambda g: rows[...], 1, own, far, s, u, w, emit)


def early_kernel(half0, half1, both, out, rows, s, u, w):
    rows[0:128, :] = main_rows(half0)
    rows[128:256, :] = main_rows(half1)

    def emit(g, half, value):
        out[half * Q : (half + 1) * Q, :] = value

    leaders(lambda g: rows[...], 1, both.at[0], both.at[1], s, u, w, emit)


STEPS = 800.0
FLOOR = 32.5
LN2 = 0.6931471805599453


def coded(v):
    level = jnp.round(jnp.log(jnp.abs(v)) * (STEPS / LN2) + STEPS * FLOOR)
    level = jnp.clip(level, 0.0, 32767.0)
    return jnp.where(v < 0, -level, level)


def decoded(c):
    level = jnp.abs(c)
    v = jnp.where(level > 0, jnp.exp(level * (LN2 / STEPS) - FLOOR * LN2), 0.0)
    return jnp.where(c < 0, -v, v)


def late_kernel(at, mine, cx0, cx1, cy0, cy1, cd0, cd1, both, r0, r1, r2, out, *scratch):
    rows, tails, box, s, u, w = scratch
    rows[0:128, :] = main_rows(cd0)
    rows[128:256, :] = main_rows(cd1)
    slot = lax.broadcasted_iota(jnp.int32, (64, LANGS * ROWS), 1)
    row = lax.broadcasted_iota(jnp.int32, (64, LANGS * ROWS), 0)
    picks = (slot == row // TAIL * ROWS + MAIN + row % TAIL).astype(jnp.float32).astype(jnp.bfloat16)
    half_picks = picks[0:32, 0 : 8 * ROWS]

    def tail_of(chunk, sel):
        flat = chunk[...].reshape(-1, WIDTH)
        return jnp.dot(sel, flat, preferred_element_type=jnp.float32).astype(jnp.bfloat16)

    rows[256:320, :] = tail_of(mine, picks)
    for k, chunk in enumerate((cx0, cx1, cy0, cy1, cd0, cd1)):
        rows[320 + k * 32 : 352 + k * 32, :] = tail_of(chunk, half_picks)

    def emit(g, half, value):
        tails[g, half] = value

    leaders(
        lambda g: rows[pl.ds(pl.multiple_of(g * 256, 256), 256), :], 2, both.at[0], both.at[1], s, u, w, emit
    )
    me = at[0]
    owner = (me, me ^ 1, me ^ 2, me ^ 3)
    none = jnp.zeros((ROWS - CAP, TOPK), jnp.float32)
    for k in range(4):
        for lang in range(LANGS):
            half, start = lang // 8, lang % 8 * MAIN
            if k == 0:
                main = r0[lang * MAIN : (lang + 1) * MAIN, :]
            elif k < 3:
                start += (k - 1) * Q
                main = (r1, r2)[half][start : start + MAIN, :]
            else:
                main = tails[0, half, start : start + MAIN, :]
            box[k, 0:MAIN, :] = main
            start = k % 2 * 64 + lang * TAIL
            box[k, MAIN:CAP, :] = tails[1, k // 2, start : start + TAIL, :]
            box[k, CAP:ROWS, :] = none
            out[lang, owner[k]] = coded(box[k]).astype(jnp.int32).astype(jnp.int16)


COST = 2 * 256 * 2048 * 768 * 8
VMEM = pl.BlockSpec(memory_space=pltpu.VMEM)
LIMIT = pltpu.CompilerParams(vmem_limit_bytes=14 << 20)
WORK = [
    pltpu.VMEM((256 * 8, 128), jnp.float32),
    pltpu.VMEM((256 * 8, 128), jnp.float32),
    pltpu.VMEM((128 * 8, 128), jnp.float32),
]


def first(chunk, own, far):
    return pl.pallas_call(
        first_kernel,
        out_shape=(
            jax.ShapeDtypeStruct((256, TOPK), jnp.float32),
            jax.ShapeDtypeStruct((2, 1024, WIDTH), jnp.bfloat16),
        ),
        in_specs=[VMEM] * 3,
        out_specs=(VMEM, VMEM),
        scratch_shapes=[pltpu.VMEM((256, WIDTH), jnp.bfloat16)] + WORK,
        compiler_params=LIMIT,
        cost_estimate=pl.CostEstimate(flops=COST, bytes_accessed=1 << 20, transcendentals=0),
        name="first",
    )(chunk, own, far)


def early(half0, half1, both):
    return pl.pallas_call(
        early_kernel,
        out_shape=jax.ShapeDtypeStruct((256, TOPK), jnp.float32),
        in_specs=[VMEM] * 3,
        out_specs=VMEM,
        scratch_shapes=[pltpu.VMEM((256, WIDTH), jnp.bfloat16)] + WORK,
        compiler_params=LIMIT,
        cost_estimate=pl.CostEstimate(flops=COST, bytes_accessed=1 << 20, transcendentals=0),
        name="early",
    )(half0, half1, both)


def late(at, chunks, both, results):
    return pl.pallas_call(
        late_kernel,
        out_shape=jax.ShapeDtypeStruct((LANGS, 4, ROWS, TOPK), jnp.int16),
        in_specs=[pl.BlockSpec(memory_space=pltpu.SMEM)] + [VMEM] * 11,
        out_specs=VMEM,
        scratch_shapes=[
            pltpu.VMEM((512, WIDTH), jnp.bfloat16),
            pltpu.VMEM((2, 2, Q, TOPK), jnp.float32),
            pltpu.VMEM((4, ROWS, TOPK), jnp.float32),
        ]
        + WORK,
        compiler_params=LIMIT,
        cost_estimate=pl.CostEstimate(flops=COST * 2, bytes_accessed=1 << 20, transcendentals=0),
        name="late",
    )(at, *chunks, both, *results)


def outbox_kernel(queries_in, routes_in, out, slots, queries, routes, sems):
    copies = (
        pltpu.make_async_copy(routes_in, routes, sems.at[0]),
        pltpu.make_async_copy(queries_in, queries, sems.at[1]),
    )
    for copy in copies:
        copy.start()
    for copy in copies:
        copy.wait()
    x = queries[...].astype(jnp.float32)
    unit = (x * lax.rsqrt(jnp.mean(x * x, axis=1, keepdims=True) + epsilon)).astype(jnp.bfloat16)
    along = jnp.broadcast_to(routes[...].astype(jnp.float32), (Q, Q))
    down = along.T
    before = lax.broadcasted_iota(jnp.int32, (Q, Q), 0) < lax.broadcasted_iota(jnp.int32, (Q, Q), 1)
    earlier = jnp.where(before & (along == down), 1.0, 0.0)
    rank = jnp.sum(earlier, axis=0, keepdims=True)
    place = routes[...] * ROWS + rank.astype(jnp.int32)
    slots[...] = place
    total = LANGS * ROWS
    hits = lax.broadcasted_iota(jnp.int32, (total, Q), 0) == jnp.broadcast_to(place, (total, Q))
    picks = jnp.where(hits, 1.0, 0.0).astype(jnp.bfloat16)
    box = jnp.dot(picks, unit, preferred_element_type=jnp.float32).astype(jnp.bfloat16)
    out[...] = box.reshape(LANGS, ROWS, WIDTH)


def outbox_of(queries, routes):
    return pl.pallas_call(
        outbox_kernel,
        out_shape=(
            jax.ShapeDtypeStruct((LANGS, ROWS, WIDTH), jnp.bfloat16),
            jax.ShapeDtypeStruct((1, Q), jnp.int32),
        ),
        in_specs=[pl.BlockSpec(memory_space=pltpu.HBM)] * 2,
        out_specs=(VMEM, VMEM),
        scratch_shapes=[
            pltpu.VMEM((Q, WIDTH), jnp.bfloat16),
            pltpu.VMEM((1, Q), jnp.int32),
            pltpu.SemaphoreType.DMA((2,)),
        ],
        compiler_params=LIMIT,
        name="outbox",
    )(queries, routes)


def join_kernel(back, slots, out, a, b):
    total = LANGS * ROWS
    hits = lax.broadcasted_iota(jnp.int32, (total, Q), 0) == jnp.broadcast_to(slots[...], (total, Q))
    picks = jnp.where(hits, 1.0, 0.0)
    picks = jnp.concatenate([picks[i * Q : (i + 1) * Q, :].T for i in range(total // Q)], axis=1)
    picks = picks.astype(jnp.bfloat16)
    for k in range(4):
        code = back[:, k].astype(jnp.int32).astype(jnp.float32).reshape(total, TOPK)
        high = code.astype(jnp.bfloat16)
        low = (code - high.astype(jnp.float32)).astype(jnp.bfloat16)
        rows = jnp.dot(picks, high, preferred_element_type=jnp.float32) + jnp.dot(
            picks, low, preferred_element_type=jnp.float32
        )
        ranks = decoded(rows).T
        a[pl.ds(k, TOPK, stride=8), :] = ranks
        a[pl.ds(k + 4, TOPK, stride=8), :] = ranks
    merge_top(a, 0, a, 0, b, 0, turn=2)
    merge_top(b, 0, b, 0, a, 0, turn=1)
    out[...] = a[pl.ds(0, TOPK, stride=8), :].T


def join(back, slots):
    return pl.pallas_call(
        join_kernel,
        out_shape=jax.ShapeDtypeStruct((Q, TOPK), jnp.float32),
        in_specs=[VMEM] * 2,
        out_specs=VMEM,
        scratch_shapes=[pltpu.VMEM((128 * 8, 128), jnp.float32)] * 2,
        compiler_params=LIMIT,
        name="join",
    )(back, slots)


AXES = ("lang", "shard")


def moves(target):
    return [
        (lang * 8 + y * 4 + x, lang * 8 + ty * 4 + tx % 4)
        for lang in range(16)
        for y in range(2)
        for x in range(4)
        for ty, tx in (target(lang % 2, y, x),)
    ]


def pair(core, y, x):
    return y, x + (1 if (x + core) % 2 == 0 else -1)


def over_x(core, y, x):
    return y, x + 2


def over_y(core, y, x):
    return 1 - y, x


TEAMS = [
    [lang * 8 + y * 4 + odd + 2 * half for lang in range(16) for y in range(2) for half in range(2)]
    for odd in range(2)
]


def shards(queries, routes, corpus):
    far = lax.ppermute(corpus, AXES, moves(pair))
    outbox, slots = outbox_of(queries, routes.reshape(1, Q))
    mine = lax.all_to_all(outbox, "lang", split_axis=0, concat_axis=0, tiled=True)
    cx0, cy0, cx1, cy1 = (
        lax.ppermute(part, AXES, moves(over)) for part in (mine[:8], mine[8:]) for over in (over_x, over_y)
    )
    r0, both = first(mine, corpus, far)
    cx0, cy0, r0 = lax.optimization_barrier((cx0, cy0, r0))
    cd0 = lax.ppermute(cx0, AXES, moves(over_y))
    r1 = early(cx0, cy0, both)
    cx1, cy1, r1 = lax.optimization_barrier((cx1, cy1, r1))
    cd1 = lax.ppermute(cy1, AXES, moves(over_x))
    r2 = early(cx1, cy1, both)
    shard = lax.axis_index("shard")
    at = (lax.shift_right_logical(shard, 2) * 2 + (lax.shift_right_logical(shard, 1) & 1)).reshape(1)
    found = late(at, (mine, cx0, cx1, cy0, cy1, cd0, cd1), both, (r0, r1, r2))
    back = lax.all_to_all(
        found.reshape(LANGS * 4, ROWS, TOPK), AXES, 0, 0, axis_index_groups=TEAMS, tiled=True
    )
    return join(back.reshape(LANGS, 4, ROWS, TOPK), slots)


def solution(mesh):
    placed = (P(AXES, None), P(AXES, None), P(AXES, None))
    return jax.shard_map(shards, mesh=mesh, in_specs=placed, out_specs=P(AXES, None), check_vma=False)
```

```python
import functools

import jax
import jax.numpy as jnp
from jax import lax
from jax.experimental import pallas as pl
from jax.experimental.pallas import tpu as pltpu
from jax.sharding import PartitionSpec as P

TOPK = 128
LANGS = 16
CAP = 20
ROWS = 24
MAIN = 16
TAIL = CAP - MAIN
Q = 128
WIDTH = 768

epsilon = 1e-06


def batcher(n):
    pairs = []
    p = 1
    while p < n:
        k = p
        while k >= 1:
            for j in range(k % p, n - k, 2 * k):
                for i in range(min(k, n - j - k)):
                    if (i + j) // (2 * p) == (i + j + k) // (2 * p):
                        pairs.append((i + j, i + j + k))
            k //= 2
        p *= 2
    return pairs


SORT32 = batcher(32)
SORT16 = batcher(16)


def wire(ref, base, i):
    return ref[pl.ds(pl.multiple_of((base + i) * 8, 8), 8), :]


def put(ref, base, i, value):
    ref[pl.ds(pl.multiple_of((base + i) * 8, 8), 8), :] = value


def sort32(ref, base):
    v = [wire(ref, base, i) for i in range(32)]
    for i, j in SORT32:
        v[i], v[j] = jnp.maximum(v[i], v[j]), jnp.minimum(v[i], v[j])
    for i in range(32):
        put(ref, base, i, v[i])


def clean(v):
    n = len(v)
    step = n // 2
    while step:
        for i in range(n):
            if not i & step:
                v[i], v[i + step] = jnp.maximum(v[i], v[i + step]), jnp.minimum(v[i], v[i + step])
        step //= 2
    return v


def clean_at(ref, base):
    v = clean([wire(ref, base, i) for i in range(32)])
    for i in range(32):
        put(ref, base, i, v[i])


def merge64(src, base, dst):
    for op, at in ((jnp.maximum, 0), (jnp.minimum, 32)):
        v = clean([op(wire(src, base, i), wire(src, base, 63 - i)) for i in range(32)])
        for i in range(32):
            put(dst, base + at, i, v[i])


def merge128(src, base, dst):
    for op, at in ((jnp.maximum, 0), (jnp.minimum, 64)):
        v = []
        for i in range(32):
            a = op(wire(src, base, i), wire(src, base, 127 - i))
            b = op(wire(src, base, i + 32), wire(src, base, 95 - i))
            v.append(jnp.maximum(a, b))
            put(dst, base + at + 32, i, jnp.minimum(a, b))
        v = clean(v)
        for i in range(32):
            put(dst, base + at, i, v[i])
        clean_at(dst, base + at + 32)


def merge_top(a, a_base, b, b_base, dst, dst_base, turn=0):
    def other(i):
        value = wire(b, b_base, 127 - i)
        return pltpu.roll(value, turn, 0) if turn else value

    v = []
    for i in range(32):
        c = [jnp.maximum(wire(a, a_base, i + 32 * k), other(i + 32 * k)) for k in range(4)]
        f0, g0 = jnp.maximum(c[0], c[2]), jnp.minimum(c[0], c[2])
        f1, g1 = jnp.maximum(c[1], c[3]), jnp.minimum(c[1], c[3])
        v.append(jnp.maximum(f0, f1))
        put(dst, dst_base + 32, i, jnp.minimum(f0, f1))
        put(dst, dst_base + 64, i, jnp.maximum(g0, g1))
        put(dst, dst_base + 96, i, jnp.minimum(g0, g1))
    v = clean(v)
    for i in range(32):
        put(dst, dst_base, i, v[i])

    def rest(k, carry):
        clean_at(dst, dst_base + 32 + 32 * k)
        return carry

    lax.fori_loop(0, 3, rest, 0)


def loop(n, body):
    def step(i, carry):
        body(i)
        return carry

    lax.fori_loop(0, n, step, 0)


def quarter_scores(corpus, rows, s, quarter):
    part = lax.dot_general(
        corpus[quarter * 256 : (quarter + 1) * 256, :],
        rows,
        (((1,), (1,)), ((), ())),
        preferred_element_type=jnp.float32,
    )
    for half in range(2):
        s[pl.ds(quarter * 2 + half, 256, stride=8), :] = part[:, half * 128 : (half + 1) * 128]


def score(corpus, rows, s):
    for quarter in range(4):
        quarter_scores(corpus, rows, s, quarter)


def order(s, u, dst):
    loop(8, lambda i: sort32(s, i * 32))
    loop(4, lambda i: merge64(s, i * 64, u))
    loop(2, lambda i: merge128(u, i * 128, s))
    merge_top(s, 0, s, 128, dst, 0)


def network(v, pairs):
    for i, j in pairs:
        v[i], v[j] = jnp.maximum(v[i], v[j]), jnp.minimum(v[i], v[j])
    return v


def best16(ref, base):
    a = network([wire(ref, base, i) for i in range(16)], SORT16)
    b = network([wire(ref, base, i) for i in range(16, 32)], SORT16)
    return clean([jnp.maximum(a[i], b[15 - i]) for i in range(16)])


def shorten(src, base, dst, dst_base):
    a = best16(src, base)
    b = best16(src, base + 32)
    peak = jnp.maximum(a[15], b[15])
    high = clean([jnp.maximum(a[i], b[15 - i]) for i in range(16)])
    low = clean([jnp.minimum(a[i], b[15 - i]) for i in range(16)])
    for i in range(16):
        put(dst, dst_base, i, high[i])
        put(dst, dst_base, 16 + i, low[i])
    return peak


def best32(src, base, dst, dst_base):
    v = clean([jnp.maximum(wire(src, base, i), wire(src, base, 63 - i)) for i in range(32)])
    for i in range(32):
        put(dst, dst_base, i, v[i])
    return v[31]


def best64(src, dst):
    v = []
    for i in range(32):
        a = jnp.maximum(wire(src, 0, i), wire(src, 0, 127 - i))
        b = jnp.maximum(wire(src, 0, i + 32), wire(src, 0, 95 - i))
        v.append(jnp.maximum(a, b))
        put(dst, 32, i, jnp.minimum(a, b))
    v = clean(v)
    for i in range(32):
        put(dst, 0, i, v[i])
    clean_at(dst, 32)
    return wire(dst, 63, 0)


def merge_turned(src, dst, turn):
    for op, at in ((jnp.maximum, 0), (jnp.minimum, 64)):
        v = []
        for i in range(32):
            a = op(wire(src, 0, i), pltpu.roll(wire(src, 0, 63 - i), turn, 0))
            b = op(wire(src, 0, i + 32), pltpu.roll(wire(src, 0, 31 - i), turn, 0))
            v.append(jnp.maximum(a, b))
            put(dst, at + 32, i, jnp.minimum(a, b))
        v = clean(v)
        for i in range(32):
            put(dst, at, i, v[i])
        clean_at(dst, at + 32)


def leaders(groups, own, far, s, s2, u, w, emit):
    units = [(g, corpus) for g in range(len(groups)) for corpus in (own, far)]
    buffers = (s, s2)
    score(own, groups[0](), s)
    peak = None
    for k, (g, _) in enumerate(units):
        here = buffers[k % 2]
        ahead = units[k + 1] if k + 1 < len(units) else None
        ahead_rows = groups[ahead[0]]() if ahead else None
        base = (k % 2) * 128
        for i in range(4):
            if ahead:
                quarter_scores(ahead[1], ahead_rows, buffers[(k + 1) % 2], i)
            now = shorten(here, i * 64, u, base + i * 32)
            peak = now if peak is None else jnp.maximum(peak, now)
        if k % 2 == 0:
            continue
        for i in range(4):
            peak = jnp.maximum(peak, best32(u, i * 64, w, i * 32))
        loop(2, lambda i: merge64(w, i * 64, u))
        peak = jnp.maximum(peak, best64(u, w))
        merge_turned(w, u, 4)
        merge_top(u, 0, u, 0, w, 0, turn=2)
        peak = jnp.maximum(peak, pltpu.roll(peak, 4, 0))
        peak = jnp.maximum(peak, pltpu.roll(peak, 2, 0))
        unsure = jnp.max(jnp.where(peak > wire(w, 127, 0), 1.0, 0.0)) > 0.0
        peak = None

        @pl.when(unsure)
        def _():
            long_way(groups[g](), own, far, s2, u, w)

        for half in range(2):
            emit(g, half, w[pl.ds(half, TOPK, stride=8), :].T)


def long_way(rows, own, far, s, u, w):
    score(own, rows, s)
    order(s, u, w)
    score(far, rows, s)
    order(s, u, u)
    merge_top(w, 0, u, 0, s, 0)
    merge_top(s, 0, s, 0, u, 0, turn=4)
    merge_top(u, 0, u, 0, w, 0, turn=2)


def main_rows(chunk):
    return chunk[:, 0:MAIN, :].reshape(-1, WIDTH)


def first_kernel(chunk, own, far, out, both, rows, *work):
    rows[...] = main_rows(chunk)
    both[0] = own[...]
    both[1] = far[...]

    def emit(g, half, value):
        out[half * Q : (half + 1) * Q, :] = value

    leaders([lambda: rows[...]], own, far, *work, emit)


def early_kernel(half0, half1, both, out, rows, *work):
    rows[0:128, :] = main_rows(half0)
    rows[128:256, :] = main_rows(half1)

    def emit(g, half, value):
        out[half * Q : (half + 1) * Q, :] = value

    leaders([lambda: rows[...]], both.at[0], both.at[1], *work, emit)


STEPS = 800.0
FLOOR = 32.5
LN2 = 0.6931471805599453


def coded(v):
    level = jnp.round(jnp.log(jnp.abs(v)) * (STEPS / LN2) + STEPS * FLOOR)
    level = jnp.clip(level, 0.0, 32767.0)
    return jnp.where(v < 0, -level, level)


def decoded(c):
    level = jnp.abs(c)
    v = jnp.where(level > 0, jnp.exp(level * (LN2 / STEPS) - FLOOR * LN2), 0.0)
    return jnp.where(c < 0, -v, v)


def late_kernel(at, mine, cx0, cx1, cy0, cy1, cd0, cd1, both, r0, r1, r2, out, *scratch):
    rows, tails, box, *work = scratch
    rows[0:128, :] = main_rows(cd0)
    rows[128:256, :] = main_rows(cd1)
    slot = lax.broadcasted_iota(jnp.int32, (64, LANGS * ROWS), 1)
    row = lax.broadcasted_iota(jnp.int32, (64, LANGS * ROWS), 0)
    picks = (slot == row // TAIL * ROWS + MAIN + row % TAIL).astype(jnp.float32).astype(jnp.bfloat16)
    half_picks = picks[0:32, 0 : 8 * ROWS]

    def tail_of(chunk, sel):
        flat = chunk[...].reshape(-1, WIDTH)
        return jnp.dot(sel, flat, preferred_element_type=jnp.float32).astype(jnp.bfloat16)

    rows[256:320, :] = tail_of(mine, picks)
    for k, chunk in enumerate((cx0, cx1, cy0, cy1, cd0, cd1)):
        rows[320 + k * 32 : 352 + k * 32, :] = tail_of(chunk, half_picks)

    def emit(g, half, value):
        tails[g, half] = value

    leaders(
        [lambda: rows[0:256, :], lambda: rows[256:512, :]], both.at[0], both.at[1], *work, emit
    )
    me = at[0]
    owner = (me, me ^ 1, me ^ 2, me ^ 3)
    none = jnp.zeros((ROWS - CAP, TOPK), jnp.float32)
    for k in range(4):
        for lang in range(LANGS):
            half, start = lang // 8, lang % 8 * MAIN
            if k == 0:
                main = r0[lang * MAIN : (lang + 1) * MAIN, :]
            elif k < 3:
                start += (k - 1) * Q
                main = (r1, r2)[half][start : start + MAIN, :]
            else:
                main = tails[0, half, start : start + MAIN, :]
            box[k, 0:MAIN, :] = main
            start = k % 2 * 64 + lang * TAIL
            box[k, MAIN:CAP, :] = tails[1, k // 2, start : start + TAIL, :]
            box[k, CAP:ROWS, :] = none
            out[lang, owner[k]] = coded(box[k]).astype(jnp.int32).astype(jnp.int16)


COST = 2 * 256 * 2048 * 768 * 8
VMEM = pl.BlockSpec(memory_space=pltpu.VMEM)
LIMIT = pltpu.CompilerParams(vmem_limit_bytes=14 << 20)
WORK = [
    pltpu.VMEM((256 * 8, 128), jnp.float32),
    pltpu.VMEM((256 * 8, 128), jnp.float32),
    pltpu.VMEM((256 * 8, 128), jnp.float32),
    pltpu.VMEM((128 * 8, 128), jnp.float32),
]


def first(chunk, own, far):
    return pl.pallas_call(
        first_kernel,
        out_shape=(
            jax.ShapeDtypeStruct((256, TOPK), jnp.float32),
            jax.ShapeDtypeStruct((2, 1024, WIDTH), jnp.bfloat16),
        ),
        in_specs=[VMEM] * 3,
        out_specs=(VMEM, VMEM),
        scratch_shapes=[pltpu.VMEM((256, WIDTH), jnp.bfloat16)] + WORK,
        compiler_params=LIMIT,
        cost_estimate=pl.CostEstimate(flops=COST, bytes_accessed=1 << 20, transcendentals=0),
        name="first",
    )(chunk, own, far)


def early(half0, half1, both):
    return pl.pallas_call(
        early_kernel,
        out_shape=jax.ShapeDtypeStruct((256, TOPK), jnp.float32),
        in_specs=[VMEM] * 3,
        out_specs=VMEM,
        scratch_shapes=[pltpu.VMEM((256, WIDTH), jnp.bfloat16)] + WORK,
        compiler_params=LIMIT,
        cost_estimate=pl.CostEstimate(flops=COST, bytes_accessed=1 << 20, transcendentals=0),
        name="early",
    )(half0, half1, both)


def late(at, chunks, both, results):
    return pl.pallas_call(
        late_kernel,
        out_shape=jax.ShapeDtypeStruct((LANGS, 4, ROWS, TOPK), jnp.int16),
        in_specs=[pl.BlockSpec(memory_space=pltpu.SMEM)] + [VMEM] * 11,
        out_specs=VMEM,
        scratch_shapes=[
            pltpu.VMEM((512, WIDTH), jnp.bfloat16),
            pltpu.VMEM((2, 2, Q, TOPK), jnp.float32),
            pltpu.VMEM((4, ROWS, TOPK), jnp.float32),
        ]
        + WORK,
        compiler_params=LIMIT,
        cost_estimate=pl.CostEstimate(flops=COST * 2, bytes_accessed=1 << 20, transcendentals=0),
        name="late",
    )(at, *chunks, both, *results)


def outbox_kernel(queries_in, routes_in, out, slots, queries, routes, sems):
    copies = (
        pltpu.make_async_copy(routes_in, routes, sems.at[0]),
        pltpu.make_async_copy(queries_in, queries, sems.at[1]),
    )
    for copy in copies:
        copy.start()
    for copy in copies:
        copy.wait()
    x = queries[...].astype(jnp.float32)
    unit = (x * lax.rsqrt(jnp.mean(x * x, axis=1, keepdims=True) + epsilon)).astype(jnp.bfloat16)
    along = jnp.broadcast_to(routes[...].astype(jnp.float32), (Q, Q))
    down = along.T
    before = lax.broadcasted_iota(jnp.int32, (Q, Q), 0) < lax.broadcasted_iota(jnp.int32, (Q, Q), 1)
    earlier = jnp.where(before & (along == down), 1.0, 0.0)
    rank = jnp.sum(earlier, axis=0, keepdims=True)
    place = routes[...] * ROWS + rank.astype(jnp.int32)
    slots[...] = place
    total = LANGS * ROWS
    hits = lax.broadcasted_iota(jnp.int32, (total, Q), 0) == jnp.broadcast_to(place, (total, Q))
    picks = jnp.where(hits, 1.0, 0.0).astype(jnp.bfloat16)
    box = jnp.dot(picks, unit, preferred_element_type=jnp.float32).astype(jnp.bfloat16)
    out[...] = box.reshape(LANGS, ROWS, WIDTH)


def outbox_of(queries, routes):
    return pl.pallas_call(
        outbox_kernel,
        out_shape=(
            jax.ShapeDtypeStruct((LANGS, ROWS, WIDTH), jnp.bfloat16),
            jax.ShapeDtypeStruct((1, Q), jnp.int32),
        ),
        in_specs=[pl.BlockSpec(memory_space=pltpu.HBM)] * 2,
        out_specs=(VMEM, VMEM),
        scratch_shapes=[
            pltpu.VMEM((Q, WIDTH), jnp.bfloat16),
            pltpu.VMEM((1, Q), jnp.int32),
            pltpu.SemaphoreType.DMA((2,)),
        ],
        compiler_params=LIMIT,
        name="outbox",
    )(queries, routes)


def join_kernel(back, slots, out, a, b):
    total = LANGS * ROWS
    hits = lax.broadcasted_iota(jnp.int32, (total, Q), 0) == jnp.broadcast_to(slots[...], (total, Q))
    picks = jnp.where(hits, 1.0, 0.0)
    picks = jnp.concatenate([picks[i * Q : (i + 1) * Q, :].T for i in range(total // Q)], axis=1)
    picks = picks.astype(jnp.bfloat16)
    for k in range(4):
        code = back[:, k].astype(jnp.int32).astype(jnp.float32).reshape(total, TOPK)
        high = code.astype(jnp.bfloat16)
        low = (code - high.astype(jnp.float32)).astype(jnp.bfloat16)
        rows = jnp.dot(picks, high, preferred_element_type=jnp.float32) + jnp.dot(
            picks, low, preferred_element_type=jnp.float32
        )
        ranks = decoded(rows).T
        a[pl.ds(k, TOPK, stride=8), :] = ranks
        a[pl.ds(k + 4, TOPK, stride=8), :] = ranks
    merge_top(a, 0, a, 0, b, 0, turn=2)
    merge_top(b, 0, b, 0, a, 0, turn=1)
    out[...] = a[pl.ds(0, TOPK, stride=8), :].T


def join(back, slots):
    return pl.pallas_call(
        join_kernel,
        out_shape=jax.ShapeDtypeStruct((Q, TOPK), jnp.float32),
        in_specs=[VMEM] * 2,
        out_specs=VMEM,
        scratch_shapes=[pltpu.VMEM((128 * 8, 128), jnp.float32)] * 2,
        compiler_params=LIMIT,
        name="join",
    )(back, slots)


AXES = ("lang", "shard")


def moves(target):
    return [
        (lang * 8 + y * 4 + x, lang * 8 + ty * 4 + tx % 4)
        for lang in range(16)
        for y in range(2)
        for x in range(4)
        for ty, tx in (target(lang % 2, y, x),)
    ]


def pair(core, y, x):
    return y, x + (1 if (x + core) % 2 == 0 else -1)


def over_x(core, y, x):
    return y, x + 2


def over_y(core, y, x):
    return 1 - y, x


TEAMS = [
    [lang * 8 + y * 4 + odd + 2 * half for lang in range(16) for y in range(2) for half in range(2)]
    for odd in range(2)
]


def shards(queries, routes, corpus):
    far = lax.ppermute(corpus, AXES, moves(pair))
    outbox, slots = outbox_of(queries, routes.reshape(1, Q))
    mine = lax.all_to_all(outbox, "lang", split_axis=0, concat_axis=0, tiled=True)
    cx0, cy0, cx1, cy1 = (
        lax.ppermute(part, AXES, moves(over)) for part in (mine[:8], mine[8:]) for over in (over_x, over_y)
    )
    r0, both = first(mine, corpus, far)
    cx0, cy0, r0 = lax.optimization_barrier((cx0, cy0, r0))
    cd0 = lax.ppermute(cx0, AXES, moves(over_y))
    r1 = early(cx0, cy0, both)
    cx1, cy1, r1 = lax.optimization_barrier((cx1, cy1, r1))
    cd1 = lax.ppermute(cy1, AXES, moves(over_x))
    r2 = early(cx1, cy1, both)
    shard = lax.axis_index("shard")
    at = (lax.shift_right_logical(shard, 2) * 2 + (lax.shift_right_logical(shard, 1) & 1)).reshape(1)
    found = late(at, (mine, cx0, cx1, cy0, cy1, cd0, cd1), both, (r0, r1, r2))
    back = lax.all_to_all(
        found.reshape(LANGS * 4, ROWS, TOPK), AXES, 0, 0, axis_index_groups=TEAMS, tiled=True
    )
    return join(back.reshape(LANGS, 4, ROWS, TOPK), slots)


def solution(mesh):
    placed = (P(AXES, None), P(AXES, None), P(AXES, None))
    return jax.shard_map(shards, mesh=mesh, in_specs=placed, out_specs=P(AXES, None), check_vma=False)
```

```python
import functools

import jax
import jax.numpy as jnp
from jax import lax
from jax.experimental import pallas as pl
from jax.experimental.pallas import tpu as pltpu
from jax.sharding import PartitionSpec as P

TOPK = 128
LANGS = 16
CAP = 20
ROWS = 24
MAIN = 16
TAIL = CAP - MAIN
Q = 128
WIDTH = 768
COLS = WIDTH // 128
SENT = CAP * COLS

epsilon = 1e-06


def batcher(n):
    pairs = []
    p = 1
    while p < n:
        k = p
        while k >= 1:
            for j in range(k % p, n - k, 2 * k):
                for i in range(min(k, n - j - k)):
                    if (i + j) // (2 * p) == (i + j + k) // (2 * p):
                        pairs.append((i + j, i + j + k))
            k //= 2
        p *= 2
    return pairs


SORT32 = batcher(32)
SORT16 = batcher(16)


def wire(ref, base, i):
    return ref[pl.ds(pl.multiple_of((base + i) * 8, 8), 8), :]


def put(ref, base, i, value):
    ref[pl.ds(pl.multiple_of((base + i) * 8, 8), 8), :] = value


def sort32(ref, base):
    v = [wire(ref, base, i) for i in range(32)]
    for i, j in SORT32:
        v[i], v[j] = jnp.maximum(v[i], v[j]), jnp.minimum(v[i], v[j])
    for i in range(32):
        put(ref, base, i, v[i])


def clean(v):
    n = len(v)
    step = n // 2
    while step:
        for i in range(n):
            if not i & step:
                v[i], v[i + step] = jnp.maximum(v[i], v[i + step]), jnp.minimum(v[i], v[i + step])
        step //= 2
    return v


def clean_at(ref, base):
    v = clean([wire(ref, base, i) for i in range(32)])
    for i in range(32):
        put(ref, base, i, v[i])


def merge64(src, base, dst):
    for op, at in ((jnp.maximum, 0), (jnp.minimum, 32)):
        v = clean([op(wire(src, base, i), wire(src, base, 63 - i)) for i in range(32)])
        for i in range(32):
            put(dst, base + at, i, v[i])


def merge128(src, base, dst):
    for op, at in ((jnp.maximum, 0), (jnp.minimum, 64)):
        v = []
        for i in range(32):
            a = op(wire(src, base, i), wire(src, base, 127 - i))
            b = op(wire(src, base, i + 32), wire(src, base, 95 - i))
            v.append(jnp.maximum(a, b))
            put(dst, base + at + 32, i, jnp.minimum(a, b))
        v = clean(v)
        for i in range(32):
            put(dst, base + at, i, v[i])
        clean_at(dst, base + at + 32)


def merge_top(a, a_base, b, b_base, dst, dst_base, turn=0):
    def other(i):
        value = wire(b, b_base, 127 - i)
        return pltpu.roll(value, turn, 0) if turn else value

    v = []
    for i in range(32):
        c = [jnp.maximum(wire(a, a_base, i + 32 * k), other(i + 32 * k)) for k in range(4)]
        f0, g0 = jnp.maximum(c[0], c[2]), jnp.minimum(c[0], c[2])
        f1, g1 = jnp.maximum(c[1], c[3]), jnp.minimum(c[1], c[3])
        v.append(jnp.maximum(f0, f1))
        put(dst, dst_base + 32, i, jnp.minimum(f0, f1))
        put(dst, dst_base + 64, i, jnp.maximum(g0, g1))
        put(dst, dst_base + 96, i, jnp.minimum(g0, g1))
    v = clean(v)
    for i in range(32):
        put(dst, dst_base, i, v[i])

    def rest(k, carry):
        clean_at(dst, dst_base + 32 + 32 * k)
        return carry

    lax.fori_loop(0, 3, rest, 0)


def loop(n, body):
    def step(i, carry):
        body(i)
        return carry

    lax.fori_loop(0, n, step, 0)


def quarter_scores(corpus, rows, s, quarter):
    part = lax.dot_general(
        corpus[quarter * 256 : (quarter + 1) * 256, :],
        rows,
        (((1,), (1,)), ((), ())),
        preferred_element_type=jnp.float32,
    )
    if rows.shape[0] == 256:
        for half in range(2):
            s[pl.ds(quarter * 2 + half, 256, stride=8), :] = part[:, half * 128 : (half + 1) * 128]
    else:
        for half in range(2):
            s[pl.ds(quarter * 2 + half, 128, stride=8), :] = part[half * 128 : (half + 1) * 128, :]


def score(corpus, rows, s):
    for quarter in range(4):
        quarter_scores(corpus, rows, s, quarter)


def order(blocks, s, u, dst):
    loop(4 * blocks, lambda i: sort32(s, i * 32))
    loop(2 * blocks, lambda i: merge64(s, i * 64, u))
    if blocks == 1:
        merge128(u, 0, dst)
    else:
        loop(2, lambda i: merge128(u, i * 128, s))
        merge_top(s, 0, s, 128, dst, 0)


def network(v, pairs):
    for i, j in pairs:
        v[i], v[j] = jnp.maximum(v[i], v[j]), jnp.minimum(v[i], v[j])
    return v


def best16(ref, base):
    a = network([wire(ref, base, i) for i in range(16)], SORT16)
    b = network([wire(ref, base, i) for i in range(16, 32)], SORT16)
    return clean([jnp.maximum(a[i], b[15 - i]) for i in range(16)])


def shorten(src, base, dst, dst_base):
    a = best16(src, base)
    b = best16(src, base + 32)
    peak = jnp.maximum(a[15], b[15])
    high = clean([jnp.maximum(a[i], b[15 - i]) for i in range(16)])
    low = clean([jnp.minimum(a[i], b[15 - i]) for i in range(16)])
    for i in range(16):
        put(dst, dst_base, i, high[i])
        put(dst, dst_base, 16 + i, low[i])
    return peak


def best32(src, base, dst, dst_base):
    v = clean([jnp.maximum(wire(src, base, i), wire(src, base, 63 - i)) for i in range(32)])
    for i in range(32):
        put(dst, dst_base, i, v[i])
    return v[31]


def best64(src, dst, turn=0):
    def other(i):
        return pltpu.roll(wire(src, 0, 63 - i), turn, 0) if turn else wire(src, 0, 127 - i)

    v = []
    for i in range(32):
        a = jnp.maximum(wire(src, 0, i), other(i))
        b = jnp.maximum(wire(src, 0, i + 32), other(i + 32))
        v.append(jnp.maximum(a, b))
        put(dst, 32, i, jnp.minimum(a, b))
    v = clean(v)
    for i in range(32):
        put(dst, 0, i, v[i])
    clean_at(dst, 32)
    return wire(dst, 63, 0)


def merge_turned(src, dst, turn):
    for op, at in ((jnp.maximum, 0), (jnp.minimum, 64)):
        v = []
        for i in range(32):
            a = op(wire(src, 0, i), pltpu.roll(wire(src, 0, 63 - i), turn, 0))
            b = op(wire(src, 0, i + 32), pltpu.roll(wire(src, 0, 31 - i), turn, 0))
            v.append(jnp.maximum(a, b))
            put(dst, at + 32, i, jnp.minimum(a, b))
        v = clean(v)
        for i in range(32):
            put(dst, at, i, v[i])
        clean_at(dst, at + 32)


def leaders(groups, own, far, s, s2, u, w, emit):
    units = [(g, corpus) for g in range(len(groups)) for corpus in (own, far)]
    buffers = (s, s2)
    score(own, groups[0][1](), s)
    peak = None
    for k, (g, _) in enumerate(units):
        blocks = groups[g][0]
        here = buffers[k % 2]
        ahead = units[k + 1] if k + 1 < len(units) else None
        ahead_rows = groups[ahead[0]][1]() if ahead else None
        base = (k % 2) * 64 * blocks
        for i in range(4):
            if ahead:
                quarter_scores(ahead[1], ahead_rows, buffers[(k + 1) % 2], i)
            if i < 2 * blocks:
                now = shorten(here, i * 64, u, base + i * 32)
                peak = now if peak is None else jnp.maximum(peak, now)
        if k % 2 == 0:
            continue
        for i in range(2 * blocks):
            peak = jnp.maximum(peak, best32(u, i * 64, w, i * 32))
        if blocks == 2:
            loop(2, lambda i: merge64(w, i * 64, u))
            peak = jnp.maximum(peak, best64(u, w))
            turns = (4, 2)
        else:
            merge64(w, 0, u)
            peak = jnp.maximum(peak, best64(u, w, turn=4))
            turns = (2, 1)
        merge_turned(w, u, turns[0])
        merge_top(u, 0, u, 0, w, 0, turn=turns[1])
        for turn in (4, 2, 1)[: 4 - blocks]:
            peak = jnp.maximum(peak, pltpu.roll(peak, turn, 0))
        unsure = jnp.max(jnp.where(peak > wire(w, 127, 0), 1.0, 0.0)) > 0.0
        peak = None

        @pl.when(unsure)
        def _():
            long_way(blocks, groups[g][1](), own, far, s if k + 1 == len(units) else s2, u, w)

        for half in range(blocks):
            emit(g, half, w[pl.ds(half, TOPK, stride=8), :].T)


def long_way(blocks, rows, own, far, s, u, w):
    score(own, rows, s)
    order(blocks, s, u, w)
    score(far, rows, s)
    if blocks == 2:
        order(blocks, s, u, u)
        merge_top(w, 0, u, 0, s, 0)
        merge_top(s, 0, s, 0, u, 0, turn=4)
        merge_top(u, 0, u, 0, w, 0, turn=2)
    else:
        loop(4, lambda i: sort32(s, i * 32))
        loop(2, lambda i: merge64(s, i * 64, u))
        merge128(u, 0, s)
        merge_top(w, 0, s, 0, u, 0)
        merge_top(u, 0, u, 0, s, 0, turn=4)
        merge_top(s, 0, s, 0, u, 0, turn=2)
        merge_top(u, 0, u, 0, w, 0, turn=1)


def main_rows(chunk):
    return jnp.concatenate(
        [chunk[:, c * MAIN : (c + 1) * MAIN, :].reshape(-1, 128) for c in range(COLS)], axis=1
    )


def tail_rows(chunk):
    langs = chunk.shape[0]
    many, each = langs * TAIL, TAIL * COLS
    shape, total = (COLS, many, langs * each), langs * each
    col, row, at = (lax.broadcasted_iota(jnp.int32, shape, d) for d in range(3))
    from_row = lax.shift_right_logical(row, 2) * each + col * TAIL + (row & 3)
    picks = jnp.where(at == from_row, 1.0, 0.0).astype(jnp.bfloat16).reshape(total, total)
    flat = chunk[:, MAIN * COLS : SENT, :].reshape(total, 128)
    found = jnp.dot(picks, flat, preferred_element_type=jnp.float32).astype(jnp.bfloat16)
    return jnp.concatenate([found[c * many : (c + 1) * many, :] for c in range(COLS)], axis=1)


def first_kernel(chunk, own, far, out, both, rows, *work):
    rows[...] = main_rows(chunk)
    both[0] = own[...]
    both[1] = far[...]

    def emit(g, half, value):
        out[half * Q : (half + 1) * Q, :] = value

    leaders([(2, lambda: rows[...])], own, far, *work, emit)


def early_kernel(half0, half1, both, out, rows, *work):
    rows[0:128, :] = main_rows(half0)
    rows[128:256, :] = main_rows(half1)

    def emit(g, half, value):
        out[half * Q : (half + 1) * Q, :] = value

    leaders([(2, lambda: rows[...])], both.at[0], both.at[1], *work, emit)


def middle_kernel(mine, cx0, cx1, cy0, cy1, both, out, tails, rows, *work):
    rows[0:128, :] = main_rows(cx1)
    rows[128:256, :] = main_rows(cy1)
    rows[256:320, :] = tail_rows(mine)
    for k, chunk in enumerate((cx0, cx1, cy0, cy1)):
        rows[320 + k * 32 : 352 + k * 32, :] = tail_rows(chunk)
    rows[448:512, :] = jnp.zeros((64, WIDTH), jnp.bfloat16)

    def emit(g, half, value):
        (out, tails)[g][half * Q : (half + 1) * Q, :] = value

    leaders(
        [(2, lambda: rows[0:256, :]), (2, lambda: rows[256:512, :])], both.at[0], both.at[1], *work, emit
    )


STEPS = 800.0
FLOOR = 32.5
LN2 = 0.6931471805599453


def coded(v):
    level = jnp.round(jnp.log(jnp.abs(v)) * (STEPS / LN2) + STEPS * FLOOR)
    level = jnp.clip(level, 0.0, 32767.0)
    return jnp.where(v < 0, -level, level)


def decoded(c):
    level = jnp.abs(c)
    v = jnp.where(level > 0, jnp.exp(level * (LN2 / STEPS) - FLOOR * LN2), 0.0)
    return jnp.where(c < 0, -v, v)


def late_kernel(at, cd0, cd1, both, r0, r1, r2, tails, out, rows, last, box, *work):
    rows[0:128, :] = main_rows(cd0)
    rows[128:256, :] = main_rows(cd1)
    rows[256:288, :] = tail_rows(cd0)
    rows[288:320, :] = tail_rows(cd1)
    rows[320:384, :] = jnp.zeros((64, WIDTH), jnp.bfloat16)

    def emit(g, half, value):
        last[g * 256 + half * Q : g * 256 + (half + 1) * Q, :] = value

    leaders(
        [(2, lambda: rows[0:256, :]), (1, lambda: rows[256:384, :])], both.at[0], both.at[1], *work, emit
    )
    me = at[0]
    owner = (me, me ^ 1, me ^ 2, me ^ 3)
    none = jnp.zeros((ROWS - CAP, TOPK), jnp.float32)
    for k in range(4):
        for lang in range(LANGS):
            half, start = lang // 8, lang % 8 * MAIN
            if k == 0:
                main = r0[lang * MAIN : (lang + 1) * MAIN, :]
            elif k < 3:
                start += (k - 1) * Q
                main = (r1, r2)[half][start : start + MAIN, :]
            else:
                main = last[lang * MAIN : (lang + 1) * MAIN, :]
            box[k, 0:MAIN, :] = main
            start = k * 64 + lang * TAIL
            if k < 3:
                box[k, MAIN:CAP, :] = tails[start : start + TAIL, :]
            else:
                box[k, MAIN:CAP, :] = last[256 + lang * TAIL : 256 + (lang + 1) * TAIL, :]
            box[k, CAP:ROWS, :] = none
            out[lang, owner[k]] = coded(box[k]).astype(jnp.int32).astype(jnp.int16)


COST = 2 * 256 * 2048 * 768 * 8
VMEM = pl.BlockSpec(memory_space=pltpu.VMEM)
LIMIT = pltpu.CompilerParams(vmem_limit_bytes=14 << 20)
WORK = [
    pltpu.VMEM((256 * 8, 128), jnp.float32),
    pltpu.VMEM((256 * 8, 128), jnp.float32),
    pltpu.VMEM((256 * 8, 128), jnp.float32),
    pltpu.VMEM((128 * 8, 128), jnp.float32),
]


def first(chunk, own, far):
    return pl.pallas_call(
        first_kernel,
        out_shape=(
            jax.ShapeDtypeStruct((256, TOPK), jnp.float32),
            jax.ShapeDtypeStruct((2, 1024, WIDTH), jnp.bfloat16),
        ),
        in_specs=[VMEM] * 3,
        out_specs=(VMEM, VMEM),
        scratch_shapes=[pltpu.VMEM((256, WIDTH), jnp.bfloat16)] + WORK,
        compiler_params=LIMIT,
        cost_estimate=pl.CostEstimate(flops=COST, bytes_accessed=1 << 20, transcendentals=0),
        name="first",
    )(chunk, own, far)


def early(half0, half1, both):
    return pl.pallas_call(
        early_kernel,
        out_shape=jax.ShapeDtypeStruct((256, TOPK), jnp.float32),
        in_specs=[VMEM] * 3,
        out_specs=VMEM,
        scratch_shapes=[pltpu.VMEM((256, WIDTH), jnp.bfloat16)] + WORK,
        compiler_params=LIMIT,
        cost_estimate=pl.CostEstimate(flops=COST, bytes_accessed=1 << 20, transcendentals=0),
        name="early",
    )(half0, half1, both)


def middle(mine, halves, both):
    return pl.pallas_call(
        middle_kernel,
        out_shape=[jax.ShapeDtypeStruct((256, TOPK), jnp.float32)] * 2,
        in_specs=[VMEM] * 6,
        out_specs=[VMEM] * 2,
        scratch_shapes=[pltpu.VMEM((512, WIDTH), jnp.bfloat16)] + WORK,
        compiler_params=LIMIT,
        cost_estimate=pl.CostEstimate(flops=COST * 2, bytes_accessed=1 << 20, transcendentals=0),
        name="middle",
    )(mine, *halves, both)


def late(at, halves, both, results):
    return pl.pallas_call(
        late_kernel,
        out_shape=jax.ShapeDtypeStruct((LANGS, 4, ROWS, TOPK), jnp.int16),
        in_specs=[pl.BlockSpec(memory_space=pltpu.SMEM)] + [VMEM] * 7,
        out_specs=VMEM,
        scratch_shapes=[
            pltpu.VMEM((384, WIDTH), jnp.bfloat16),
            pltpu.VMEM((384, TOPK), jnp.float32),
            pltpu.VMEM((4, ROWS, TOPK), jnp.float32),
        ]
        + WORK,
        compiler_params=LIMIT,
        cost_estimate=pl.CostEstimate(flops=COST * 2, bytes_accessed=1 << 20, transcendentals=0),
        name="late",
    )(at, *halves, both, *results)


def outbox_kernel(queries_in, routes_in, out, slots, queries, routes, sems):
    copies = (
        pltpu.make_async_copy(routes_in, routes, sems.at[0]),
        pltpu.make_async_copy(queries_in, queries, sems.at[1]),
    )
    for copy in copies:
        copy.start()
    for copy in copies:
        copy.wait()
    x = queries[...].astype(jnp.float32)
    unit = (x * lax.rsqrt(jnp.mean(x * x, axis=1, keepdims=True) + epsilon)).astype(jnp.bfloat16)
    along = jnp.broadcast_to(routes[...].astype(jnp.float32), (Q, Q))
    down = along.T
    before = lax.broadcasted_iota(jnp.int32, (Q, Q), 0) < lax.broadcasted_iota(jnp.int32, (Q, Q), 1)
    earlier = jnp.where(before & (along == down), 1.0, 0.0)
    rank = jnp.sum(earlier, axis=0, keepdims=True).astype(jnp.int32)
    lang = routes[...]
    slots[...] = lang * ROWS + rank
    main_at = jnp.where(rank < MAIN, lang * MAIN + rank, -1)
    hits = lax.broadcasted_iota(jnp.int32, (LANGS * MAIN, Q), 0) == jnp.broadcast_to(main_at, (LANGS * MAIN, Q))
    picks = jnp.where(hits, 1.0, 0.0).astype(jnp.bfloat16)
    box = jnp.dot(picks, unit, preferred_element_type=jnp.float32).astype(jnp.bfloat16)
    for c in range(COLS):
        out[:, c * MAIN : (c + 1) * MAIN, :] = box[:, c * 128 : (c + 1) * 128].reshape(LANGS, MAIN, 128)
    each = TAIL * COLS
    tail_at = jnp.where(rank < MAIN, -1, lang * TAIL + rank - MAIN)
    shape = (LANGS, each, Q)
    of_lang, row = (lax.broadcasted_iota(jnp.int32, shape, d) for d in range(2))
    hits = of_lang * TAIL + (row & 3) == jnp.broadcast_to(tail_at.reshape(1, 1, Q), shape)
    tail = jnp.zeros((LANGS * each, 128), jnp.float32)
    for c in range(COLS):
        picks = jnp.where(hits & (lax.shift_right_logical(row, 2) == c), 1.0, 0.0)
        picks = picks.astype(jnp.bfloat16).reshape(LANGS * each, Q)
        tail = tail + jnp.dot(picks, unit[:, c * 128 : (c + 1) * 128], preferred_element_type=jnp.float32)
    out[:, MAIN * COLS : SENT, :] = tail.astype(jnp.bfloat16).reshape(LANGS, each, 128)


def outbox_of(queries, routes):
    return pl.pallas_call(
        outbox_kernel,
        out_shape=(
            jax.ShapeDtypeStruct((LANGS, SENT, 128), jnp.bfloat16),
            jax.ShapeDtypeStruct((1, Q), jnp.int32),
        ),
        in_specs=[pl.BlockSpec(memory_space=pltpu.HBM)] * 2,
        out_specs=(VMEM, VMEM),
        scratch_shapes=[
            pltpu.VMEM((Q, WIDTH), jnp.bfloat16),
            pltpu.VMEM((1, Q), jnp.int32),
            pltpu.SemaphoreType.DMA((2,)),
        ],
        compiler_params=LIMIT,
        name="outbox",
    )(queries, routes)


def join_kernel(back, slots, out, a, b):
    total = LANGS * ROWS
    hits = lax.broadcasted_iota(jnp.int32, (total, Q), 0) == jnp.broadcast_to(slots[...], (total, Q))
    picks = jnp.where(hits, 1.0, 0.0)
    picks = jnp.concatenate([picks[i * Q : (i + 1) * Q, :].T for i in range(total // Q)], axis=1)
    picks = picks.astype(jnp.bfloat16)
    for k in range(4):
        code = back[:, k].astype(jnp.int32).astype(jnp.float32).reshape(total, TOPK)
        high = code.astype(jnp.bfloat16)
        low = (code - high.astype(jnp.float32)).astype(jnp.bfloat16)
        rows = jnp.dot(picks, high, preferred_element_type=jnp.float32) + jnp.dot(
            picks, low, preferred_element_type=jnp.float32
        )
        ranks = decoded(rows).T
        a[pl.ds(k, TOPK, stride=8), :] = ranks
        a[pl.ds(k + 4, TOPK, stride=8), :] = ranks
    merge_top(a, 0, a, 0, b, 0, turn=2)
    merge_top(b, 0, b, 0, a, 0, turn=1)
    out[...] = a[pl.ds(0, TOPK, stride=8), :].T


def join(back, slots):
    return pl.pallas_call(
        join_kernel,
        out_shape=jax.ShapeDtypeStruct((Q, TOPK), jnp.float32),
        in_specs=[VMEM] * 2,
        out_specs=VMEM,
        scratch_shapes=[pltpu.VMEM((128 * 8, 128), jnp.float32)] * 2,
        compiler_params=LIMIT,
        name="join",
    )(back, slots)


AXES = ("lang", "shard")


def moves(target):
    return [
        (lang * 8 + y * 4 + x, lang * 8 + ty * 4 + tx % 4)
        for lang in range(16)
        for y in range(2)
        for x in range(4)
        for ty, tx in (target(lang % 2, y, x),)
    ]


def pair(core, y, x):
    return y, x + (1 if (x + core) % 2 == 0 else -1)


def over_x(core, y, x):
    return y, x + 2


def over_y(core, y, x):
    return 1 - y, x


TEAMS = [
    [lang * 8 + y * 4 + odd + 2 * half for lang in range(16) for y in range(2) for half in range(2)]
    for odd in range(2)
]


def shards(queries, routes, corpus):
    far = lax.ppermute(corpus, AXES, moves(pair))
    outbox, slots = outbox_of(queries, routes.reshape(1, Q))
    mine = lax.all_to_all(outbox, "lang", split_axis=0, concat_axis=0, tiled=True)
    cx0, cy0, cx1, cy1 = (
        lax.ppermute(part, AXES, moves(over)) for part in (mine[:8], mine[8:]) for over in (over_x, over_y)
    )
    r0, both = first(mine, corpus, far)
    cx0, cy0, r0 = lax.optimization_barrier((cx0, cy0, r0))
    cd0 = lax.ppermute(cx0, AXES, moves(over_y))
    r1 = early(cx0, cy0, both)
    cx1, cy1, r1 = lax.optimization_barrier((cx1, cy1, r1))
    cd1 = lax.ppermute(cy1, AXES, moves(over_x))
    r2, tails = middle(mine, (cx0, cx1, cy0, cy1), both)
    shard = lax.axis_index("shard")
    at = (lax.shift_right_logical(shard, 2) * 2 + (lax.shift_right_logical(shard, 1) & 1)).reshape(1)
    found = late(at, (cd0, cd1), both, (r0, r1, r2, tails))
    back = lax.all_to_all(
        found.reshape(LANGS * 4, ROWS, TOPK), AXES, 0, 0, axis_index_groups=TEAMS, tiled=True
    )
    return join(back.reshape(LANGS, 4, ROWS, TOPK), slots)


def solution(mesh):
    placed = (P(AXES, None), P(AXES, None), P(AXES, None))
    return jax.shard_map(shards, mesh=mesh, in_specs=placed, out_specs=P(AXES, None), check_vma=False)
```

```python
import functools

import jax
import jax.numpy as jnp
from jax import lax
from jax.experimental import pallas as pl
from jax.experimental.pallas import tpu as pltpu
from jax.sharding import PartitionSpec as P

TOPK = 128
LANGS = 16
CAP = 20
ROWS = 24
MAIN = 16
TAIL = CAP - MAIN
Q = 128
WIDTH = 768
COLS = WIDTH // 128
SENT = CAP * COLS

epsilon = 1e-06


def batcher(n):
    pairs = []
    p = 1
    while p < n:
        k = p
        while k >= 1:
            for j in range(k % p, n - k, 2 * k):
                for i in range(min(k, n - j - k)):
                    if (i + j) // (2 * p) == (i + j + k) // (2 * p):
                        pairs.append((i + j, i + j + k))
            k //= 2
        p *= 2
    return pairs


SORT32 = batcher(32)
SORT16 = batcher(16)
AHEAD = 2


def wire(ref, base, i):
    return ref[pl.ds(pl.multiple_of((base + i) * 8, 8), 8), :]


def put(ref, base, i, value):
    ref[pl.ds(pl.multiple_of((base + i) * 8, 8), 8), :] = value


def sort32(ref, base):
    v = [wire(ref, base, i) for i in range(32)]
    for i, j in SORT32:
        v[i], v[j] = jnp.maximum(v[i], v[j]), jnp.minimum(v[i], v[j])
    for i in range(32):
        put(ref, base, i, v[i])


def clean(v):
    n = len(v)
    step = n // 2
    while step:
        for i in range(n):
            if not i & step:
                v[i], v[i + step] = jnp.maximum(v[i], v[i + step]), jnp.minimum(v[i], v[i + step])
        step //= 2
    return v


def clean_at(ref, base):
    v = clean([wire(ref, base, i) for i in range(32)])
    for i in range(32):
        put(ref, base, i, v[i])


def merge64(src, base, dst):
    for op, at in ((jnp.maximum, 0), (jnp.minimum, 32)):
        v = clean([op(wire(src, base, i), wire(src, base, 63 - i)) for i in range(32)])
        for i in range(32):
            put(dst, base + at, i, v[i])


def merge128(src, base, dst):
    for op, at in ((jnp.maximum, 0), (jnp.minimum, 64)):
        v = []
        for i in range(32):
            a = op(wire(src, base, i), wire(src, base, 127 - i))
            b = op(wire(src, base, i + 32), wire(src, base, 95 - i))
            v.append(jnp.maximum(a, b))
            put(dst, base + at + 32, i, jnp.minimum(a, b))
        v = clean(v)
        for i in range(32):
            put(dst, base + at, i, v[i])
        clean_at(dst, base + at + 32)


def merge_top(a, a_base, b, b_base, dst, dst_base, turn=0):
    def other(i):
        value = wire(b, b_base, 127 - i)
        return pltpu.roll(value, turn, 0) if turn else value

    v = []
    for i in range(32):
        c = [jnp.maximum(wire(a, a_base, i + 32 * k), other(i + 32 * k)) for k in range(4)]
        f0, g0 = jnp.maximum(c[0], c[2]), jnp.minimum(c[0], c[2])
        f1, g1 = jnp.maximum(c[1], c[3]), jnp.minimum(c[1], c[3])
        v.append(jnp.maximum(f0, f1))
        put(dst, dst_base + 32, i, jnp.minimum(f0, f1))
        put(dst, dst_base + 64, i, jnp.maximum(g0, g1))
        put(dst, dst_base + 96, i, jnp.minimum(g0, g1))
    v = clean(v)
    for i in range(32):
        put(dst, dst_base, i, v[i])

    def rest(k, carry):
        clean_at(dst, dst_base + 32 + 32 * k)
        return carry

    lax.fori_loop(0, 3, rest, 0)


def loop(n, body):
    def step(i, carry):
        body(i)
        return carry

    lax.fori_loop(0, n, step, 0)


def wires_of(corpus, rows, parts, i, whole=False):
    blocks = rows.shape[0] // 128
    apart, nth, kind = (256, i, 0) if blocks == 2 else (128, i // 2, i % 2 * 4)
    starts = [(kind + k) * apart + nth * 64 for k in range(4)]
    scores = lax.dot_general(
        jnp.concatenate([corpus[at : at + 64, :] for at in starts], axis=0),
        rows,
        (((1,), (1,)), ((), ())),
        preferred_element_type=jnp.float32,
    )
    ref, at = (parts, nth * 512) if whole else (parts[nth], 0)
    for k in range(4):
        for half in range(blocks):
            place = pl.ds(at + (kind + k) * blocks + half, 64, stride=8)
            ref[place, :] = scores[k * 64 : (k + 1) * 64, half * 128 : (half + 1) * 128]


def score(corpus, rows, s):
    for i in range(4):
        wires_of(corpus, rows, s, i, whole=True)


def order(blocks, s, u, dst):
    loop(4 * blocks, lambda i: sort32(s, i * 32))
    loop(2 * blocks, lambda i: merge64(s, i * 64, u))
    if blocks == 1:
        merge128(u, 0, dst)
    else:
        loop(2, lambda i: merge128(u, i * 128, s))
        merge_top(s, 0, s, 128, dst, 0)


def network(v, pairs):
    for i, j in pairs:
        v[i], v[j] = jnp.maximum(v[i], v[j]), jnp.minimum(v[i], v[j])
    return v


def best16(ref, base):
    a = network([wire(ref, base, i) for i in range(16)], SORT16)
    b = network([wire(ref, base, i) for i in range(16, 32)], SORT16)
    return clean([jnp.maximum(a[i], b[15 - i]) for i in range(16)])


def shorten(src, base, dst, dst_base):
    a = best16(src, base)
    b = best16(src, base + 32)
    peak = jnp.maximum(a[15], b[15])
    high = clean([jnp.maximum(a[i], b[15 - i]) for i in range(16)])
    low = clean([jnp.minimum(a[i], b[15 - i]) for i in range(16)])
    for i in range(16):
        put(dst, dst_base, i, high[i])
        put(dst, dst_base, 16 + i, low[i])
    return peak


def best32(src, base, dst, dst_base):
    v = clean([jnp.maximum(wire(src, base, i), wire(src, base, 63 - i)) for i in range(32)])
    for i in range(32):
        put(dst, dst_base, i, v[i])
    return v[31]


def best64(src, dst, turn=0):
    def other(i):
        return pltpu.roll(wire(src, 0, 63 - i), turn, 0) if turn else wire(src, 0, 127 - i)

    v = []
    for i in range(32):
        a = jnp.maximum(wire(src, 0, i), other(i))
        b = jnp.maximum(wire(src, 0, i + 32), other(i + 32))
        v.append(jnp.maximum(a, b))
        put(dst, 32, i, jnp.minimum(a, b))
    v = clean(v)
    for i in range(32):
        put(dst, 0, i, v[i])
    clean_at(dst, 32)
    return wire(dst, 63, 0)


def merge_turned(src, dst, turn):
    for op, at in ((jnp.maximum, 0), (jnp.minimum, 64)):
        v = []
        for i in range(32):
            a = op(wire(src, 0, i), pltpu.roll(wire(src, 0, 63 - i), turn, 0))
            b = op(wire(src, 0, i + 32), pltpu.roll(wire(src, 0, 31 - i), turn, 0))
            v.append(jnp.maximum(a, b))
            put(dst, at + 32, i, jnp.minimum(a, b))
        v = clean(v)
        for i in range(32):
            put(dst, at, i, v[i])
        clean_at(dst, at + 32)


def leaders(groups, own, far, *work, emit):
    near_parts, far_parts, (s, u, w) = work[:4], work[4:8], work[8:]
    sides = (near_parts, far_parts)
    parts = [(g, side, i) for g in range(len(groups)) for side in range(2) for i in range(4)]

    def scored(k):
        if k < len(parts):
            g, side, i = parts[k]
            wires_of((own, far)[side](), groups[g][1](), sides[side], i)

    for k in range(AHEAD):
        scored(k)
    peak = None
    for k, (g, side, i) in enumerate(parts):
        scored(k + AHEAD)
        blocks = groups[g][0]
        if blocks == 2 or i % 2 == 1:
            nth = i if blocks == 2 else i // 2
            now = shorten(sides[side][nth], 0, u, side * 64 * blocks + nth * 32)
            peak = now if peak is None else jnp.maximum(peak, now)
        if side == 0 or i < 3:
            continue
        for j in range(2 * blocks):
            peak = jnp.maximum(peak, best32(u, j * 64, w, j * 32))
        if blocks == 2:
            loop(2, lambda j: merge64(w, j * 64, u))
            peak = jnp.maximum(peak, best64(u, w))
            turns = (4, 2)
        else:
            merge64(w, 0, u)
            peak = jnp.maximum(peak, best64(u, w, turn=4))
            turns = (2, 1)
        merge_turned(w, u, turns[0])
        merge_top(u, 0, u, 0, w, 0, turn=turns[1])
        for turn in (4, 2, 1)[: 4 - blocks]:
            peak = jnp.maximum(peak, pltpu.roll(peak, turn, 0))
        unsure = jnp.max(jnp.where(peak > wire(w, 127, 0), 1.0, 0.0)) > 0.0
        peak = None

        @pl.when(unsure)
        def _():
            long_way(blocks, groups[g][1](), own(), far(), s, u, w)

        for half in range(blocks):
            emit(g, half, w[pl.ds(half, TOPK, stride=8), :].T)


def long_way(blocks, rows, own, far, s, u, w):
    score(own, rows, s)
    order(blocks, s, u, w)
    score(far, rows, s)
    if blocks == 2:
        order(blocks, s, u, u)
        merge_top(w, 0, u, 0, s, 0)
        merge_top(s, 0, s, 0, u, 0, turn=4)
        merge_top(u, 0, u, 0, w, 0, turn=2)
    else:
        loop(4, lambda i: sort32(s, i * 32))
        loop(2, lambda i: merge64(s, i * 64, u))
        merge128(u, 0, s)
        merge_top(w, 0, s, 0, u, 0)
        merge_top(u, 0, u, 0, s, 0, turn=4)
        merge_top(s, 0, s, 0, u, 0, turn=2)
        merge_top(u, 0, u, 0, w, 0, turn=1)


def main_rows(chunk):
    return jnp.concatenate(
        [chunk[:, c * MAIN : (c + 1) * MAIN, :].reshape(-1, 128) for c in range(COLS)], axis=1
    )


def tail_rows(chunk):
    langs = chunk.shape[0]
    many, each = langs * TAIL, TAIL * COLS
    shape, total = (COLS, many, langs * each), langs * each
    col, row, at = (lax.broadcasted_iota(jnp.int32, shape, d) for d in range(3))
    from_row = lax.shift_right_logical(row, 2) * each + col * TAIL + (row & 3)
    picks = jnp.where(at == from_row, 1.0, 0.0).astype(jnp.bfloat16).reshape(total, total)
    flat = chunk[:, MAIN * COLS : SENT, :].reshape(total, 128)
    found = jnp.dot(picks, flat, preferred_element_type=jnp.float32).astype(jnp.bfloat16)
    return jnp.concatenate([found[c * many : (c + 1) * many, :] for c in range(COLS)], axis=1)


def first_kernel(chunk, own, far_in, out, far, rows, sem, *work):
    copy = pltpu.make_async_copy(far_in, far, sem)
    copy.start()
    rows[...] = main_rows(chunk)
    waited = []

    def partner():
        if not waited:
            copy.wait()
            waited.append(True)
        return far

    def emit(g, half, value):
        out[half * Q : (half + 1) * Q, :] = value

    leaders([(2, lambda: rows[...])], lambda: own, partner, *work, emit=emit)


def early_kernel(half0, half1, own, far, out, rows, *work):
    rows[0:128, :] = main_rows(half0)
    rows[128:256, :] = main_rows(half1)

    def emit(g, half, value):
        out[half * Q : (half + 1) * Q, :] = value

    leaders([(2, lambda: rows[...])], lambda: own, lambda: far, *work, emit=emit)


def middle_kernel(mine, cx0, cx1, cy0, cy1, own, far, out, tails, rows, *work):
    rows[0:128, :] = main_rows(cx1)
    rows[128:256, :] = main_rows(cy1)
    rows[256:320, :] = tail_rows(mine)
    for k, chunk in enumerate((cx0, cx1, cy0, cy1)):
        rows[320 + k * 32 : 352 + k * 32, :] = tail_rows(chunk)
    rows[448:512, :] = jnp.zeros((64, WIDTH), jnp.bfloat16)

    def emit(g, half, value):
        (out, tails)[g][half * Q : (half + 1) * Q, :] = value

    leaders(
        [(2, lambda: rows[0:256, :]), (2, lambda: rows[256:512, :])], lambda: own, lambda: far, *work, emit=emit
    )


STEPS = 800.0
FLOOR = 32.5
LN2 = 0.6931471805599453


def coded(v):
    level = jnp.round(jnp.log(jnp.abs(v)) * (STEPS / LN2) + STEPS * FLOOR)
    level = jnp.clip(level, 0.0, 32767.0)
    return jnp.where(v < 0, -level, level)


def decoded(c):
    level = jnp.abs(c)
    v = jnp.where(level > 0, jnp.exp(level * (LN2 / STEPS) - FLOOR * LN2), 0.0)
    return jnp.where(c < 0, -v, v)


def late_kernel(at, cd0, cd1, own, far, r0, r1, r2, tails, out, rows, last, box, *work):
    rows[0:128, :] = main_rows(cd0)
    rows[128:256, :] = main_rows(cd1)
    rows[256:288, :] = tail_rows(cd0)
    rows[288:320, :] = tail_rows(cd1)
    rows[320:384, :] = jnp.zeros((64, WIDTH), jnp.bfloat16)

    def emit(g, half, value):
        last[g * 256 + half * Q : g * 256 + (half + 1) * Q, :] = value

    leaders(
        [(2, lambda: rows[0:256, :]), (1, lambda: rows[256:384, :])], lambda: own, lambda: far, *work, emit=emit
    )
    me = at[0]
    owner = (me, me ^ 1, me ^ 2, me ^ 3)
    none = jnp.zeros((ROWS - CAP, TOPK), jnp.float32)
    for k in range(4):
        for lang in range(LANGS):
            half, start = lang // 8, lang % 8 * MAIN
            if k == 0:
                main = r0[lang * MAIN : (lang + 1) * MAIN, :]
            elif k < 3:
                start += (k - 1) * Q
                main = (r1, r2)[half][start : start + MAIN, :]
            else:
                main = last[lang * MAIN : (lang + 1) * MAIN, :]
            box[k, 0:MAIN, :] = main
            start = k * 64 + lang * TAIL
            if k < 3:
                box[k, MAIN:CAP, :] = tails[start : start + TAIL, :]
            else:
                box[k, MAIN:CAP, :] = last[256 + lang * TAIL : 256 + (lang + 1) * TAIL, :]
            box[k, CAP:ROWS, :] = none
            out[lang, owner[k]] = coded(box[k]).astype(jnp.int32).astype(jnp.int16)


COST = 2 * 256 * 2048 * 768 * 8
VMEM = pl.BlockSpec(memory_space=pltpu.VMEM)
LIMIT = pltpu.CompilerParams(vmem_limit_bytes=14 << 20)
WORK = [pltpu.VMEM((64 * 8, 128), jnp.float32)] * 8 + [
    pltpu.VMEM((256 * 8, 128), jnp.float32),
    pltpu.VMEM((256 * 8, 128), jnp.float32),
    pltpu.VMEM((128 * 8, 128), jnp.float32),
]


def first(chunk, own, far):
    return pl.pallas_call(
        first_kernel,
        out_shape=(
            jax.ShapeDtypeStruct((256, TOPK), jnp.float32),
            jax.ShapeDtypeStruct((1024, WIDTH), jnp.bfloat16),
        ),
        in_specs=[VMEM, VMEM, pl.BlockSpec(memory_space=pl.ANY)],
        out_specs=(VMEM, VMEM),
        scratch_shapes=[pltpu.VMEM((256, WIDTH), jnp.bfloat16), pltpu.SemaphoreType.DMA] + WORK,
        compiler_params=LIMIT,
        cost_estimate=pl.CostEstimate(flops=COST, bytes_accessed=1 << 20, transcendentals=0),
        name="first",
    )(chunk, own, far)


def early(half0, half1, own, far):
    return pl.pallas_call(
        early_kernel,
        out_shape=jax.ShapeDtypeStruct((256, TOPK), jnp.float32),
        in_specs=[VMEM] * 4,
        out_specs=VMEM,
        scratch_shapes=[pltpu.VMEM((256, WIDTH), jnp.bfloat16)] + WORK,
        compiler_params=LIMIT,
        cost_estimate=pl.CostEstimate(flops=COST, bytes_accessed=1 << 20, transcendentals=0),
        name="early",
    )(half0, half1, own, far)


def middle(mine, halves, own, far):
    return pl.pallas_call(
        middle_kernel,
        out_shape=[jax.ShapeDtypeStruct((256, TOPK), jnp.float32)] * 2,
        in_specs=[VMEM] * 7,
        out_specs=[VMEM] * 2,
        scratch_shapes=[pltpu.VMEM((512, WIDTH), jnp.bfloat16)] + WORK,
        compiler_params=LIMIT,
        cost_estimate=pl.CostEstimate(flops=COST * 2, bytes_accessed=1 << 20, transcendentals=0),
        name="middle",
    )(mine, *halves, own, far)


def late(at, halves, own, far, results):
    return pl.pallas_call(
        late_kernel,
        out_shape=jax.ShapeDtypeStruct((LANGS, 4, ROWS, TOPK), jnp.int16),
        in_specs=[pl.BlockSpec(memory_space=pltpu.SMEM)] + [VMEM] * 8,
        out_specs=VMEM,
        scratch_shapes=[
            pltpu.VMEM((384, WIDTH), jnp.bfloat16),
            pltpu.VMEM((384, TOPK), jnp.float32),
            pltpu.VMEM((4, ROWS, TOPK), jnp.float32),
        ]
        + WORK,
        compiler_params=LIMIT,
        cost_estimate=pl.CostEstimate(flops=COST * 2, bytes_accessed=1 << 20, transcendentals=0),
        name="late",
    )(at, *halves, own, far, *results)


def outbox_kernel(queries_in, routes_in, out, slots, queries, routes, sems):
    copies = (
        pltpu.make_async_copy(routes_in, routes, sems.at[0]),
        pltpu.make_async_copy(queries_in, queries, sems.at[1]),
    )
    for copy in copies:
        copy.start()
    for copy in copies:
        copy.wait()
    x = queries[...].astype(jnp.float32)
    unit = (x * lax.rsqrt(jnp.mean(x * x, axis=1, keepdims=True) + epsilon)).astype(jnp.bfloat16)
    along = jnp.broadcast_to(routes[...].astype(jnp.float32), (Q, Q))
    down = along.T
    before = lax.broadcasted_iota(jnp.int32, (Q, Q), 0) < lax.broadcasted_iota(jnp.int32, (Q, Q), 1)
    earlier = jnp.where(before & (along == down), 1.0, 0.0)
    rank = jnp.sum(earlier, axis=0, keepdims=True).astype(jnp.int32)
    lang = routes[...]
    slots[...] = lang * ROWS + rank
    main_at = jnp.where(rank < MAIN, lang * MAIN + rank, -1)
    hits = lax.broadcasted_iota(jnp.int32, (LANGS * MAIN, Q), 0) == jnp.broadcast_to(main_at, (LANGS * MAIN, Q))
    picks = jnp.where(hits, 1.0, 0.0).astype(jnp.bfloat16)
    box = jnp.dot(picks, unit, preferred_element_type=jnp.float32).astype(jnp.bfloat16)
    for c in range(COLS):
        out[:, c * MAIN : (c + 1) * MAIN, :] = box[:, c * 128 : (c + 1) * 128].reshape(LANGS, MAIN, 128)
    each = TAIL * COLS
    tail_at = jnp.where(rank < MAIN, -1, lang * TAIL + rank - MAIN)
    shape = (LANGS, each, Q)
    of_lang, row = (lax.broadcasted_iota(jnp.int32, shape, d) for d in range(2))
    hits = of_lang * TAIL + (row & 3) == jnp.broadcast_to(tail_at.reshape(1, 1, Q), shape)
    tail = jnp.zeros((LANGS * each, 128), jnp.float32)
    for c in range(COLS):
        picks = jnp.where(hits & (lax.shift_right_logical(row, 2) == c), 1.0, 0.0)
        picks = picks.astype(jnp.bfloat16).reshape(LANGS * each, Q)
        tail = tail + jnp.dot(picks, unit[:, c * 128 : (c + 1) * 128], preferred_element_type=jnp.float32)
    out[:, MAIN * COLS : SENT, :] = tail.astype(jnp.bfloat16).reshape(LANGS, each, 128)


def outbox_of(queries, routes):
    return pl.pallas_call(
        outbox_kernel,
        out_shape=(
            jax.ShapeDtypeStruct((LANGS, SENT, 128), jnp.bfloat16),
            jax.ShapeDtypeStruct((1, Q), jnp.int32),
        ),
        in_specs=[pl.BlockSpec(memory_space=pltpu.HBM)] * 2,
        out_specs=(VMEM, VMEM),
        scratch_shapes=[
            pltpu.VMEM((Q, WIDTH), jnp.bfloat16),
            pltpu.VMEM((1, Q), jnp.int32),
            pltpu.SemaphoreType.DMA((2,)),
        ],
        compiler_params=pltpu.CompilerParams(vmem_limit_bytes=60 << 20),
        name="outbox",
    )(queries, routes)


def join_kernel(back, slots, out, a, b):
    total = LANGS * ROWS
    hits = lax.broadcasted_iota(jnp.int32, (total, Q), 0) == jnp.broadcast_to(slots[...], (total, Q))
    picks = jnp.where(hits, 1.0, 0.0)
    picks = jnp.concatenate([picks[i * Q : (i + 1) * Q, :].T for i in range(total // Q)], axis=1)
    picks = picks.astype(jnp.bfloat16)
    for k in range(4):
        code = back[:, k].astype(jnp.int32).astype(jnp.float32).reshape(total, TOPK)
        high = code.astype(jnp.bfloat16)
        low = (code - high.astype(jnp.float32)).astype(jnp.bfloat16)
        rows = jnp.dot(picks, high, preferred_element_type=jnp.float32) + jnp.dot(
            picks, low, preferred_element_type=jnp.float32
        )
        ranks = decoded(rows).T
        a[pl.ds(k, TOPK, stride=8), :] = ranks
        a[pl.ds(k + 4, TOPK, stride=8), :] = ranks
    merge_top(a, 0, a, 0, b, 0, turn=2)
    merge_top(b, 0, b, 0, a, 0, turn=1)
    out[...] = a[pl.ds(0, TOPK, stride=8), :].T


def join(back, slots):
    return pl.pallas_call(
        join_kernel,
        out_shape=jax.ShapeDtypeStruct((Q, TOPK), jnp.float32),
        in_specs=[VMEM] * 2,
        out_specs=VMEM,
        scratch_shapes=[pltpu.VMEM((128 * 8, 128), jnp.float32)] * 2,
        compiler_params=LIMIT,
        name="join",
    )(back, slots)


AXES = ("lang", "shard")


def moves(target):
    return [
        (lang * 8 + y * 4 + x, lang * 8 + ty * 4 + tx % 4)
        for lang in range(16)
        for y in range(2)
        for x in range(4)
        for ty, tx in (target(lang % 2, y, x),)
    ]


def pair(core, y, x):
    return y, x + (1 if (x + core) % 2 == 0 else -1)


def over_x(core, y, x):
    return y, x + 2


def over_y(core, y, x):
    return 1 - y, x


TEAMS = [
    [lang * 8 + y * 4 + odd + 2 * half for lang in range(16) for y in range(2) for half in range(2)]
    for odd in range(2)
]


def shards(queries, routes, corpus):
    far = lax.ppermute(corpus, AXES, moves(pair))
    outbox, slots = outbox_of(queries, routes.reshape(1, Q))
    mine = lax.all_to_all(outbox, "lang", split_axis=0, concat_axis=0, tiled=True)
    cx0, cy0, cx1, cy1 = (
        lax.ppermute(part, AXES, moves(over)) for part in (mine[:8], mine[8:]) for over in (over_x, over_y)
    )
    r0, far = first(mine, corpus, far)
    cx0, cy0, r0 = lax.optimization_barrier((cx0, cy0, r0))
    cd0 = lax.ppermute(cx0, AXES, moves(over_y))
    r1 = early(cx0, cy0, corpus, far)
    cx1, cy1, r1 = lax.optimization_barrier((cx1, cy1, r1))
    cd1 = lax.ppermute(cy1, AXES, moves(over_x))
    r2, tails = middle(mine, (cx0, cx1, cy0, cy1), corpus, far)
    shard = lax.axis_index("shard")
    at = (lax.shift_right_logical(shard, 2) * 2 + (lax.shift_right_logical(shard, 1) & 1)).reshape(1)
    found = late(at, (cd0, cd1), corpus, far, (r0, r1, r2, tails))
    back = lax.all_to_all(
        found.reshape(LANGS * 4, ROWS, TOPK), AXES, 0, 0, axis_index_groups=TEAMS, tiled=True
    )
    return join(back.reshape(LANGS, 4, ROWS, TOPK), slots)


def solution(mesh):
    placed = (P(AXES, None), P(AXES, None), P(AXES, None))
    return jax.shard_map(shards, mesh=mesh, in_specs=placed, out_specs=P(AXES, None), check_vma=False)
```

```python
import functools

import jax
import jax.numpy as jnp
from jax import lax
from jax.experimental import pallas as pl
from jax.experimental.pallas import tpu as pltpu
from jax.sharding import PartitionSpec as P

TOPK = 128
LANGS = 16
CAP = 20
ROWS = 24
MAIN = 16
TAIL = CAP - MAIN
Q = 128
WIDTH = 768
COLS = WIDTH // 128
SENT = CAP * COLS

epsilon = 1e-06


def batcher(n):
    pairs = []
    p = 1
    while p < n:
        k = p
        while k >= 1:
            for j in range(k % p, n - k, 2 * k):
                for i in range(min(k, n - j - k)):
                    if (i + j) // (2 * p) == (i + j + k) // (2 * p):
                        pairs.append((i + j, i + j + k))
            k //= 2
        p *= 2
    return pairs


SORT32 = batcher(32)
SORT16 = batcher(16)
AHEAD = 2


def wire(ref, base, i):
    return ref[pl.ds(pl.multiple_of((base + i) * 8, 8), 8), :]


def put(ref, base, i, value):
    ref[pl.ds(pl.multiple_of((base + i) * 8, 8), 8), :] = value


def sort32(ref, base):
    v = [wire(ref, base, i) for i in range(32)]
    for i, j in SORT32:
        v[i], v[j] = jnp.maximum(v[i], v[j]), jnp.minimum(v[i], v[j])
    for i in range(32):
        put(ref, base, i, v[i])


def clean(v):
    n = len(v)
    step = n // 2
    while step:
        for i in range(n):
            if not i & step:
                v[i], v[i + step] = jnp.maximum(v[i], v[i + step]), jnp.minimum(v[i], v[i + step])
        step //= 2
    return v


def clean_at(ref, base):
    v = clean([wire(ref, base, i) for i in range(32)])
    for i in range(32):
        put(ref, base, i, v[i])


def merge64(src, base, dst):
    for op, at in ((jnp.maximum, 0), (jnp.minimum, 32)):
        v = clean([op(wire(src, base, i), wire(src, base, 63 - i)) for i in range(32)])
        for i in range(32):
            put(dst, base + at, i, v[i])


def merge128(src, base, dst):
    for op, at in ((jnp.maximum, 0), (jnp.minimum, 64)):
        v = []
        for i in range(32):
            a = op(wire(src, base, i), wire(src, base, 127 - i))
            b = op(wire(src, base, i + 32), wire(src, base, 95 - i))
            v.append(jnp.maximum(a, b))
            put(dst, base + at + 32, i, jnp.minimum(a, b))
        v = clean(v)
        for i in range(32):
            put(dst, base + at, i, v[i])
        clean_at(dst, base + at + 32)


def merge_top(a, a_base, b, b_base, dst, dst_base, turn=0):
    def other(i):
        value = wire(b, b_base, 127 - i)
        return pltpu.roll(value, turn, 0) if turn else value

    v = []
    for i in range(32):
        c = [jnp.maximum(wire(a, a_base, i + 32 * k), other(i + 32 * k)) for k in range(4)]
        f0, g0 = jnp.maximum(c[0], c[2]), jnp.minimum(c[0], c[2])
        f1, g1 = jnp.maximum(c[1], c[3]), jnp.minimum(c[1], c[3])
        v.append(jnp.maximum(f0, f1))
        put(dst, dst_base + 32, i, jnp.minimum(f0, f1))
        put(dst, dst_base + 64, i, jnp.maximum(g0, g1))
        put(dst, dst_base + 96, i, jnp.minimum(g0, g1))
    v = clean(v)
    for i in range(32):
        put(dst, dst_base, i, v[i])

    def rest(k, carry):
        clean_at(dst, dst_base + 32 + 32 * k)
        return carry

    lax.fori_loop(0, 3, rest, 0)


def loop(n, body):
    def step(i, carry):
        body(i)
        return carry

    lax.fori_loop(0, n, step, 0)


def wires_of(corpus, rows, parts, i, whole=False):
    blocks = rows.shape[0] // 128
    apart, nth, kind = (256, i, 0) if blocks == 2 else (128, i // 2, i % 2 * 4)
    starts = [(kind + k) * apart + nth * 64 for k in range(4)]
    scores = lax.dot_general(
        jnp.concatenate([corpus[at : at + 64, :] for at in starts], axis=0),
        rows,
        (((1,), (1,)), ((), ())),
        preferred_element_type=jnp.float32,
    )
    ref, at = (parts, nth * 512) if whole else (parts[nth], 0)
    for k in range(4):
        for half in range(blocks):
            place = pl.ds(at + (kind + k) * blocks + half, 64, stride=8)
            ref[place, :] = scores[k * 64 : (k + 1) * 64, half * 128 : (half + 1) * 128]


def score(corpus, rows, s):
    for i in range(4):
        wires_of(corpus, rows, s, i, whole=True)


def order(blocks, s, u, dst):
    loop(4 * blocks, lambda i: sort32(s, i * 32))
    loop(2 * blocks, lambda i: merge64(s, i * 64, u))
    if blocks == 1:
        merge128(u, 0, dst)
    else:
        loop(2, lambda i: merge128(u, i * 128, s))
        merge_top(s, 0, s, 128, dst, 0)


def network(v, pairs):
    for i, j in pairs:
        v[i], v[j] = jnp.maximum(v[i], v[j]), jnp.minimum(v[i], v[j])
    return v


def best16(ref, base):
    a = network([wire(ref, base, i) for i in range(16)], SORT16)
    b = network([wire(ref, base, i) for i in range(16, 32)], SORT16)
    return clean([jnp.maximum(a[i], b[15 - i]) for i in range(16)])


def shorten(src, base, dst, dst_base):
    a = best16(src, base)
    b = best16(src, base + 32)
    peak = jnp.maximum(a[15], b[15])
    high = clean([jnp.maximum(a[i], b[15 - i]) for i in range(16)])
    low = clean([jnp.minimum(a[i], b[15 - i]) for i in range(16)])
    for i in range(16):
        put(dst, dst_base, i, high[i])
        put(dst, dst_base, 16 + i, low[i])
    return peak


def best32(src, base, dst, dst_base):
    v = clean([jnp.maximum(wire(src, base, i), wire(src, base, 63 - i)) for i in range(32)])
    for i in range(32):
        put(dst, dst_base, i, v[i])
    return v[31]


def best64(src, dst, turn=0):
    def other(i):
        return pltpu.roll(wire(src, 0, 63 - i), turn, 0) if turn else wire(src, 0, 127 - i)

    v = []
    for i in range(32):
        a = jnp.maximum(wire(src, 0, i), other(i))
        b = jnp.maximum(wire(src, 0, i + 32), other(i + 32))
        v.append(jnp.maximum(a, b))
        put(dst, 32, i, jnp.minimum(a, b))
    v = clean(v)
    for i in range(32):
        put(dst, 0, i, v[i])
    clean_at(dst, 32)
    return wire(dst, 63, 0)


def merge_turned(src, dst, turn):
    for op, at in ((jnp.maximum, 0), (jnp.minimum, 64)):
        v = []
        for i in range(32):
            a = op(wire(src, 0, i), pltpu.roll(wire(src, 0, 63 - i), turn, 0))
            b = op(wire(src, 0, i + 32), pltpu.roll(wire(src, 0, 31 - i), turn, 0))
            v.append(jnp.maximum(a, b))
            put(dst, at + 32, i, jnp.minimum(a, b))
        v = clean(v)
        for i in range(32):
            put(dst, at, i, v[i])
        clean_at(dst, at + 32)


def leaders(groups, own, far, *work, emit):
    near_parts, far_parts, (s, u, w) = work[:4], work[4:8], work[8:]
    sides = (near_parts, far_parts)
    parts = [(g, side, i) for g in range(len(groups)) for side in range(2) for i in range(4)]

    def scored(k):
        if k < len(parts):
            g, side, i = parts[k]
            wires_of((own, far)[side](), groups[g][1](), sides[side], i)

    for k in range(AHEAD):
        scored(k)
    peak = None
    for k, (g, side, i) in enumerate(parts):
        scored(k + AHEAD)
        blocks = groups[g][0]
        if blocks == 2 or i % 2 == 1:
            nth = i if blocks == 2 else i // 2
            now = shorten(sides[side][nth], 0, u, side * 64 * blocks + nth * 32)
            peak = now if peak is None else jnp.maximum(peak, now)
        if side == 0 or i < 3:
            continue
        for j in range(2 * blocks):
            peak = jnp.maximum(peak, best32(u, j * 64, w, j * 32))
        if blocks == 2:
            loop(2, lambda j: merge64(w, j * 64, u))
            peak = jnp.maximum(peak, best64(u, w))
            turns = (4, 2)
        else:
            merge64(w, 0, u)
            peak = jnp.maximum(peak, best64(u, w, turn=4))
            turns = (2, 1)
        merge_turned(w, u, turns[0])
        merge_top(u, 0, u, 0, w, 0, turn=turns[1])
        for turn in (4, 2, 1)[: 4 - blocks]:
            peak = jnp.maximum(peak, pltpu.roll(peak, turn, 0))
        unsure = jnp.max(jnp.where(peak > wire(w, 127, 0), 1.0, 0.0)) > 0.0
        peak = None

        @pl.when(unsure)
        def _():
            long_way(blocks, groups[g][1](), own(), far(), s, u, w)

        for half in range(blocks):
            emit(g, half, w[pl.ds(half, TOPK, stride=8), :].T)


def long_way(blocks, rows, own, far, s, u, w):
    score(own, rows, s)
    order(blocks, s, u, w)
    score(far, rows, s)
    if blocks == 2:
        order(blocks, s, u, u)
        merge_top(w, 0, u, 0, s, 0)
        merge_top(s, 0, s, 0, u, 0, turn=4)
        merge_top(u, 0, u, 0, w, 0, turn=2)
    else:
        loop(4, lambda i: sort32(s, i * 32))
        loop(2, lambda i: merge64(s, i * 64, u))
        merge128(u, 0, s)
        merge_top(w, 0, s, 0, u, 0)
        merge_top(u, 0, u, 0, s, 0, turn=4)
        merge_top(s, 0, s, 0, u, 0, turn=2)
        merge_top(u, 0, u, 0, w, 0, turn=1)


def main_rows(chunk):
    return jnp.concatenate(
        [chunk[:, c * MAIN : (c + 1) * MAIN, :].reshape(-1, 128) for c in range(COLS)], axis=1
    )


def tail_rows(chunk):
    langs = chunk.shape[0]
    many, each = langs * TAIL, TAIL * COLS
    shape, total = (COLS, many, langs * each), langs * each
    col, row, at = (lax.broadcasted_iota(jnp.int32, shape, d) for d in range(3))
    from_row = lax.shift_right_logical(row, 2) * each + col * TAIL + (row & 3)
    picks = jnp.where(at == from_row, 1.0, 0.0).astype(jnp.bfloat16).reshape(total, total)
    flat = chunk[:, MAIN * COLS : SENT, :].reshape(total, 128)
    found = jnp.dot(picks, flat, preferred_element_type=jnp.float32).astype(jnp.bfloat16)
    return jnp.concatenate([found[c * many : (c + 1) * many, :] for c in range(COLS)], axis=1)


def first_kernel(chunk, own, far, out, rows, *work):
    rows[...] = main_rows(chunk)

    def emit(g, half, value):
        out[half * Q : (half + 1) * Q, :] = value

    leaders([(2, lambda: rows[...])], lambda: own, lambda: far, *work, emit=emit)


def early_kernel(half0, half1, own, far, out, rows, *work):
    rows[0:128, :] = main_rows(half0)
    rows[128:256, :] = main_rows(half1)

    def emit(g, half, value):
        out[half * Q : (half + 1) * Q, :] = value

    leaders([(2, lambda: rows[...])], lambda: own, lambda: far, *work, emit=emit)


def middle_kernel(mine, cx0, cx1, cy0, cy1, own, far, out, tails, rows, *work):
    rows[0:128, :] = main_rows(cx1)
    rows[128:256, :] = main_rows(cy1)
    rows[256:320, :] = tail_rows(mine)
    for k, chunk in enumerate((cx0, cx1, cy0, cy1)):
        rows[320 + k * 32 : 352 + k * 32, :] = tail_rows(chunk)
    rows[448:512, :] = jnp.zeros((64, WIDTH), jnp.bfloat16)

    def emit(g, half, value):
        (out, tails)[g][half * Q : (half + 1) * Q, :] = value

    leaders(
        [(2, lambda: rows[0:256, :]), (2, lambda: rows[256:512, :])], lambda: own, lambda: far, *work, emit=emit
    )


STEPS = 800.0
FLOOR = 32.5
LN2 = 0.6931471805599453


def coded(v):
    level = jnp.round(jnp.log(jnp.abs(v)) * (STEPS / LN2) + STEPS * FLOOR)
    level = jnp.clip(level, 0.0, 32767.0)
    return jnp.where(v < 0, -level, level)


def decoded(c):
    level = jnp.abs(c)
    v = jnp.where(level > 0, jnp.exp(level * (LN2 / STEPS) - FLOOR * LN2), 0.0)
    return jnp.where(c < 0, -v, v)


def late_kernel(at, cd0, cd1, own, far, r0, r1, r2, tails, keep, give, rows, last, box, *work):
    rows[0:128, :] = main_rows(cd0)
    rows[128:256, :] = main_rows(cd1)
    rows[256:288, :] = tail_rows(cd0)
    rows[288:320, :] = tail_rows(cd1)
    rows[320:384, :] = jnp.zeros((64, WIDTH), jnp.bfloat16)

    def emit(g, half, value):
        last[g * 256 + half * Q : g * 256 + (half + 1) * Q, :] = value

    leaders(
        [(2, lambda: rows[0:256, :]), (1, lambda: rows[256:384, :])], lambda: own, lambda: far, *work, emit=emit
    )
    me, side = at[0], at[1].astype(jnp.float32)
    owner = (me, me ^ 1, me ^ 2, me ^ 3)
    none = jnp.zeros((ROWS - CAP, TOPK), jnp.float32)
    for k in range(4):
        for lang in range(LANGS):
            half, start = lang // 8, lang % 8 * MAIN
            if k == 0:
                main = r0[lang * MAIN : (lang + 1) * MAIN, :]
            elif k < 3:
                start += (k - 1) * Q
                main = (r1, r2)[half][start : start + MAIN, :]
            else:
                main = last[lang * MAIN : (lang + 1) * MAIN, :]
            here = 2 * k + lang % 2
            box[here, 0:MAIN, :] = main
            start = k * 64 + lang * TAIL
            if k < 3:
                box[here, MAIN:CAP, :] = tails[start : start + TAIL, :]
            else:
                box[here, MAIN:CAP, :] = last[256 + lang * TAIL : 256 + (lang + 1) * TAIL, :]
            box[here, CAP:ROWS, :] = none
            if lang % 2 == 1:
                even, odd = coded(box[2 * k]), coded(box[2 * k + 1])
                shift = (odd - even) * side
                keep[lang // 2, owner[k], 0] = (even + shift).astype(jnp.int32).astype(jnp.int16)
                give[lang // 2, owner[k]] = (odd - shift).astype(jnp.int32).astype(jnp.int16)


COST = 2 * 256 * 2048 * 768 * 8
VMEM = pl.BlockSpec(memory_space=pltpu.VMEM)
LIMIT = pltpu.CompilerParams(vmem_limit_bytes=14 << 20)
WORK = [pltpu.VMEM((64 * 8, 128), jnp.float32)] * 8 + [
    pltpu.VMEM((256 * 8, 128), jnp.float32),
    pltpu.VMEM((256 * 8, 128), jnp.float32),
    pltpu.VMEM((128 * 8, 128), jnp.float32),
]


def first(chunk, own, far):
    return pl.pallas_call(
        first_kernel,
        out_shape=jax.ShapeDtypeStruct((256, TOPK), jnp.float32),
        in_specs=[VMEM] * 3,
        out_specs=VMEM,
        scratch_shapes=[pltpu.VMEM((256, WIDTH), jnp.bfloat16)] + WORK,
        compiler_params=LIMIT,
        cost_estimate=pl.CostEstimate(flops=COST, bytes_accessed=1 << 20, transcendentals=0),
        name="first",
    )(chunk, own, far)


def early(half0, half1, own, far):
    return pl.pallas_call(
        early_kernel,
        out_shape=jax.ShapeDtypeStruct((256, TOPK), jnp.float32),
        in_specs=[VMEM] * 4,
        out_specs=VMEM,
        scratch_shapes=[pltpu.VMEM((256, WIDTH), jnp.bfloat16)] + WORK,
        compiler_params=LIMIT,
        cost_estimate=pl.CostEstimate(flops=COST, bytes_accessed=1 << 20, transcendentals=0),
        name="early",
    )(half0, half1, own, far)


def middle(mine, halves, own, far):
    return pl.pallas_call(
        middle_kernel,
        out_shape=[jax.ShapeDtypeStruct((256, TOPK), jnp.float32)] * 2,
        in_specs=[VMEM] * 7,
        out_specs=[VMEM] * 2,
        scratch_shapes=[pltpu.VMEM((512, WIDTH), jnp.bfloat16)] + WORK,
        compiler_params=LIMIT,
        cost_estimate=pl.CostEstimate(flops=COST * 2, bytes_accessed=1 << 20, transcendentals=0),
        name="middle",
    )(mine, *halves, own, far)


def late(at, halves, own, far, results):
    return pl.pallas_call(
        late_kernel,
        out_shape=(
            jax.ShapeDtypeStruct((LANGS // 2, 4, 2, ROWS, TOPK), jnp.int16),
            jax.ShapeDtypeStruct((LANGS // 2, 4, ROWS, TOPK), jnp.int16),
        ),
        in_specs=[pl.BlockSpec(memory_space=pltpu.SMEM)] + [VMEM] * 8,
        out_specs=(VMEM, VMEM),
        scratch_shapes=[
            pltpu.VMEM((384, WIDTH), jnp.bfloat16),
            pltpu.VMEM((384, TOPK), jnp.float32),
            pltpu.VMEM((8, ROWS, TOPK), jnp.float32),
        ]
        + WORK,
        compiler_params=LIMIT,
        cost_estimate=pl.CostEstimate(flops=COST * 2, bytes_accessed=1 << 20, transcendentals=0),
        name="late",
    )(at, *halves, own, far, *results)


def outbox_kernel(at, queries_in, routes_in, out, slots, queries, routes, sems):
    copies = (
        pltpu.make_async_copy(routes_in, routes, sems.at[0]),
        pltpu.make_async_copy(queries_in, queries, sems.at[1]),
    )
    for copy in copies:
        copy.start()
    for copy in copies:
        copy.wait()
    x = queries[...].astype(jnp.float32)
    unit = (x * lax.rsqrt(jnp.mean(x * x, axis=1, keepdims=True) + epsilon)).astype(jnp.bfloat16)
    along = jnp.broadcast_to(routes[...].astype(jnp.float32), (Q, Q))
    down = along.T
    before = lax.broadcasted_iota(jnp.int32, (Q, Q), 0) < lax.broadcasted_iota(jnp.int32, (Q, Q), 1)
    earlier = jnp.where(before & (along == down), 1.0, 0.0)
    rank = jnp.sum(earlier, axis=0, keepdims=True).astype(jnp.int32)
    lang = routes[...]
    slots[...] = (lang ^ at[1]) * ROWS + rank
    main_at = jnp.where(rank < MAIN, lang * MAIN + rank, -1)
    hits = lax.broadcasted_iota(jnp.int32, (LANGS * MAIN, Q), 0) == jnp.broadcast_to(main_at, (LANGS * MAIN, Q))
    picks = jnp.where(hits, 1.0, 0.0).astype(jnp.bfloat16)
    box = jnp.dot(picks, unit, preferred_element_type=jnp.float32).astype(jnp.bfloat16)
    for c in range(COLS):
        out[:, c * MAIN : (c + 1) * MAIN, :] = box[:, c * 128 : (c + 1) * 128].reshape(LANGS, MAIN, 128)
    each = TAIL * COLS
    tail_at = jnp.where(rank < MAIN, -1, lang * TAIL + rank - MAIN)
    shape = (LANGS, each, Q)
    of_lang, row = (lax.broadcasted_iota(jnp.int32, shape, d) for d in range(2))
    hits = of_lang * TAIL + (row & 3) == jnp.broadcast_to(tail_at.reshape(1, 1, Q), shape)
    tail = jnp.zeros((LANGS * each, 128), jnp.float32)
    for c in range(COLS):
        picks = jnp.where(hits & (lax.shift_right_logical(row, 2) == c), 1.0, 0.0)
        picks = picks.astype(jnp.bfloat16).reshape(LANGS * each, Q)
        tail = tail + jnp.dot(picks, unit[:, c * 128 : (c + 1) * 128], preferred_element_type=jnp.float32)
    out[:, MAIN * COLS : SENT, :] = tail.astype(jnp.bfloat16).reshape(LANGS, each, 128)


def outbox_of(at, queries, routes):
    return pl.pallas_call(
        outbox_kernel,
        out_shape=(
            jax.ShapeDtypeStruct((LANGS, SENT, 128), jnp.bfloat16),
            jax.ShapeDtypeStruct((1, Q), jnp.int32),
        ),
        in_specs=[pl.BlockSpec(memory_space=pltpu.SMEM)] + [pl.BlockSpec(memory_space=pltpu.HBM)] * 2,
        out_specs=(VMEM, VMEM),
        scratch_shapes=[
            pltpu.VMEM((Q, WIDTH), jnp.bfloat16),
            pltpu.VMEM((1, Q), jnp.int32),
            pltpu.SemaphoreType.DMA((2,)),
        ],
        compiler_params=pltpu.CompilerParams(vmem_limit_bytes=60 << 20),
        name="outbox",
    )(at, queries, routes)


def join_kernel(back, slots, out, a, b):
    total = LANGS * ROWS
    hits = lax.broadcasted_iota(jnp.int32, (total, Q), 0) == jnp.broadcast_to(slots[...], (total, Q))
    picks = jnp.where(hits, 1.0, 0.0)
    picks = jnp.concatenate([picks[i * Q : (i + 1) * Q, :].T for i in range(total // Q)], axis=1)
    picks = picks.astype(jnp.bfloat16)
    for k in range(4):
        code = back[:, k].astype(jnp.int32).astype(jnp.float32).reshape(total, TOPK)
        high = code.astype(jnp.bfloat16)
        low = (code - high.astype(jnp.float32)).astype(jnp.bfloat16)
        rows = jnp.dot(picks, high, preferred_element_type=jnp.float32) + jnp.dot(
            picks, low, preferred_element_type=jnp.float32
        )
        ranks = decoded(rows).T
        a[pl.ds(k, TOPK, stride=8), :] = ranks
        a[pl.ds(k + 4, TOPK, stride=8), :] = ranks
    merge_top(a, 0, a, 0, b, 0, turn=2)
    merge_top(b, 0, b, 0, a, 0, turn=1)
    out[...] = a[pl.ds(0, TOPK, stride=8), :].T


def join(back, slots):
    return pl.pallas_call(
        join_kernel,
        out_shape=jax.ShapeDtypeStruct((Q, TOPK), jnp.float32),
        in_specs=[VMEM] * 2,
        out_specs=VMEM,
        scratch_shapes=[pltpu.VMEM((128 * 8, 128), jnp.float32)] * 2,
        compiler_params=LIMIT,
        name="join",
    )(back, slots)


AXES = ("lang", "shard")


def moves(target):
    return [
        (lang * 8 + y * 4 + x, lang * 8 + ty * 4 + tx % 4)
        for lang in range(16)
        for y in range(2)
        for x in range(4)
        for ty, tx in (target(lang % 2, y, x),)
    ]


def pair(core, y, x):
    return y, x + (1 if (x + core) % 2 == 0 else -1)


def over_x(core, y, x):
    return y, x + 2


def over_y(core, y, x):
    return 1 - y, x


TEAMS = [
    [lang * 8 + y * 4 + odd + 2 * half for lang in range(core, 16, 2) for y in range(2) for half in range(2)]
    for core in range(2)
    for odd in range(2)
]


def shards(queries, routes, corpus):
    far = lax.ppermute(corpus, AXES, moves(pair))
    shard, core = lax.axis_index("shard"), lax.axis_index("lang") & 1
    seat = lax.shift_right_logical(shard, 2) * 2 + (lax.shift_right_logical(shard, 1) & 1)
    at = jnp.stack([seat, core])
    outbox, slots = outbox_of(at, queries, routes.reshape(1, Q))
    mine = lax.all_to_all(outbox, "lang", split_axis=0, concat_axis=0, tiled=True)
    mine, far = lax.optimization_barrier((mine, far))
    cx0, cy0, cx1, cy1 = (
        lax.ppermute(part, AXES, moves(over)) for part in (mine[:8], mine[8:]) for over in (over_x, over_y)
    )
    r0 = first(mine, corpus, far)
    cx0, cy0, r0 = lax.optimization_barrier((cx0, cy0, r0))
    cd0 = lax.ppermute(cx0, AXES, moves(over_y))
    r1 = early(cx0, cy0, corpus, far)
    cx1, cy1, r1 = lax.optimization_barrier((cx1, cy1, r1))
    cd1 = lax.ppermute(cy1, AXES, moves(over_x))
    r2, tails = middle(mine, (cx0, cx1, cy0, cy1), corpus, far)
    keep, give = late(at, (cd0, cd1), corpus, far, (r0, r1, r2, tails))
    other = lax.ppermute(give, AXES, [(d, d ^ 8) for d in range(128)])
    sent = lax.dynamic_update_slice(keep, other[:, :, None], (0, 0, 1, 0, 0))
    sent = sent.reshape(LANGS * 2, 2 * ROWS, TOPK)
    back = lax.all_to_all(sent, AXES, 0, 0, axis_index_groups=TEAMS, tiled=True)
    return join(back.reshape(LANGS // 2, 4, 2 * ROWS, TOPK), slots)


def solution(mesh):
    placed = (P(AXES, None), P(AXES, None), P(AXES, None))
    return jax.shard_map(shards, mesh=mesh, in_specs=placed, out_specs=P(AXES, None), check_vma=False)
```

```python
import functools

import jax
import jax.numpy as jnp
from jax import lax
from jax.experimental import pallas as pl
from jax.experimental.pallas import tpu as pltpu
from jax.sharding import PartitionSpec as P

TOPK = 128
LANGS = 16
CAP = 20
ROWS = 24
MAIN = 16
TAIL = CAP - MAIN
Q = 128
WIDTH = 768
COLS = WIDTH // 128
SENT = CAP * COLS

epsilon = 1e-06


def batcher(n):
    pairs = []
    p = 1
    while p < n:
        k = p
        while k >= 1:
            for j in range(k % p, n - k, 2 * k):
                for i in range(min(k, n - j - k)):
                    if (i + j) // (2 * p) == (i + j + k) // (2 * p):
                        pairs.append((i + j, i + j + k))
            k //= 2
        p *= 2
    return pairs


SORT32 = batcher(32)
SORT16 = batcher(16)
AHEAD = 2


def wire(ref, base, i):
    return ref[pl.ds(pl.multiple_of((base + i) * 8, 8), 8), :]


def put(ref, base, i, value):
    ref[pl.ds(pl.multiple_of((base + i) * 8, 8), 8), :] = value


def sort32(ref, base):
    v = [wire(ref, base, i) for i in range(32)]
    for i, j in SORT32:
        v[i], v[j] = jnp.maximum(v[i], v[j]), jnp.minimum(v[i], v[j])
    for i in range(32):
        put(ref, base, i, v[i])


def clean(v):
    n = len(v)
    step = n // 2
    while step:
        for i in range(n):
            if not i & step:
                v[i], v[i + step] = jnp.maximum(v[i], v[i + step]), jnp.minimum(v[i], v[i + step])
        step //= 2
    return v


def clean_at(ref, base):
    v = clean([wire(ref, base, i) for i in range(32)])
    for i in range(32):
        put(ref, base, i, v[i])


def merge64(src, base, dst):
    for op, at in ((jnp.maximum, 0), (jnp.minimum, 32)):
        v = clean([op(wire(src, base, i), wire(src, base, 63 - i)) for i in range(32)])
        for i in range(32):
            put(dst, base + at, i, v[i])


def merge128(src, base, dst):
    for op, at in ((jnp.maximum, 0), (jnp.minimum, 64)):
        v = []
        for i in range(32):
            a = op(wire(src, base, i), wire(src, base, 127 - i))
            b = op(wire(src, base, i + 32), wire(src, base, 95 - i))
            v.append(jnp.maximum(a, b))
            put(dst, base + at + 32, i, jnp.minimum(a, b))
        v = clean(v)
        for i in range(32):
            put(dst, base + at, i, v[i])
        clean_at(dst, base + at + 32)


def merge_top(a, a_base, b, b_base, dst, dst_base, turn=0):
    def other(i):
        value = wire(b, b_base, 127 - i)
        return pltpu.roll(value, turn, 0) if turn else value

    v = []
    for i in range(32):
        c = [jnp.maximum(wire(a, a_base, i + 32 * k), other(i + 32 * k)) for k in range(4)]
        f0, g0 = jnp.maximum(c[0], c[2]), jnp.minimum(c[0], c[2])
        f1, g1 = jnp.maximum(c[1], c[3]), jnp.minimum(c[1], c[3])
        v.append(jnp.maximum(f0, f1))
        put(dst, dst_base + 32, i, jnp.minimum(f0, f1))
        put(dst, dst_base + 64, i, jnp.maximum(g0, g1))
        put(dst, dst_base + 96, i, jnp.minimum(g0, g1))
    v = clean(v)
    for i in range(32):
        put(dst, dst_base, i, v[i])

    def rest(k, carry):
        clean_at(dst, dst_base + 32 + 32 * k)
        return carry

    lax.fori_loop(0, 3, rest, 0)


def loop(n, body):
    def step(i, carry):
        body(i)
        return carry

    lax.fori_loop(0, n, step, 0)


def wires_of(corpus, rows, parts, i, whole=False):
    blocks = rows.shape[0] // 128
    apart, nth, kind = (256, i, 0) if blocks == 2 else (128, i // 2, i % 2 * 4)
    starts = [(kind + k) * apart + nth * 64 for k in range(4)]
    scores = lax.dot_general(
        jnp.concatenate([corpus[at : at + 64, :] for at in starts], axis=0),
        rows,
        (((1,), (1,)), ((), ())),
        preferred_element_type=jnp.float32,
    )
    ref, at = (parts, nth * 512) if whole else (parts[nth], 0)
    for k in range(4):
        for half in range(blocks):
            place = pl.ds(at + (kind + k) * blocks + half, 64, stride=8)
            ref[place, :] = scores[k * 64 : (k + 1) * 64, half * 128 : (half + 1) * 128]


def score(corpus, rows, s):
    for i in range(4):
        wires_of(corpus, rows, s, i, whole=True)


def order(blocks, s, u, dst):
    loop(4 * blocks, lambda i: sort32(s, i * 32))
    loop(2 * blocks, lambda i: merge64(s, i * 64, u))
    if blocks == 1:
        merge128(u, 0, dst)
    else:
        loop(2, lambda i: merge128(u, i * 128, s))
        merge_top(s, 0, s, 128, dst, 0)


def network(v, pairs):
    for i, j in pairs:
        v[i], v[j] = jnp.maximum(v[i], v[j]), jnp.minimum(v[i], v[j])
    return v


def best16(ref, base):
    a = network([wire(ref, base, i) for i in range(16)], SORT16)
    b = network([wire(ref, base, i) for i in range(16, 32)], SORT16)
    return clean([jnp.maximum(a[i], b[15 - i]) for i in range(16)])


def shorten(src, base, dst, dst_base):
    a = best16(src, base)
    b = best16(src, base + 32)
    peak = jnp.maximum(a[15], b[15])
    high = clean([jnp.maximum(a[i], b[15 - i]) for i in range(16)])
    low = clean([jnp.minimum(a[i], b[15 - i]) for i in range(16)])
    for i in range(16):
        put(dst, dst_base, i, high[i])
        put(dst, dst_base, 16 + i, low[i])
    return peak


def best32(src, base, dst, dst_base):
    v = clean([jnp.maximum(wire(src, base, i), wire(src, base, 63 - i)) for i in range(32)])
    for i in range(32):
        put(dst, dst_base, i, v[i])
    return v[31]


def best64(src, dst, turn=0):
    def other(i):
        return pltpu.roll(wire(src, 0, 63 - i), turn, 0) if turn else wire(src, 0, 127 - i)

    v = []
    for i in range(32):
        a = jnp.maximum(wire(src, 0, i), other(i))
        b = jnp.maximum(wire(src, 0, i + 32), other(i + 32))
        v.append(jnp.maximum(a, b))
        put(dst, 32, i, jnp.minimum(a, b))
    v = clean(v)
    for i in range(32):
        put(dst, 0, i, v[i])
    clean_at(dst, 32)
    return wire(dst, 63, 0)


def merge_turned(src, dst, turn):
    for op, at in ((jnp.maximum, 0), (jnp.minimum, 64)):
        v = []
        for i in range(32):
            a = op(wire(src, 0, i), pltpu.roll(wire(src, 0, 63 - i), turn, 0))
            b = op(wire(src, 0, i + 32), pltpu.roll(wire(src, 0, 31 - i), turn, 0))
            v.append(jnp.maximum(a, b))
            put(dst, at + 32, i, jnp.minimum(a, b))
        v = clean(v)
        for i in range(32):
            put(dst, at, i, v[i])
        clean_at(dst, at + 32)


def leaders(groups, own, far, *work, emit):
    near_parts, far_parts, (s, u, w) = work[:4], work[4:8], work[8:]
    sides = (near_parts, far_parts)
    parts = [(g, side, i) for g in range(len(groups)) for side in range(2) for i in range(4)]

    def scored(k):
        if k < len(parts):
            g, side, i = parts[k]
            wires_of((own, far)[side](), groups[g][1](), sides[side], i)

    for k in range(AHEAD):
        scored(k)
    peak = None
    for k, (g, side, i) in enumerate(parts):
        scored(k + AHEAD)
        blocks = groups[g][0]
        if blocks == 2 or i % 2 == 1:
            nth = i if blocks == 2 else i // 2
            now = shorten(sides[side][nth], 0, u, side * 64 * blocks + nth * 32)
            peak = now if peak is None else jnp.maximum(peak, now)
        if side == 0 or i < 3:
            continue
        for j in range(2 * blocks):
            peak = jnp.maximum(peak, best32(u, j * 64, w, j * 32))
        if blocks == 2:
            loop(2, lambda j: merge64(w, j * 64, u))
            peak = jnp.maximum(peak, best64(u, w))
            turns = (4, 2)
        else:
            merge64(w, 0, u)
            peak = jnp.maximum(peak, best64(u, w, turn=4))
            turns = (2, 1)
        merge_turned(w, u, turns[0])
        merge_top(u, 0, u, 0, w, 0, turn=turns[1])
        for turn in (4, 2, 1)[: 4 - blocks]:
            peak = jnp.maximum(peak, pltpu.roll(peak, turn, 0))
        unsure = jnp.max(jnp.where(peak > wire(w, 127, 0), 1.0, 0.0)) > 0.0
        peak = None

        @pl.when(unsure)
        def _():
            long_way(blocks, groups[g][1](), own(), far(), s, u, w)

        for half in range(blocks):
            emit(g, half, w[pl.ds(half, TOPK, stride=8), :].T)


def long_way(blocks, rows, own, far, s, u, w):
    score(own, rows, s)
    order(blocks, s, u, w)
    score(far, rows, s)
    if blocks == 2:
        order(blocks, s, u, u)
        merge_top(w, 0, u, 0, s, 0)
        merge_top(s, 0, s, 0, u, 0, turn=4)
        merge_top(u, 0, u, 0, w, 0, turn=2)
    else:
        loop(4, lambda i: sort32(s, i * 32))
        loop(2, lambda i: merge64(s, i * 64, u))
        merge128(u, 0, s)
        merge_top(w, 0, s, 0, u, 0)
        merge_top(u, 0, u, 0, s, 0, turn=4)
        merge_top(s, 0, s, 0, u, 0, turn=2)
        merge_top(u, 0, u, 0, w, 0, turn=1)


def main_rows(chunk):
    return jnp.concatenate(
        [chunk[:, c * MAIN : (c + 1) * MAIN, :].reshape(-1, 128) for c in range(COLS)], axis=1
    )


def tail_rows(chunk):
    langs = chunk.shape[0]
    many, each = langs * TAIL, TAIL * COLS
    shape, total = (COLS, many, langs * each), langs * each
    col, row, at = (lax.broadcasted_iota(jnp.int32, shape, d) for d in range(3))
    from_row = lax.shift_right_logical(row, 2) * each + col * TAIL + (row & 3)
    picks = jnp.where(at == from_row, 1.0, 0.0).astype(jnp.bfloat16).reshape(total, total)
    flat = chunk[:, MAIN * COLS : SENT, :].reshape(total, 128)
    found = jnp.dot(picks, flat, preferred_element_type=jnp.float32).astype(jnp.bfloat16)
    return jnp.concatenate([found[c * many : (c + 1) * many, :] for c in range(COLS)], axis=1)


def first_kernel(chunk, own, far_in, out, far, rows, sem, *work):
    copy = pltpu.make_async_copy(far_in, far, sem)
    copy.start()
    rows[...] = main_rows(chunk)
    waited = []

    def partner():
        if not waited:
            copy.wait()
            waited.append(True)
        return far

    def emit(g, half, value):
        out[half * Q : (half + 1) * Q, :] = value

    leaders([(2, lambda: rows[...])], lambda: own, partner, *work, emit=emit)


def early_kernel(half0, half1, own, far, out, rows, *work):
    rows[0:128, :] = main_rows(half0)
    rows[128:256, :] = main_rows(half1)

    def emit(g, half, value):
        out[half * Q : (half + 1) * Q, :] = value

    leaders([(2, lambda: rows[...])], lambda: own, lambda: far, *work, emit=emit)


def middle_kernel(mine, cx0, cx1, cy0, cy1, own, far, out, tails, rows, *work):
    rows[0:128, :] = main_rows(cx1)
    rows[128:256, :] = main_rows(cy1)
    rows[256:320, :] = tail_rows(mine)
    for k, chunk in enumerate((cx0, cx1, cy0, cy1)):
        rows[320 + k * 32 : 352 + k * 32, :] = tail_rows(chunk)
    rows[448:512, :] = jnp.zeros((64, WIDTH), jnp.bfloat16)

    def emit(g, half, value):
        (out, tails)[g][half * Q : (half + 1) * Q, :] = value

    leaders(
        [(2, lambda: rows[0:256, :]), (2, lambda: rows[256:512, :])], lambda: own, lambda: far, *work, emit=emit
    )


STEPS = 800.0
FLOOR = 32.5
LN2 = 0.6931471805599453


def coded(v):
    level = jnp.round(jnp.log(jnp.abs(v)) * (STEPS / LN2) + STEPS * FLOOR)
    level = jnp.clip(level, 0.0, 32767.0)
    return jnp.where(v < 0, -level, level)


def decoded(c):
    level = jnp.abs(c)
    v = jnp.where(level > 0, jnp.exp(level * (LN2 / STEPS) - FLOOR * LN2), 0.0)
    return jnp.where(c < 0, -v, v)


def late_kernel(at, cd0, cd1, own, far, r0, r1, r2, tails, keep, give, rows, last, box, *work):
    rows[0:128, :] = main_rows(cd0)
    rows[128:256, :] = main_rows(cd1)
    rows[256:288, :] = tail_rows(cd0)
    rows[288:320, :] = tail_rows(cd1)
    rows[320:384, :] = jnp.zeros((64, WIDTH), jnp.bfloat16)

    def emit(g, half, value):
        last[g * 256 + half * Q : g * 256 + (half + 1) * Q, :] = value

    leaders(
        [(2, lambda: rows[0:256, :]), (1, lambda: rows[256:384, :])], lambda: own, lambda: far, *work, emit=emit
    )
    me, side = at[0], at[1].astype(jnp.float32)
    owner = (me, me ^ 1, me ^ 2, me ^ 3)
    none = jnp.zeros((ROWS - CAP, TOPK), jnp.float32)
    for k in range(4):
        for lang in range(LANGS):
            half, start = lang // 8, lang % 8 * MAIN
            if k == 0:
                main = r0[lang * MAIN : (lang + 1) * MAIN, :]
            elif k < 3:
                start += (k - 1) * Q
                main = (r1, r2)[half][start : start + MAIN, :]
            else:
                main = last[lang * MAIN : (lang + 1) * MAIN, :]
            here = 2 * k + lang % 2
            box[here, 0:MAIN, :] = main
            start = k * 64 + lang * TAIL
            if k < 3:
                box[here, MAIN:CAP, :] = tails[start : start + TAIL, :]
            else:
                box[here, MAIN:CAP, :] = last[256 + lang * TAIL : 256 + (lang + 1) * TAIL, :]
            box[here, CAP:ROWS, :] = none
            if lang % 2 == 1:
                even, odd = coded(box[2 * k]), coded(box[2 * k + 1])
                shift = (odd - even) * side
                keep[lang // 2, owner[k], 0] = (even + shift).astype(jnp.int32).astype(jnp.int16)
                give[lang // 2, owner[k]] = (odd - shift).astype(jnp.int32).astype(jnp.int16)


COST = 2 * 256 * 2048 * 768 * 8
VMEM = pl.BlockSpec(memory_space=pltpu.VMEM)
LIMIT = pltpu.CompilerParams(vmem_limit_bytes=14 << 20)
WORK = [pltpu.VMEM((64 * 8, 128), jnp.float32)] * 8 + [
    pltpu.VMEM((256 * 8, 128), jnp.float32),
    pltpu.VMEM((256 * 8, 128), jnp.float32),
    pltpu.VMEM((128 * 8, 128), jnp.float32),
]


def first(chunk, own, far):
    return pl.pallas_call(
        first_kernel,
        out_shape=(
            jax.ShapeDtypeStruct((256, TOPK), jnp.float32),
            jax.ShapeDtypeStruct((1024, WIDTH), jnp.bfloat16),
        ),
        in_specs=[VMEM, VMEM, pl.BlockSpec(memory_space=pl.ANY)],
        out_specs=(VMEM, VMEM),
        scratch_shapes=[pltpu.VMEM((256, WIDTH), jnp.bfloat16), pltpu.SemaphoreType.DMA] + WORK,
        compiler_params=LIMIT,
        cost_estimate=pl.CostEstimate(flops=COST, bytes_accessed=1 << 20, transcendentals=0),
        name="first",
    )(chunk, own, far)


def early(half0, half1, own, far):
    return pl.pallas_call(
        early_kernel,
        out_shape=jax.ShapeDtypeStruct((256, TOPK), jnp.float32),
        in_specs=[VMEM] * 4,
        out_specs=VMEM,
        scratch_shapes=[pltpu.VMEM((256, WIDTH), jnp.bfloat16)] + WORK,
        compiler_params=LIMIT,
        cost_estimate=pl.CostEstimate(flops=COST, bytes_accessed=1 << 20, transcendentals=0),
        name="early",
    )(half0, half1, own, far)


def middle(mine, halves, own, far):
    return pl.pallas_call(
        middle_kernel,
        out_shape=[jax.ShapeDtypeStruct((256, TOPK), jnp.float32)] * 2,
        in_specs=[VMEM] * 7,
        out_specs=[VMEM] * 2,
        scratch_shapes=[pltpu.VMEM((512, WIDTH), jnp.bfloat16)] + WORK,
        compiler_params=LIMIT,
        cost_estimate=pl.CostEstimate(flops=COST * 2, bytes_accessed=1 << 20, transcendentals=0),
        name="middle",
    )(mine, *halves, own, far)


def late(at, halves, own, far, results):
    return pl.pallas_call(
        late_kernel,
        out_shape=(
            jax.ShapeDtypeStruct((LANGS // 2, 4, 2, ROWS, TOPK), jnp.int16),
            jax.ShapeDtypeStruct((LANGS // 2, 4, ROWS, TOPK), jnp.int16),
        ),
        in_specs=[pl.BlockSpec(memory_space=pltpu.SMEM)] + [VMEM] * 8,
        out_specs=(VMEM, VMEM),
        scratch_shapes=[
            pltpu.VMEM((384, WIDTH), jnp.bfloat16),
            pltpu.VMEM((384, TOPK), jnp.float32),
            pltpu.VMEM((8, ROWS, TOPK), jnp.float32),
        ]
        + WORK,
        compiler_params=LIMIT,
        cost_estimate=pl.CostEstimate(flops=COST * 2, bytes_accessed=1 << 20, transcendentals=0),
        name="late",
    )(at, *halves, own, far, *results)


def outbox_kernel(queries_in, routes_in, out, slots, queries, routes, sems):
    copies = (
        pltpu.make_async_copy(routes_in, routes, sems.at[0]),
        pltpu.make_async_copy(queries_in, queries, sems.at[1]),
    )
    for copy in copies:
        copy.start()
    for copy in copies:
        copy.wait()
    x = queries[...].astype(jnp.float32)
    unit = (x * lax.rsqrt(jnp.mean(x * x, axis=1, keepdims=True) + epsilon)).astype(jnp.bfloat16)
    along = jnp.broadcast_to(routes[...].astype(jnp.float32), (Q, Q))
    down = along.T
    before = lax.broadcasted_iota(jnp.int32, (Q, Q), 0) < lax.broadcasted_iota(jnp.int32, (Q, Q), 1)
    earlier = jnp.where(before & (along == down), 1.0, 0.0)
    rank = jnp.sum(earlier, axis=0, keepdims=True).astype(jnp.int32)
    lang = routes[...]
    for side in range(2):
        slots[side] = (lang ^ side) * ROWS + rank
    main_at = jnp.where(rank < MAIN, lang * MAIN + rank, -1)
    hits = lax.broadcasted_iota(jnp.int32, (LANGS * MAIN, Q), 0) == jnp.broadcast_to(main_at, (LANGS * MAIN, Q))
    picks = jnp.where(hits, 1.0, 0.0).astype(jnp.bfloat16)
    box = jnp.dot(picks, unit, preferred_element_type=jnp.float32).astype(jnp.bfloat16)
    for c in range(COLS):
        out[:, c * MAIN : (c + 1) * MAIN, :] = box[:, c * 128 : (c + 1) * 128].reshape(LANGS, MAIN, 128)
    each = TAIL * COLS
    tail_at = jnp.where(rank < MAIN, -1, lang * TAIL + rank - MAIN)
    shape = (LANGS, each, Q)
    of_lang, row = (lax.broadcasted_iota(jnp.int32, shape, d) for d in range(2))
    hits = of_lang * TAIL + (row & 3) == jnp.broadcast_to(tail_at.reshape(1, 1, Q), shape)
    tail = jnp.zeros((LANGS * each, 128), jnp.float32)
    for c in range(COLS):
        picks = jnp.where(hits & (lax.shift_right_logical(row, 2) == c), 1.0, 0.0)
        picks = picks.astype(jnp.bfloat16).reshape(LANGS * each, Q)
        tail = tail + jnp.dot(picks, unit[:, c * 128 : (c + 1) * 128], preferred_element_type=jnp.float32)
    out[:, MAIN * COLS : SENT, :] = tail.astype(jnp.bfloat16).reshape(LANGS, each, 128)


def outbox_of(queries, routes):
    return pl.pallas_call(
        outbox_kernel,
        out_shape=(
            jax.ShapeDtypeStruct((LANGS, SENT, 128), jnp.bfloat16),
            jax.ShapeDtypeStruct((2, 1, Q), jnp.int32),
        ),
        in_specs=[pl.BlockSpec(memory_space=pltpu.HBM)] * 2,
        out_specs=(VMEM, VMEM),
        scratch_shapes=[
            pltpu.VMEM((Q, WIDTH), jnp.bfloat16),
            pltpu.VMEM((1, Q), jnp.int32),
            pltpu.SemaphoreType.DMA((2,)),
        ],
        compiler_params=pltpu.CompilerParams(vmem_limit_bytes=60 << 20),
        name="outbox",
    )(queries, routes)


def join_kernel(at, back, slots, out, a, b):
    total = LANGS * ROWS
    hits = lax.broadcasted_iota(jnp.int32, (total, Q), 0) == jnp.broadcast_to(slots[at[1]], (total, Q))
    picks = jnp.where(hits, 1.0, 0.0)
    picks = jnp.concatenate([picks[i * Q : (i + 1) * Q, :].T for i in range(total // Q)], axis=1)
    picks = picks.astype(jnp.bfloat16)
    for k in range(4):
        code = back[:, k].astype(jnp.int32).astype(jnp.float32).reshape(total, TOPK)
        high = code.astype(jnp.bfloat16)
        low = (code - high.astype(jnp.float32)).astype(jnp.bfloat16)
        rows = jnp.dot(picks, high, preferred_element_type=jnp.float32) + jnp.dot(
            picks, low, preferred_element_type=jnp.float32
        )
        ranks = decoded(rows).T
        a[pl.ds(k, TOPK, stride=8), :] = ranks
        a[pl.ds(k + 4, TOPK, stride=8), :] = ranks
    merge_top(a, 0, a, 0, b, 0, turn=2)
    merge_top(b, 0, b, 0, a, 0, turn=1)
    out[...] = a[pl.ds(0, TOPK, stride=8), :].T


def join(at, back, slots):
    return pl.pallas_call(
        join_kernel,
        out_shape=jax.ShapeDtypeStruct((Q, TOPK), jnp.float32),
        in_specs=[pl.BlockSpec(memory_space=pltpu.SMEM)] + [VMEM] * 2,
        out_specs=VMEM,
        scratch_shapes=[pltpu.VMEM((128 * 8, 128), jnp.float32)] * 2,
        compiler_params=LIMIT,
        name="join",
    )(at, back, slots)


AXES = ("lang", "shard")


def moves(target):
    return [
        (lang * 8 + y * 4 + x, lang * 8 + ty * 4 + tx % 4)
        for lang in range(16)
        for y in range(2)
        for x in range(4)
        for ty, tx in (target(lang % 2, y, x),)
    ]


def pair(core, y, x):
    return y, x + (1 if (x + core) % 2 == 0 else -1)


def over_x(core, y, x):
    return y, x + 2


def over_y(core, y, x):
    return 1 - y, x


TEAMS = [
    [lang * 8 + y * 4 + odd + 2 * half for lang in range(core, 16, 2) for y in range(2) for half in range(2)]
    for core in range(2)
    for odd in range(2)
]


def shards(queries, routes, corpus):
    far = lax.ppermute(corpus, AXES, moves(pair))
    outbox, slots = outbox_of(queries, routes.reshape(1, Q))
    mine = lax.all_to_all(outbox, "lang", split_axis=0, concat_axis=0, tiled=True)
    cx0, cy0, cx1, cy1 = (
        lax.ppermute(part, AXES, moves(over)) for part in (mine[:8], mine[8:]) for over in (over_x, over_y)
    )
    r0, far = first(mine, corpus, far)
    cx0, cy0, r0 = lax.optimization_barrier((cx0, cy0, r0))
    cd0 = lax.ppermute(cx0, AXES, moves(over_y))
    r1 = early(cx0, cy0, corpus, far)
    cx1, cy1, r1 = lax.optimization_barrier((cx1, cy1, r1))
    cd1 = lax.ppermute(cy1, AXES, moves(over_x))
    r2, tails = middle(mine, (cx0, cx1, cy0, cy1), corpus, far)
    shard, core = lax.axis_index("shard"), lax.axis_index("lang") & 1
    seat = lax.shift_right_logical(shard, 2) * 2 + (lax.shift_right_logical(shard, 1) & 1)
    at = jnp.stack([seat, core])
    keep, give = late(at, (cd0, cd1), corpus, far, (r0, r1, r2, tails))
    other = lax.ppermute(give, AXES, [(d, d ^ 8) for d in range(128)])
    sent = lax.dynamic_update_slice(keep, other[:, :, None], (0, 0, 1, 0, 0))
    sent = sent.reshape(LANGS * 2, 2 * ROWS, TOPK)
    back = lax.all_to_all(sent, AXES, 0, 0, axis_index_groups=TEAMS, tiled=True)
    return join(at, back.reshape(LANGS // 2, 4, 2 * ROWS, TOPK), slots)


def solution(mesh):
    placed = (P(AXES, None), P(AXES, None), P(AXES, None))
    return jax.shard_map(shards, mesh=mesh, in_specs=placed, out_specs=P(AXES, None), check_vma=False)
```

```python
import functools

import jax
import jax.numpy as jnp
from jax import lax
from jax.experimental import pallas as pl
from jax.experimental.pallas import tpu as pltpu
from jax.sharding import PartitionSpec as P

TOPK = 128
LANGS = 16
CAP = 20
ROWS = 24
MAIN = 16
TAIL = CAP - MAIN
Q = 128
WIDTH = 768
COLS = WIDTH // 128
SENT = CAP * COLS

epsilon = 1e-06


def batcher(n):
    pairs = []
    p = 1
    while p < n:
        k = p
        while k >= 1:
            for j in range(k % p, n - k, 2 * k):
                for i in range(min(k, n - j - k)):
                    if (i + j) // (2 * p) == (i + j + k) // (2 * p):
                        pairs.append((i + j, i + j + k))
            k //= 2
        p *= 2
    return pairs


SORT32 = batcher(32)
SORT16 = batcher(16)
AHEAD = 2


def wire(ref, base, i):
    return ref[pl.ds(pl.multiple_of((base + i) * 8, 8), 8), :]


def put(ref, base, i, value):
    ref[pl.ds(pl.multiple_of((base + i) * 8, 8), 8), :] = value


def sort32(ref, base):
    v = [wire(ref, base, i) for i in range(32)]
    for i, j in SORT32:
        v[i], v[j] = jnp.maximum(v[i], v[j]), jnp.minimum(v[i], v[j])
    for i in range(32):
        put(ref, base, i, v[i])


def clean(v):
    n = len(v)
    step = n // 2
    while step:
        for i in range(n):
            if not i & step:
                v[i], v[i + step] = jnp.maximum(v[i], v[i + step]), jnp.minimum(v[i], v[i + step])
        step //= 2
    return v


def clean_at(ref, base):
    v = clean([wire(ref, base, i) for i in range(32)])
    for i in range(32):
        put(ref, base, i, v[i])


def merge64(src, base, dst):
    for op, at in ((jnp.maximum, 0), (jnp.minimum, 32)):
        v = clean([op(wire(src, base, i), wire(src, base, 63 - i)) for i in range(32)])
        for i in range(32):
            put(dst, base + at, i, v[i])


def merge128(src, base, dst):
    for op, at in ((jnp.maximum, 0), (jnp.minimum, 64)):
        v = []
        for i in range(32):
            a = op(wire(src, base, i), wire(src, base, 127 - i))
            b = op(wire(src, base, i + 32), wire(src, base, 95 - i))
            v.append(jnp.maximum(a, b))
            put(dst, base + at + 32, i, jnp.minimum(a, b))
        v = clean(v)
        for i in range(32):
            put(dst, base + at, i, v[i])
        clean_at(dst, base + at + 32)


def merge_top(a, a_base, b, b_base, dst, dst_base, turn=0):
    def other(i):
        value = wire(b, b_base, 127 - i)
        return pltpu.roll(value, turn, 0) if turn else value

    v = []
    for i in range(32):
        c = [jnp.maximum(wire(a, a_base, i + 32 * k), other(i + 32 * k)) for k in range(4)]
        f0, g0 = jnp.maximum(c[0], c[2]), jnp.minimum(c[0], c[2])
        f1, g1 = jnp.maximum(c[1], c[3]), jnp.minimum(c[1], c[3])
        v.append(jnp.maximum(f0, f1))
        put(dst, dst_base + 32, i, jnp.minimum(f0, f1))
        put(dst, dst_base + 64, i, jnp.maximum(g0, g1))
        put(dst, dst_base + 96, i, jnp.minimum(g0, g1))
    v = clean(v)
    for i in range(32):
        put(dst, dst_base, i, v[i])

    def rest(k, carry):
        clean_at(dst, dst_base + 32 + 32 * k)
        return carry

    lax.fori_loop(0, 3, rest, 0)


def loop(n, body):
    def step(i, carry):
        body(i)
        return carry

    lax.fori_loop(0, n, step, 0)


def wires_of(corpus, rows, parts, i, whole=False):
    blocks = rows.shape[0] // 128
    apart, nth, kind = (256, i, 0) if blocks == 2 else (128, i // 2, i % 2 * 4)
    starts = [(kind + k) * apart + nth * 64 for k in range(4)]
    scores = lax.dot_general(
        jnp.concatenate([corpus[at : at + 64, :] for at in starts], axis=0),
        rows,
        (((1,), (1,)), ((), ())),
        preferred_element_type=jnp.float32,
    )
    ref, at = (parts, nth * 512) if whole else (parts[nth], 0)
    for k in range(4):
        for half in range(blocks):
            place = pl.ds(at + (kind + k) * blocks + half, 64, stride=8)
            ref[place, :] = scores[k * 64 : (k + 1) * 64, half * 128 : (half + 1) * 128]


def score(corpus, rows, s):
    for i in range(4):
        wires_of(corpus, rows, s, i, whole=True)


def order(blocks, s, u, dst):
    loop(4 * blocks, lambda i: sort32(s, i * 32))
    loop(2 * blocks, lambda i: merge64(s, i * 64, u))
    if blocks == 1:
        merge128(u, 0, dst)
    else:
        loop(2, lambda i: merge128(u, i * 128, s))
        merge_top(s, 0, s, 128, dst, 0)


def network(v, pairs):
    for i, j in pairs:
        v[i], v[j] = jnp.maximum(v[i], v[j]), jnp.minimum(v[i], v[j])
    return v


def best16(ref, base):
    a = network([wire(ref, base, i) for i in range(16)], SORT16)
    b = network([wire(ref, base, i) for i in range(16, 32)], SORT16)
    return clean([jnp.maximum(a[i], b[15 - i]) for i in range(16)])


def shorten(src, base, dst, dst_base):
    a = best16(src, base)
    b = best16(src, base + 32)
    peak = jnp.maximum(a[15], b[15])
    high = clean([jnp.maximum(a[i], b[15 - i]) for i in range(16)])
    low = clean([jnp.minimum(a[i], b[15 - i]) for i in range(16)])
    for i in range(16):
        put(dst, dst_base, i, high[i])
        put(dst, dst_base, 16 + i, low[i])
    return peak


def best32(src, base, dst, dst_base):
    v = clean([jnp.maximum(wire(src, base, i), wire(src, base, 63 - i)) for i in range(32)])
    for i in range(32):
        put(dst, dst_base, i, v[i])
    return v[31]


def best64(src, dst, turn=0):
    def other(i):
        return pltpu.roll(wire(src, 0, 63 - i), turn, 0) if turn else wire(src, 0, 127 - i)

    v = []
    for i in range(32):
        a = jnp.maximum(wire(src, 0, i), other(i))
        b = jnp.maximum(wire(src, 0, i + 32), other(i + 32))
        v.append(jnp.maximum(a, b))
        put(dst, 32, i, jnp.minimum(a, b))
    v = clean(v)
    for i in range(32):
        put(dst, 0, i, v[i])
    clean_at(dst, 32)
    return wire(dst, 63, 0)


def merge_turned(src, dst, turn):
    for op, at in ((jnp.maximum, 0), (jnp.minimum, 64)):
        v = []
        for i in range(32):
            a = op(wire(src, 0, i), pltpu.roll(wire(src, 0, 63 - i), turn, 0))
            b = op(wire(src, 0, i + 32), pltpu.roll(wire(src, 0, 31 - i), turn, 0))
            v.append(jnp.maximum(a, b))
            put(dst, at + 32, i, jnp.minimum(a, b))
        v = clean(v)
        for i in range(32):
            put(dst, at, i, v[i])
        clean_at(dst, at + 32)


def leaders(groups, own, far, *work, emit):
    near_parts, far_parts, (s, u, w) = work[:4], work[4:8], work[8:]
    sides = (near_parts, far_parts)
    parts = [(g, side, i) for g in range(len(groups)) for side in range(2) for i in range(4)]

    def scored(k):
        if k < len(parts):
            g, side, i = parts[k]
            wires_of((own, far)[side](), groups[g][1](), sides[side], i)

    for k in range(AHEAD):
        scored(k)
    peak = None
    for k, (g, side, i) in enumerate(parts):
        scored(k + AHEAD)
        blocks = groups[g][0]
        if blocks == 2 or i % 2 == 1:
            nth = i if blocks == 2 else i // 2
            now = shorten(sides[side][nth], 0, u, side * 64 * blocks + nth * 32)
            peak = now if peak is None else jnp.maximum(peak, now)
        if side == 0 or i < 3:
            continue
        for j in range(2 * blocks):
            peak = jnp.maximum(peak, best32(u, j * 64, w, j * 32))
        if blocks == 2:
            loop(2, lambda j: merge64(w, j * 64, u))
            peak = jnp.maximum(peak, best64(u, w))
            turns = (4, 2)
        else:
            merge64(w, 0, u)
            peak = jnp.maximum(peak, best64(u, w, turn=4))
            turns = (2, 1)
        merge_turned(w, u, turns[0])
        merge_top(u, 0, u, 0, w, 0, turn=turns[1])
        for turn in (4, 2, 1)[: 4 - blocks]:
            peak = jnp.maximum(peak, pltpu.roll(peak, turn, 0))
        unsure = jnp.max(jnp.where(peak > wire(w, 127, 0), 1.0, 0.0)) > 0.0
        peak = None

        @pl.when(unsure)
        def _():
            long_way(blocks, groups[g][1](), own(), far(), s, u, w)

        for half in range(blocks):
            emit(g, half, w[pl.ds(half, TOPK, stride=8), :].T)


def long_way(blocks, rows, own, far, s, u, w):
    score(own, rows, s)
    order(blocks, s, u, w)
    score(far, rows, s)
    if blocks == 2:
        order(blocks, s, u, u)
        merge_top(w, 0, u, 0, s, 0)
        merge_top(s, 0, s, 0, u, 0, turn=4)
        merge_top(u, 0, u, 0, w, 0, turn=2)
    else:
        loop(4, lambda i: sort32(s, i * 32))
        loop(2, lambda i: merge64(s, i * 64, u))
        merge128(u, 0, s)
        merge_top(w, 0, s, 0, u, 0)
        merge_top(u, 0, u, 0, s, 0, turn=4)
        merge_top(s, 0, s, 0, u, 0, turn=2)
        merge_top(u, 0, u, 0, w, 0, turn=1)


def main_rows(chunk):
    return jnp.concatenate(
        [chunk[:, c * MAIN : (c + 1) * MAIN, :].reshape(-1, 128) for c in range(COLS)], axis=1
    )


def tail_rows(chunk):
    langs = chunk.shape[0]
    many, each = langs * TAIL, TAIL * COLS
    shape, total = (COLS, many, langs * each), langs * each
    col, row, at = (lax.broadcasted_iota(jnp.int32, shape, d) for d in range(3))
    from_row = lax.shift_right_logical(row, 2) * each + col * TAIL + (row & 3)
    picks = jnp.where(at == from_row, 1.0, 0.0).astype(jnp.bfloat16).reshape(total, total)
    flat = chunk[:, MAIN * COLS : SENT, :].reshape(total, 128)
    found = jnp.dot(picks, flat, preferred_element_type=jnp.float32).astype(jnp.bfloat16)
    return jnp.concatenate([found[c * many : (c + 1) * many, :] for c in range(COLS)], axis=1)


def first_kernel(chunk, own, far_in, out, far, rows, sem, *work):
    copy = pltpu.make_async_copy(far_in, far, sem)
    copy.start()
    rows[...] = main_rows(chunk)
    waited = []

    def partner():
        if not waited:
            copy.wait()
            waited.append(True)
        return far

    def emit(g, half, value):
        out[half * Q : (half + 1) * Q, :] = value

    leaders([(2, lambda: rows[...])], lambda: own, partner, *work, emit=emit)


def early_kernel(half0, half1, own, far, out, rows, *work):
    rows[0:128, :] = main_rows(half0)
    rows[128:256, :] = main_rows(half1)

    def emit(g, half, value):
        out[half * Q : (half + 1) * Q, :] = value

    leaders([(2, lambda: rows[...])], lambda: own, lambda: far, *work, emit=emit)


def middle_kernel(mine, cx0, cx1, cy0, cy1, own, far, out, tails, rows, *work):
    rows[0:128, :] = main_rows(cx1)
    rows[128:256, :] = main_rows(cy1)
    rows[256:320, :] = tail_rows(mine)
    for k, chunk in enumerate((cx0, cx1, cy0, cy1)):
        rows[320 + k * 32 : 352 + k * 32, :] = tail_rows(chunk)
    rows[448:512, :] = jnp.zeros((64, WIDTH), jnp.bfloat16)

    def emit(g, half, value):
        (out, tails)[g][half * Q : (half + 1) * Q, :] = value

    leaders(
        [(2, lambda: rows[0:256, :]), (2, lambda: rows[256:512, :])], lambda: own, lambda: far, *work, emit=emit
    )


STEPS = 800.0
FLOOR = 32.5
LN2 = 0.6931471805599453


def coded(v):
    level = jnp.round(jnp.log(jnp.abs(v)) * (STEPS / LN2) + STEPS * FLOOR)
    level = jnp.clip(level, 0.0, 32767.0)
    return jnp.where(v < 0, -level, level)


def decoded(c):
    level = jnp.abs(c)
    v = jnp.where(level > 0, jnp.exp(level * (LN2 / STEPS) - FLOOR * LN2), 0.0)
    return jnp.where(c < 0, -v, v)


def late_kernel(at, cd0, cd1, own, far, r0, r1, r2, tails, out, rows, last, box, *work):
    rows[0:128, :] = main_rows(cd0)
    rows[128:256, :] = main_rows(cd1)
    rows[256:288, :] = tail_rows(cd0)
    rows[288:320, :] = tail_rows(cd1)
    rows[320:384, :] = jnp.zeros((64, WIDTH), jnp.bfloat16)

    def emit(g, half, value):
        last[g * 256 + half * Q : g * 256 + (half + 1) * Q, :] = value

    leaders(
        [(2, lambda: rows[0:256, :]), (1, lambda: rows[256:384, :])], lambda: own, lambda: far, *work, emit=emit
    )
    me = at[0]
    owner = (me, me ^ 2, me ^ 1, me ^ 3)
    none = jnp.zeros((ROWS - CAP, TOPK), jnp.float32)
    for k in range(4):
        for lang in range(LANGS):
            half, start = lang // 8, lang % 8 * MAIN
            if k == 0:
                main = r0[lang * MAIN : (lang + 1) * MAIN, :]
            elif k < 3:
                start += (k - 1) * Q
                main = (r1, r2)[half][start : start + MAIN, :]
            else:
                main = last[lang * MAIN : (lang + 1) * MAIN, :]
            box[k, 0:MAIN, :] = main
            start = k * 64 + lang * TAIL
            if k < 3:
                box[k, MAIN:CAP, :] = tails[start : start + TAIL, :]
            else:
                box[k, MAIN:CAP, :] = last[256 + lang * TAIL : 256 + (lang + 1) * TAIL, :]
            box[k, CAP:ROWS, :] = none
            out[lang % 2, owner[k], lang // 2] = coded(box[k]).astype(jnp.int32).astype(jnp.int16)


COST = 2 * 256 * 2048 * 768 * 8
VMEM = pl.BlockSpec(memory_space=pltpu.VMEM)
LIMIT = pltpu.CompilerParams(vmem_limit_bytes=14 << 20)
WORK = [pltpu.VMEM((64 * 8, 128), jnp.float32)] * 8 + [
    pltpu.VMEM((256 * 8, 128), jnp.float32),
    pltpu.VMEM((256 * 8, 128), jnp.float32),
    pltpu.VMEM((128 * 8, 128), jnp.float32),
]


def first(chunk, own, far):
    return pl.pallas_call(
        first_kernel,
        out_shape=(
            jax.ShapeDtypeStruct((256, TOPK), jnp.float32),
            jax.ShapeDtypeStruct((1024, WIDTH), jnp.bfloat16),
        ),
        in_specs=[VMEM, VMEM, pl.BlockSpec(memory_space=pl.ANY)],
        out_specs=(VMEM, VMEM),
        scratch_shapes=[pltpu.VMEM((256, WIDTH), jnp.bfloat16), pltpu.SemaphoreType.DMA] + WORK,
        compiler_params=LIMIT,
        cost_estimate=pl.CostEstimate(flops=COST, bytes_accessed=1 << 20, transcendentals=0),
        name="first",
    )(chunk, own, far)


def early(half0, half1, own, far):
    return pl.pallas_call(
        early_kernel,
        out_shape=jax.ShapeDtypeStruct((256, TOPK), jnp.float32),
        in_specs=[VMEM] * 4,
        out_specs=VMEM,
        scratch_shapes=[pltpu.VMEM((256, WIDTH), jnp.bfloat16)] + WORK,
        compiler_params=LIMIT,
        cost_estimate=pl.CostEstimate(flops=COST, bytes_accessed=1 << 20, transcendentals=0),
        name="early",
    )(half0, half1, own, far)


def middle(mine, halves, own, far):
    return pl.pallas_call(
        middle_kernel,
        out_shape=[jax.ShapeDtypeStruct((256, TOPK), jnp.float32)] * 2,
        in_specs=[VMEM] * 7,
        out_specs=[VMEM] * 2,
        scratch_shapes=[pltpu.VMEM((512, WIDTH), jnp.bfloat16)] + WORK,
        compiler_params=LIMIT,
        cost_estimate=pl.CostEstimate(flops=COST * 2, bytes_accessed=1 << 20, transcendentals=0),
        name="middle",
    )(mine, *halves, own, far)


def late(at, halves, own, far, results):
    return pl.pallas_call(
        late_kernel,
        out_shape=jax.ShapeDtypeStruct((2, 4, LANGS // 2, ROWS, TOPK), jnp.int16),
        in_specs=[pl.BlockSpec(memory_space=pltpu.SMEM)] + [VMEM] * 8,
        out_specs=VMEM,
        scratch_shapes=[
            pltpu.VMEM((384, WIDTH), jnp.bfloat16),
            pltpu.VMEM((384, TOPK), jnp.float32),
            pltpu.VMEM((4, ROWS, TOPK), jnp.float32),
        ]
        + WORK,
        compiler_params=LIMIT,
        cost_estimate=pl.CostEstimate(flops=COST * 2, bytes_accessed=1 << 20, transcendentals=0),
        name="late",
    )(at, *halves, own, far, *results)


def outbox_kernel(queries_in, routes_in, out, slots, queries, routes, sems):
    copies = (
        pltpu.make_async_copy(routes_in, routes, sems.at[0]),
        pltpu.make_async_copy(queries_in, queries, sems.at[1]),
    )
    for copy in copies:
        copy.start()
    for copy in copies:
        copy.wait()
    x = queries[...].astype(jnp.float32)
    unit = (x * lax.rsqrt(jnp.mean(x * x, axis=1, keepdims=True) + epsilon)).astype(jnp.bfloat16)
    along = jnp.broadcast_to(routes[...].astype(jnp.float32), (Q, Q))
    down = along.T
    before = lax.broadcasted_iota(jnp.int32, (Q, Q), 0) < lax.broadcasted_iota(jnp.int32, (Q, Q), 1)
    earlier = jnp.where(before & (along == down), 1.0, 0.0)
    rank = jnp.sum(earlier, axis=0, keepdims=True).astype(jnp.int32)
    lang = routes[...]
    slots[...] = ((lang & 1) * (LANGS // 2) + lax.shift_right_logical(lang, 1)) * ROWS + rank
    main_at = jnp.where(rank < MAIN, lang * MAIN + rank, -1)
    hits = lax.broadcasted_iota(jnp.int32, (LANGS * MAIN, Q), 0) == jnp.broadcast_to(main_at, (LANGS * MAIN, Q))
    picks = jnp.where(hits, 1.0, 0.0).astype(jnp.bfloat16)
    box = jnp.dot(picks, unit, preferred_element_type=jnp.float32).astype(jnp.bfloat16)
    for c in range(COLS):
        out[:, c * MAIN : (c + 1) * MAIN, :] = box[:, c * 128 : (c + 1) * 128].reshape(LANGS, MAIN, 128)
    each = TAIL * COLS
    tail_at = jnp.where(rank < MAIN, -1, lang * TAIL + rank - MAIN)
    shape = (LANGS, each, Q)
    of_lang, row = (lax.broadcasted_iota(jnp.int32, shape, d) for d in range(2))
    hits = of_lang * TAIL + (row & 3) == jnp.broadcast_to(tail_at.reshape(1, 1, Q), shape)
    tail = jnp.zeros((LANGS * each, 128), jnp.float32)
    for c in range(COLS):
        picks = jnp.where(hits & (lax.shift_right_logical(row, 2) == c), 1.0, 0.0)
        picks = picks.astype(jnp.bfloat16).reshape(LANGS * each, Q)
        tail = tail + jnp.dot(picks, unit[:, c * 128 : (c + 1) * 128], preferred_element_type=jnp.float32)
    out[:, MAIN * COLS : SENT, :] = tail.astype(jnp.bfloat16).reshape(LANGS, each, 128)


def outbox_of(queries, routes):
    return pl.pallas_call(
        outbox_kernel,
        out_shape=(
            jax.ShapeDtypeStruct((LANGS, SENT, 128), jnp.bfloat16),
            jax.ShapeDtypeStruct((1, Q), jnp.int32),
        ),
        in_specs=[pl.BlockSpec(memory_space=pltpu.HBM)] * 2,
        out_specs=(VMEM, VMEM),
        scratch_shapes=[
            pltpu.VMEM((Q, WIDTH), jnp.bfloat16),
            pltpu.VMEM((1, Q), jnp.int32),
            pltpu.SemaphoreType.DMA((2,)),
        ],
        compiler_params=pltpu.CompilerParams(vmem_limit_bytes=60 << 20),
        name="outbox",
    )(queries, routes)


def join_kernel(back, slots, out, a, b):
    total = LANGS * ROWS
    hits = lax.broadcasted_iota(jnp.int32, (total, Q), 0) == jnp.broadcast_to(slots[...], (total, Q))
    picks = jnp.where(hits, 1.0, 0.0)
    picks = jnp.concatenate([picks[i * Q : (i + 1) * Q, :].T for i in range(total // Q)], axis=1)
    picks = picks.astype(jnp.bfloat16)
    for k in range(4):
        code = back[:, k].astype(jnp.int32).astype(jnp.float32).reshape(total, TOPK)
        high = code.astype(jnp.bfloat16)
        low = (code - high.astype(jnp.float32)).astype(jnp.bfloat16)
        rows = jnp.dot(picks, high, preferred_element_type=jnp.float32) + jnp.dot(
            picks, low, preferred_element_type=jnp.float32
        )
        ranks = decoded(rows).T
        a[pl.ds(k, TOPK, stride=8), :] = ranks
        a[pl.ds(k + 4, TOPK, stride=8), :] = ranks
    merge_top(a, 0, a, 0, b, 0, turn=2)
    merge_top(b, 0, b, 0, a, 0, turn=1)
    out[...] = a[pl.ds(0, TOPK, stride=8), :].T


def join(back, slots):
    return pl.pallas_call(
        join_kernel,
        out_shape=jax.ShapeDtypeStruct((Q, TOPK), jnp.float32),
        in_specs=[VMEM] * 2,
        out_specs=VMEM,
        scratch_shapes=[pltpu.VMEM((128 * 8, 128), jnp.float32)] * 2,
        compiler_params=LIMIT,
        name="join",
    )(back, slots)


AXES = ("lang", "shard")


def moves(target):
    return [
        (lang * 8 + y * 4 + x, lang * 8 + ty * 4 + tx % 4)
        for lang in range(16)
        for y in range(2)
        for x in range(4)
        for ty, tx in (target(lang % 2, y, x),)
    ]


def pair(core, y, x):
    return y, x + (1 if (x + core) % 2 == 0 else -1)


def over_x(core, y, x):
    return y, x + 2


def over_y(core, y, x):
    return 1 - y, x


TEAMS = [
    [
        (pair * 2 + core) * 8 + y * 4 + odd + 2 * half
        for core in range(2)
        for half in range(2)
        for y in range(2)
        for pair in range(8)
    ]
    for odd in range(2)
]


def shards(queries, routes, corpus):
    far = lax.ppermute(corpus, AXES, moves(pair))
    outbox, slots = outbox_of(queries, routes.reshape(1, Q))
    mine = lax.all_to_all(outbox, "lang", split_axis=0, concat_axis=0, tiled=True)
    cx0, cy0, cx1, cy1 = (
        lax.ppermute(part, AXES, moves(over)) for part in (mine[:8], mine[8:]) for over in (over_x, over_y)
    )
    r0, far = first(mine, corpus, far)
    cx0, cy0, r0 = lax.optimization_barrier((cx0, cy0, r0))
    cd0 = lax.ppermute(cx0, AXES, moves(over_y))
    r1 = early(cx0, cy0, corpus, far)
    cx1, cy1, r1 = lax.optimization_barrier((cx1, cy1, r1))
    cd1 = lax.ppermute(cy1, AXES, moves(over_x))
    r2, tails = middle(mine, (cx0, cx1, cy0, cy1), corpus, far)
    shard = lax.axis_index("shard")
    at = (lax.shift_right_logical(shard, 2) + (shard & 2)).reshape(1)
    found = late(at, (cd0, cd1), corpus, far, (r0, r1, r2, tails))
    back = lax.all_to_all(
        found.reshape(LANGS * 4, ROWS, TOPK), AXES, 0, 0, axis_index_groups=TEAMS, tiled=True
    )
    return join(back.reshape(2, 4, LANGS // 2, ROWS, TOPK), slots)


def solution(mesh):
    placed = (P(AXES, None), P(AXES, None), P(AXES, None))
    return jax.shard_map(shards, mesh=mesh, in_specs=placed, out_specs=P(AXES, None), check_vma=False)
```

```python
import functools

import jax
import jax.numpy as jnp
from jax import lax
from jax.experimental import pallas as pl
from jax.experimental.pallas import tpu as pltpu
from jax.sharding import PartitionSpec as P

TOPK = 128
LANGS = 16
CAP = 20
ROWS = 24
MAIN = 16
TAIL = CAP - MAIN
Q = 128
WIDTH = 768
COLS = WIDTH // 128
SENT = CAP * COLS

epsilon = 1e-06


def batcher(n):
    pairs = []
    p = 1
    while p < n:
        k = p
        while k >= 1:
            for j in range(k % p, n - k, 2 * k):
                for i in range(min(k, n - j - k)):
                    if (i + j) // (2 * p) == (i + j + k) // (2 * p):
                        pairs.append((i + j, i + j + k))
            k //= 2
        p *= 2
    return pairs


SORT32 = batcher(32)
SORT16 = batcher(16)


def wire(ref, base, i):
    return ref[pl.ds(pl.multiple_of((base + i) * 8, 8), 8), :]


def put(ref, base, i, value):
    ref[pl.ds(pl.multiple_of((base + i) * 8, 8), 8), :] = value


def sort32(ref, base):
    v = [wire(ref, base, i) for i in range(32)]
    for i, j in SORT32:
        v[i], v[j] = jnp.maximum(v[i], v[j]), jnp.minimum(v[i], v[j])
    for i in range(32):
        put(ref, base, i, v[i])


def clean(v):
    n = len(v)
    step = n // 2
    while step:
        for i in range(n):
            if not i & step:
                v[i], v[i + step] = jnp.maximum(v[i], v[i + step]), jnp.minimum(v[i], v[i + step])
        step //= 2
    return v


def clean_at(ref, base):
    v = clean([wire(ref, base, i) for i in range(32)])
    for i in range(32):
        put(ref, base, i, v[i])


def merge64(src, base, dst):
    for op, at in ((jnp.maximum, 0), (jnp.minimum, 32)):
        v = clean([op(wire(src, base, i), wire(src, base, 63 - i)) for i in range(32)])
        for i in range(32):
            put(dst, base + at, i, v[i])


def merge128(src, base, dst):
    for op, at in ((jnp.maximum, 0), (jnp.minimum, 64)):
        v = []
        for i in range(32):
            a = op(wire(src, base, i), wire(src, base, 127 - i))
            b = op(wire(src, base, i + 32), wire(src, base, 95 - i))
            v.append(jnp.maximum(a, b))
            put(dst, base + at + 32, i, jnp.minimum(a, b))
        v = clean(v)
        for i in range(32):
            put(dst, base + at, i, v[i])
        clean_at(dst, base + at + 32)


def merge_top(a, a_base, b, b_base, dst, dst_base, turn=0):
    def other(i):
        value = wire(b, b_base, 127 - i)
        return pltpu.roll(value, turn, 0) if turn else value

    v = []
    for i in range(32):
        c = [jnp.maximum(wire(a, a_base, i + 32 * k), other(i + 32 * k)) for k in range(4)]
        f0, g0 = jnp.maximum(c[0], c[2]), jnp.minimum(c[0], c[2])
        f1, g1 = jnp.maximum(c[1], c[3]), jnp.minimum(c[1], c[3])
        v.append(jnp.maximum(f0, f1))
        put(dst, dst_base + 32, i, jnp.minimum(f0, f1))
        put(dst, dst_base + 64, i, jnp.maximum(g0, g1))
        put(dst, dst_base + 96, i, jnp.minimum(g0, g1))
    v = clean(v)
    for i in range(32):
        put(dst, dst_base, i, v[i])

    def rest(k, carry):
        clean_at(dst, dst_base + 32 + 32 * k)
        return carry

    lax.fori_loop(0, 3, rest, 0)


def loop(n, body):
    def step(i, carry):
        body(i)
        return carry

    lax.fori_loop(0, n, step, 0)


def wires_of(corpus, rows, parts, i, whole=False):
    blocks = rows.shape[0] // 128
    apart, nth, kind = (256, i, 0) if blocks == 2 else (128, i // 2, i % 2 * 4)
    starts = [(kind + k) * apart + nth * 64 for k in range(4)]
    scores = lax.dot_general(
        jnp.concatenate([corpus[at : at + 64, :] for at in starts], axis=0),
        rows,
        (((1,), (1,)), ((), ())),
        preferred_element_type=jnp.float32,
    )
    ref, at = (parts, nth * 512) if whole else (parts[nth], 0)
    for k in range(4):
        for half in range(blocks):
            place = pl.ds(at + (kind + k) * blocks + half, 64, stride=8)
            ref[place, :] = scores[k * 64 : (k + 1) * 64, half * 128 : (half + 1) * 128]


def score(corpus, rows, s):
    for i in range(4):
        wires_of(corpus, rows, s, i, whole=True)


def order(blocks, s, u, dst):
    loop(4 * blocks, lambda i: sort32(s, i * 32))
    loop(2 * blocks, lambda i: merge64(s, i * 64, u))
    if blocks == 1:
        merge128(u, 0, dst)
    else:
        loop(2, lambda i: merge128(u, i * 128, s))
        merge_top(s, 0, s, 128, dst, 0)


def network(v, pairs):
    for i, j in pairs:
        v[i], v[j] = jnp.maximum(v[i], v[j]), jnp.minimum(v[i], v[j])
    return v


def best16(ref, base):
    a = network([wire(ref, base, i) for i in range(16)], SORT16)
    b = network([wire(ref, base, i) for i in range(16, 32)], SORT16)
    return clean([jnp.maximum(a[i], b[15 - i]) for i in range(16)])


def shorten(src, base, dst, dst_base):
    a = best16(src, base)
    b = best16(src, base + 32)
    peak = jnp.maximum(a[15], b[15])
    high = clean([jnp.maximum(a[i], b[15 - i]) for i in range(16)])
    low = clean([jnp.minimum(a[i], b[15 - i]) for i in range(16)])
    for i in range(16):
        put(dst, dst_base, i, high[i])
        put(dst, dst_base, 16 + i, low[i])
    return peak


def best32(src, base, dst, dst_base):
    v = clean([jnp.maximum(wire(src, base, i), wire(src, base, 63 - i)) for i in range(32)])
    for i in range(32):
        put(dst, dst_base, i, v[i])
    return v[31]


def best64(src, dst, turn=0):
    def other(i):
        return pltpu.roll(wire(src, 0, 63 - i), turn, 0) if turn else wire(src, 0, 127 - i)

    v = []
    for i in range(32):
        a = jnp.maximum(wire(src, 0, i), other(i))
        b = jnp.maximum(wire(src, 0, i + 32), other(i + 32))
        v.append(jnp.maximum(a, b))
        put(dst, 32, i, jnp.minimum(a, b))
    v = clean(v)
    for i in range(32):
        put(dst, 0, i, v[i])
    clean_at(dst, 32)
    return wire(dst, 63, 0)


def merge_turned(src, dst, turn):
    for op, at in ((jnp.maximum, 0), (jnp.minimum, 64)):
        v = []
        for i in range(32):
            a = op(wire(src, 0, i), pltpu.roll(wire(src, 0, 63 - i), turn, 0))
            b = op(wire(src, 0, i + 32), pltpu.roll(wire(src, 0, 31 - i), turn, 0))
            v.append(jnp.maximum(a, b))
            put(dst, at + 32, i, jnp.minimum(a, b))
        v = clean(v)
        for i in range(32):
            put(dst, at, i, v[i])
        clean_at(dst, at + 32)


def leaders(groups, own, far, *work, emit, ahead=2):
    near_parts, far_parts, (s, u, w) = work[:4], work[4:8], work[8:]
    sides = (near_parts, far_parts)
    parts = [(g, side, i) for g in range(len(groups)) for side in range(2) for i in range(4)]

    def scored(k):
        if k < len(parts):
            g, side, i = parts[k]
            wires_of((own, far)[side](), groups[g][1](), sides[side], i)

    for k in range(ahead):
        scored(k)
    peak = None
    for k, (g, side, i) in enumerate(parts):
        scored(k + ahead)
        blocks = groups[g][0]
        if blocks == 2 or i % 2 == 1:
            nth = i if blocks == 2 else i // 2
            now = shorten(sides[side][nth], 0, u, side * 64 * blocks + nth * 32)
            peak = now if peak is None else jnp.maximum(peak, now)
        if side == 0 or i < 3:
            continue
        for j in range(2 * blocks):
            peak = jnp.maximum(peak, best32(u, j * 64, w, j * 32))
        if blocks == 2:
            loop(2, lambda j: merge64(w, j * 64, u))
            peak = jnp.maximum(peak, best64(u, w))
            turns = (4, 2)
        else:
            merge64(w, 0, u)
            peak = jnp.maximum(peak, best64(u, w, turn=4))
            turns = (2, 1)
        merge_turned(w, u, turns[0])
        merge_top(u, 0, u, 0, w, 0, turn=turns[1])
        for turn in (4, 2, 1)[: 4 - blocks]:
            peak = jnp.maximum(peak, pltpu.roll(peak, turn, 0))
        unsure = jnp.max(jnp.where(peak > wire(w, 127, 0), 1.0, 0.0)) > 0.0
        peak = None

        def give(g=g, blocks=blocks):
            for half in range(blocks):
                emit(g, half, w[pl.ds(half, TOPK, stride=8), :].T)

        give()

        @pl.when(unsure)
        def _(g=g, blocks=blocks, give=give):
            long_way(blocks, groups[g][1](), own(), far(), s, u, w)
            give()


def long_way(blocks, rows, own, far, s, u, w):
    score(own, rows, s)
    order(blocks, s, u, w)
    score(far, rows, s)
    if blocks == 2:
        order(blocks, s, u, u)
        merge_top(w, 0, u, 0, s, 0)
        merge_top(s, 0, s, 0, u, 0, turn=4)
        merge_top(u, 0, u, 0, w, 0, turn=2)
    else:
        loop(4, lambda i: sort32(s, i * 32))
        loop(2, lambda i: merge64(s, i * 64, u))
        merge128(u, 0, s)
        merge_top(w, 0, s, 0, u, 0)
        merge_top(u, 0, u, 0, s, 0, turn=4)
        merge_top(s, 0, s, 0, u, 0, turn=2)
        merge_top(u, 0, u, 0, w, 0, turn=1)


def main_rows(chunk):
    return jnp.concatenate(
        [chunk[:, c * MAIN : (c + 1) * MAIN, :].reshape(-1, 128) for c in range(COLS)], axis=1
    )


def tail_rows(chunk):
    langs = chunk.shape[0]
    many, each = langs * TAIL, TAIL * COLS
    shape, total = (COLS, many, langs * each), langs * each
    col, row, at = (lax.broadcasted_iota(jnp.int32, shape, d) for d in range(3))
    from_row = lax.shift_right_logical(row, 2) * each + col * TAIL + (row & 3)
    picks = jnp.where(at == from_row, 1.0, 0.0).astype(jnp.bfloat16).reshape(total, total)
    flat = chunk[:, MAIN * COLS : SENT, :].reshape(total, 128)
    found = jnp.dot(picks, flat, preferred_element_type=jnp.float32).astype(jnp.bfloat16)
    return jnp.concatenate([found[c * many : (c + 1) * many, :] for c in range(COLS)], axis=1)


def first_kernel(chunk, own, far_in, out, far, rows, sem, *work):
    copy = pltpu.make_async_copy(far_in, far, sem)
    copy.start()
    rows[...] = main_rows(chunk)
    waited = []

    def partner():
        if not waited:
            copy.wait()
            waited.append(True)
        return far

    def emit(g, half, value):
        out[half * Q : (half + 1) * Q, :] = value

    leaders([(2, lambda: rows[...])], lambda: own, partner, *work, emit=emit, ahead=0)


def early_kernel(half0, half1, own, far, out, rows, *work):
    rows[0:128, :] = main_rows(half0)
    rows[128:256, :] = main_rows(half1)

    def emit(g, half, value):
        out[half * Q : (half + 1) * Q, :] = value

    leaders([(2, lambda: rows[...])], lambda: own, lambda: far, *work, emit=emit)


def middle_kernel(mine, cx0, cx1, cy0, cy1, own, far, out, tails, rows, *work):
    rows[0:128, :] = main_rows(cx1)
    rows[128:256, :] = main_rows(cy1)
    rows[256:320, :] = tail_rows(mine)
    for k, chunk in enumerate((cx0, cx1, cy0, cy1)):
        rows[320 + k * 32 : 352 + k * 32, :] = tail_rows(chunk)
    rows[448:512, :] = jnp.zeros((64, WIDTH), jnp.bfloat16)

    def emit(g, half, value):
        (out, tails)[g][half * Q : (half + 1) * Q, :] = value

    leaders(
        [(2, lambda: rows[0:256, :]), (2, lambda: rows[256:512, :])], lambda: own, lambda: far, *work, emit=emit
    )


STEPS = 800.0
FLOOR = 32.5
LN2 = 0.6931471805599453


def coded(v):
    level = jnp.round(jnp.log(jnp.abs(v)) * (STEPS / LN2) + STEPS * FLOOR)
    level = jnp.clip(level, 0.0, 32767.0)
    return jnp.where(v < 0, -level, level)


def decoded(c):
    level = jnp.abs(c)
    v = jnp.where(level > 0, jnp.exp(level * (LN2 / STEPS) - FLOOR * LN2), 0.0)
    return jnp.where(c < 0, -v, v)


def late_kernel(at, cd0, cd1, own, far, r0, r1, r2, tails, out, rows, last, box, *work):
    rows[0:128, :] = main_rows(cd0)
    rows[128:256, :] = main_rows(cd1)
    rows[256:288, :] = tail_rows(cd0)
    rows[288:320, :] = tail_rows(cd1)
    rows[320:384, :] = jnp.zeros((64, WIDTH), jnp.bfloat16)

    def emit(g, half, value):
        last[g * 256 + half * Q : g * 256 + (half + 1) * Q, :] = value

    leaders(
        [(2, lambda: rows[0:256, :]), (1, lambda: rows[256:384, :])], lambda: own, lambda: far, *work, emit=emit
    )
    me = at[0]
    owner = (me, me ^ 1, me ^ 2, me ^ 3)
    none = jnp.zeros((ROWS - CAP, TOPK), jnp.float32)
    for k in range(4):
        for lang in range(LANGS):
            half, start = lang // 8, lang % 8 * MAIN
            if k == 0:
                main = r0[lang * MAIN : (lang + 1) * MAIN, :]
            elif k < 3:
                start += (k - 1) * Q
                main = (r1, r2)[half][start : start + MAIN, :]
            else:
                main = last[lang * MAIN : (lang + 1) * MAIN, :]
            box[k, 0:MAIN, :] = main
            start = k * 64 + lang * TAIL
            if k < 3:
                box[k, MAIN:CAP, :] = tails[start : start + TAIL, :]
            else:
                box[k, MAIN:CAP, :] = last[256 + lang * TAIL : 256 + (lang + 1) * TAIL, :]
            box[k, CAP:ROWS, :] = none
            out[lang, owner[k]] = coded(box[k]).astype(jnp.int32).astype(jnp.int16)


COST = 2 * 256 * 2048 * 768 * 8
VMEM = pl.BlockSpec(memory_space=pltpu.VMEM)
LIMIT = pltpu.CompilerParams(vmem_limit_bytes=14 << 20)
WORK = [pltpu.VMEM((64 * 8, 128), jnp.float32)] * 8 + [
    pltpu.VMEM((256 * 8, 128), jnp.float32),
    pltpu.VMEM((256 * 8, 128), jnp.float32),
    pltpu.VMEM((128 * 8, 128), jnp.float32),
]


def first(chunk, own, far):
    return pl.pallas_call(
        first_kernel,
        out_shape=(
            jax.ShapeDtypeStruct((256, TOPK), jnp.float32),
            jax.ShapeDtypeStruct((1024, WIDTH), jnp.bfloat16),
        ),
        in_specs=[VMEM, VMEM, pl.BlockSpec(memory_space=pl.ANY)],
        out_specs=(VMEM, VMEM),
        scratch_shapes=[pltpu.VMEM((256, WIDTH), jnp.bfloat16), pltpu.SemaphoreType.DMA] + WORK,
        compiler_params=LIMIT,
        cost_estimate=pl.CostEstimate(flops=COST, bytes_accessed=1 << 20, transcendentals=0),
        name="first",
    )(chunk, own, far)


def early(half0, half1, own, far):
    return pl.pallas_call(
        early_kernel,
        out_shape=jax.ShapeDtypeStruct((256, TOPK), jnp.float32),
        in_specs=[VMEM] * 4,
        out_specs=VMEM,
        scratch_shapes=[pltpu.VMEM((256, WIDTH), jnp.bfloat16)] + WORK,
        compiler_params=LIMIT,
        cost_estimate=pl.CostEstimate(flops=COST, bytes_accessed=1 << 20, transcendentals=0),
        name="early",
    )(half0, half1, own, far)


def middle(mine, halves, own, far):
    return pl.pallas_call(
        middle_kernel,
        out_shape=[jax.ShapeDtypeStruct((256, TOPK), jnp.float32)] * 2,
        in_specs=[VMEM] * 7,
        out_specs=[VMEM] * 2,
        scratch_shapes=[pltpu.VMEM((512, WIDTH), jnp.bfloat16)] + WORK,
        compiler_params=LIMIT,
        cost_estimate=pl.CostEstimate(flops=COST * 2, bytes_accessed=1 << 20, transcendentals=0),
        name="middle",
    )(mine, *halves, own, far)


def late(at, halves, own, far, results):
    return pl.pallas_call(
        late_kernel,
        out_shape=jax.ShapeDtypeStruct((LANGS, 4, ROWS, TOPK), jnp.int16),
        in_specs=[pl.BlockSpec(memory_space=pltpu.SMEM)] + [VMEM] * 8,
        out_specs=VMEM,
        scratch_shapes=[
            pltpu.VMEM((384, WIDTH), jnp.bfloat16),
            pltpu.VMEM((384, TOPK), jnp.float32),
            pltpu.VMEM((4, ROWS, TOPK), jnp.float32),
        ]
        + WORK,
        compiler_params=LIMIT,
        cost_estimate=pl.CostEstimate(flops=COST * 2, bytes_accessed=1 << 20, transcendentals=0),
        name="late",
    )(at, *halves, own, far, *results)


def outbox_kernel(queries_in, routes_in, out, slots, queries, routes, sems):
    copies = (
        pltpu.make_async_copy(routes_in, routes, sems.at[0]),
        pltpu.make_async_copy(queries_in, queries, sems.at[1]),
    )
    for copy in copies:
        copy.start()
    copies[0].wait()
    along = jnp.broadcast_to(routes[...].astype(jnp.float32), (Q, Q))
    down = along.T
    before = lax.broadcasted_iota(jnp.int32, (Q, Q), 0) < lax.broadcasted_iota(jnp.int32, (Q, Q), 1)
    earlier = jnp.where(before & (along == down), 1.0, 0.0)
    rank = jnp.sum(earlier, axis=0, keepdims=True).astype(jnp.int32)
    lang = routes[...]
    slots[...] = lang * ROWS + rank
    main_at = jnp.where(rank < MAIN, lang * MAIN + rank, -1)
    hits = lax.broadcasted_iota(jnp.int32, (LANGS * MAIN, Q), 0) == jnp.broadcast_to(main_at, (LANGS * MAIN, Q))
    picks = jnp.where(hits, 1.0, 0.0).astype(jnp.bfloat16)
    each = TAIL * COLS
    tail_at = jnp.where(rank < MAIN, -1, lang * TAIL + rank - MAIN)
    shape = (LANGS, each, Q)
    of_lang, row = (lax.broadcasted_iota(jnp.int32, shape, d) for d in range(2))
    hits = of_lang * TAIL + (row & 3) == jnp.broadcast_to(tail_at.reshape(1, 1, Q), shape)
    tail_picks = [
        jnp.where(hits & (lax.shift_right_logical(row, 2) == c), 1.0, 0.0).astype(jnp.bfloat16).reshape(LANGS * each, Q)
        for c in range(COLS)
    ]
    copies[1].wait()
    x = queries[...].astype(jnp.float32)
    unit = (x * lax.rsqrt(jnp.mean(x * x, axis=1, keepdims=True) + epsilon)).astype(jnp.bfloat16)
    box = jnp.dot(picks, unit, preferred_element_type=jnp.float32).astype(jnp.bfloat16)
    for c in range(COLS):
        out[:, c * MAIN : (c + 1) * MAIN, :] = box[:, c * 128 : (c + 1) * 128].reshape(LANGS, MAIN, 128)
    tail = jnp.zeros((LANGS * each, 128), jnp.float32)
    for c in range(COLS):
        tail = tail + jnp.dot(tail_picks[c], unit[:, c * 128 : (c + 1) * 128], preferred_element_type=jnp.float32)
    out[:, MAIN * COLS : SENT, :] = tail.astype(jnp.bfloat16).reshape(LANGS, each, 128)


def outbox_of(queries, routes):
    return pl.pallas_call(
        outbox_kernel,
        out_shape=(
            jax.ShapeDtypeStruct((LANGS, SENT, 128), jnp.bfloat16),
            jax.ShapeDtypeStruct((1, Q), jnp.int32),
        ),
        in_specs=[pl.BlockSpec(memory_space=pltpu.HBM)] * 2,
        out_specs=(VMEM, VMEM),
        scratch_shapes=[
            pltpu.VMEM((Q, WIDTH), jnp.bfloat16),
            pltpu.VMEM((1, Q), jnp.int32),
            pltpu.SemaphoreType.DMA((2,)),
        ],
        compiler_params=pltpu.CompilerParams(vmem_limit_bytes=60 << 20),
        name="outbox",
    )(queries, routes)


def join_kernel(back, slots, out, a, b):
    total = LANGS * ROWS
    hits = lax.broadcasted_iota(jnp.int32, (total, Q), 0) == jnp.broadcast_to(slots[...], (total, Q))
    picks = jnp.where(hits, 1.0, 0.0)
    picks = jnp.concatenate([picks[i * Q : (i + 1) * Q, :].T for i in range(total // Q)], axis=1)
    picks = picks.astype(jnp.bfloat16)
    for k in range(4):
        code = back[:, k].astype(jnp.int32).astype(jnp.float32).reshape(total, TOPK)
        high = code.astype(jnp.bfloat16)
        low = (code - high.astype(jnp.float32)).astype(jnp.bfloat16)
        rows = jnp.dot(picks, high, preferred_element_type=jnp.float32) + jnp.dot(
            picks, low, preferred_element_type=jnp.float32
        )
        ranks = decoded(rows).T
        a[pl.ds(k, TOPK, stride=8), :] = ranks
        a[pl.ds(k + 4, TOPK, stride=8), :] = ranks
    merge_top(a, 0, a, 0, b, 0, turn=2)
    merge_top(b, 0, b, 0, a, 0, turn=1)
    out[...] = a[pl.ds(0, TOPK, stride=8), :].T


def join(back, slots):
    return pl.pallas_call(
        join_kernel,
        out_shape=jax.ShapeDtypeStruct((Q, TOPK), jnp.float32),
        in_specs=[VMEM] * 2,
        out_specs=VMEM,
        scratch_shapes=[pltpu.VMEM((128 * 8, 128), jnp.float32)] * 2,
        compiler_params=LIMIT,
        name="join",
    )(back, slots)


AXES = ("lang", "shard")


def moves(target):
    return [
        (lang * 8 + y * 4 + x, lang * 8 + ty * 4 + tx % 4)
        for lang in range(16)
        for y in range(2)
        for x in range(4)
        for ty, tx in (target(lang % 2, y, x),)
    ]


def pair(core, y, x):
    return y, x + (1 if (x + core) % 2 == 0 else -1)


def over_x(core, y, x):
    return y, x + 2


def over_y(core, y, x):
    return 1 - y, x


TEAMS = [
    [lang * 8 + y * 4 + odd + 2 * half for lang in range(16) for y in range(2) for half in range(2)]
    for odd in range(2)
]


def shards(queries, routes, corpus):
    far = lax.ppermute(corpus, AXES, moves(pair))
    outbox, slots = outbox_of(queries, routes.reshape(1, Q))
    mine = lax.all_to_all(outbox, "lang", split_axis=0, concat_axis=0, tiled=True)
    cx0, cy0, cx1, cy1 = (
        lax.ppermute(part, AXES, moves(over)) for part in (mine[:8], mine[8:]) for over in (over_x, over_y)
    )
    r0, far = first(mine, corpus, far)
    cx0, cy0, r0 = lax.optimization_barrier((cx0, cy0, r0))
    cd0 = lax.ppermute(cx0, AXES, moves(over_y))
    r1 = early(cx0, cy0, corpus, far)
    cx1, cy1, r1 = lax.optimization_barrier((cx1, cy1, r1))
    cd1 = lax.ppermute(cy1, AXES, moves(over_x))
    r2, tails = middle(mine, (cx0, cx1, cy0, cy1), corpus, far)
    shard = lax.axis_index("shard")
    at = (lax.shift_right_logical(shard, 2) * 2 + (lax.shift_right_logical(shard, 1) & 1)).reshape(1)
    found = late(at, (cd0, cd1), corpus, far, (r0, r1, r2, tails))
    back = lax.all_to_all(
        found.reshape(LANGS * 4, ROWS, TOPK), AXES, 0, 0, axis_index_groups=TEAMS, tiled=True
    )
    return join(back.reshape(LANGS, 4, ROWS, TOPK), slots)


def solution(mesh):
    placed = (P(AXES, None), P(AXES, None), P(AXES, None))
    return jax.shard_map(shards, mesh=mesh, in_specs=placed, out_specs=P(AXES, None), check_vma=False)
```

```python
import functools

import jax
import jax.numpy as jnp
from jax import lax
from jax.experimental import pallas as pl
from jax.experimental.pallas import tpu as pltpu
from jax.sharding import PartitionSpec as P

TOPK = 128
LANGS = 16
CAP = 20
ROWS = 24
MAIN = 16
TAIL = CAP - MAIN
Q = 128
WIDTH = 768
COLS = WIDTH // 128
SENT = CAP * COLS

epsilon = 1e-06


def batcher(n):
    pairs = []
    p = 1
    while p < n:
        k = p
        while k >= 1:
            for j in range(k % p, n - k, 2 * k):
                for i in range(min(k, n - j - k)):
                    if (i + j) // (2 * p) == (i + j + k) // (2 * p):
                        pairs.append((i + j, i + j + k))
            k //= 2
        p *= 2
    return pairs


SORT32 = batcher(32)
SORT16 = batcher(16)


def wire(ref, base, i):
    return ref[pl.ds(pl.multiple_of((base + i) * 8, 8), 8), :]


def put(ref, base, i, value):
    ref[pl.ds(pl.multiple_of((base + i) * 8, 8), 8), :] = value


def sort32(ref, base):
    v = [wire(ref, base, i) for i in range(32)]
    for i, j in SORT32:
        v[i], v[j] = jnp.maximum(v[i], v[j]), jnp.minimum(v[i], v[j])
    for i in range(32):
        put(ref, base, i, v[i])


def clean(v):
    n = len(v)
    step = n // 2
    while step:
        for i in range(n):
            if not i & step:
                v[i], v[i + step] = jnp.maximum(v[i], v[i + step]), jnp.minimum(v[i], v[i + step])
        step //= 2
    return v


def clean_at(ref, base):
    v = clean([wire(ref, base, i) for i in range(32)])
    for i in range(32):
        put(ref, base, i, v[i])


def merge64(src, base, dst):
    for op, at in ((jnp.maximum, 0), (jnp.minimum, 32)):
        v = clean([op(wire(src, base, i), wire(src, base, 63 - i)) for i in range(32)])
        for i in range(32):
            put(dst, base + at, i, v[i])


def merge128(src, base, dst):
    for op, at in ((jnp.maximum, 0), (jnp.minimum, 64)):
        v = []
        for i in range(32):
            a = op(wire(src, base, i), wire(src, base, 127 - i))
            b = op(wire(src, base, i + 32), wire(src, base, 95 - i))
            v.append(jnp.maximum(a, b))
            put(dst, base + at + 32, i, jnp.minimum(a, b))
        v = clean(v)
        for i in range(32):
            put(dst, base + at, i, v[i])
        clean_at(dst, base + at + 32)


def merge_top(a, a_base, b, b_base, dst, dst_base, turn=0):
    def other(i):
        value = wire(b, b_base, 127 - i)
        return pltpu.roll(value, turn, 0) if turn else value

    v = []
    for i in range(32):
        c = [jnp.maximum(wire(a, a_base, i + 32 * k), other(i + 32 * k)) for k in range(4)]
        f0, g0 = jnp.maximum(c[0], c[2]), jnp.minimum(c[0], c[2])
        f1, g1 = jnp.maximum(c[1], c[3]), jnp.minimum(c[1], c[3])
        v.append(jnp.maximum(f0, f1))
        put(dst, dst_base + 32, i, jnp.minimum(f0, f1))
        put(dst, dst_base + 64, i, jnp.maximum(g0, g1))
        put(dst, dst_base + 96, i, jnp.minimum(g0, g1))
    v = clean(v)
    for i in range(32):
        put(dst, dst_base, i, v[i])

    def rest(k, carry):
        clean_at(dst, dst_base + 32 + 32 * k)
        return carry

    lax.fori_loop(0, 3, rest, 0)


def loop(n, body):
    def step(i, carry):
        body(i)
        return carry

    lax.fori_loop(0, n, step, 0)


def wires_of(corpus, rows, parts, i, whole=False):
    blocks = rows.shape[0] // 128
    apart, nth, kind = (256, i, 0) if blocks == 2 else (128, i // 2, i % 2 * 4)
    starts = [(kind + k) * apart + nth * 64 for k in range(4)]
    scores = lax.dot_general(
        jnp.concatenate([corpus[at : at + 64, :] for at in starts], axis=0),
        rows,
        (((1,), (1,)), ((), ())),
        preferred_element_type=jnp.float32,
    )
    ref, at = (parts, nth * 512) if whole else (parts[nth], 0)
    for k in range(4):
        for half in range(blocks):
            place = pl.ds(at + (kind + k) * blocks + half, 64, stride=8)
            ref[place, :] = scores[k * 64 : (k + 1) * 64, half * 128 : (half + 1) * 128]


def score(corpus, rows, s):
    for i in range(4):
        wires_of(corpus, rows, s, i, whole=True)


def order(blocks, s, u, dst):
    loop(4 * blocks, lambda i: sort32(s, i * 32))
    loop(2 * blocks, lambda i: merge64(s, i * 64, u))
    if blocks == 1:
        merge128(u, 0, dst)
    else:
        loop(2, lambda i: merge128(u, i * 128, s))
        merge_top(s, 0, s, 128, dst, 0)


def network(v, pairs):
    for i, j in pairs:
        v[i], v[j] = jnp.maximum(v[i], v[j]), jnp.minimum(v[i], v[j])
    return v


def best16(ref, base):
    a = network([wire(ref, base, i) for i in range(16)], SORT16)
    b = network([wire(ref, base, i) for i in range(16, 32)], SORT16)
    return clean([jnp.maximum(a[i], b[15 - i]) for i in range(16)])


def shorten(src, base, dst, dst_base):
    a = best16(src, base)
    b = best16(src, base + 32)
    peak = jnp.maximum(a[15], b[15])
    high = clean([jnp.maximum(a[i], b[15 - i]) for i in range(16)])
    low = clean([jnp.minimum(a[i], b[15 - i]) for i in range(16)])
    for i in range(16):
        put(dst, dst_base, i, high[i])
        put(dst, dst_base, 16 + i, low[i])
    return peak


def best32(src, base, dst, dst_base):
    v = clean([jnp.maximum(wire(src, base, i), wire(src, base, 63 - i)) for i in range(32)])
    for i in range(32):
        put(dst, dst_base, i, v[i])
    return v[31]


def best64(src, dst, turn=0):
    def other(i):
        return pltpu.roll(wire(src, 0, 63 - i), turn, 0) if turn else wire(src, 0, 127 - i)

    v = []
    for i in range(32):
        a = jnp.maximum(wire(src, 0, i), other(i))
        b = jnp.maximum(wire(src, 0, i + 32), other(i + 32))
        v.append(jnp.maximum(a, b))
        put(dst, 32, i, jnp.minimum(a, b))
    v = clean(v)
    for i in range(32):
        put(dst, 0, i, v[i])
    clean_at(dst, 32)
    return wire(dst, 63, 0)


def merge_turned(src, dst, turn):
    for op, at in ((jnp.maximum, 0), (jnp.minimum, 64)):
        v = []
        for i in range(32):
            a = op(wire(src, 0, i), pltpu.roll(wire(src, 0, 63 - i), turn, 0))
            b = op(wire(src, 0, i + 32), pltpu.roll(wire(src, 0, 31 - i), turn, 0))
            v.append(jnp.maximum(a, b))
            put(dst, at + 32, i, jnp.minimum(a, b))
        v = clean(v)
        for i in range(32):
            put(dst, at, i, v[i])
        clean_at(dst, at + 32)


def leaders(groups, own, far, *work, emit, ahead=2):
    near_parts, far_parts, (s, u, w) = work[:4], work[4:8], work[8:]
    sides = (near_parts, far_parts)
    parts = [(g, side, i) for g in range(len(groups)) for side in range(2) for i in range(4)]

    def scored(k):
        if k < len(parts):
            g, side, i = parts[k]
            wires_of((own, far)[side](), groups[g][1](), sides[side], i)

    for k in range(ahead):
        scored(k)
    peak = None
    for k, (g, side, i) in enumerate(parts):
        scored(k + ahead)
        blocks = groups[g][0]
        if blocks == 2 or i % 2 == 1:
            nth = i if blocks == 2 else i // 2
            now = shorten(sides[side][nth], 0, u, side * 64 * blocks + nth * 32)
            peak = now if peak is None else jnp.maximum(peak, now)
        if side == 0 or i < 3:
            continue
        for j in range(2 * blocks):
            peak = jnp.maximum(peak, best32(u, j * 64, w, j * 32))
        if blocks == 2:
            loop(2, lambda j: merge64(w, j * 64, u))
            peak = jnp.maximum(peak, best64(u, w))
            turns = (4, 2)
        else:
            merge64(w, 0, u)
            peak = jnp.maximum(peak, best64(u, w, turn=4))
            turns = (2, 1)
        merge_turned(w, u, turns[0])
        merge_top(u, 0, u, 0, w, 0, turn=turns[1])
        for turn in (4, 2, 1)[: 4 - blocks]:
            peak = jnp.maximum(peak, pltpu.roll(peak, turn, 0))
        unsure = jnp.max(jnp.where(peak > wire(w, 127, 0), 1.0, 0.0)) > 0.0
        peak = None

        def give(g=g, blocks=blocks):
            for half in range(blocks):
                emit(g, half, w[pl.ds(half, TOPK, stride=8), :].T)

        give()

        @pl.when(unsure)
        def _(g=g, blocks=blocks, give=give):
            long_way(blocks, groups[g][1](), own(), far(), s, u, w)
            give()


def long_way(blocks, rows, own, far, s, u, w):
    score(own, rows, s)
    order(blocks, s, u, w)
    score(far, rows, s)
    if blocks == 2:
        order(blocks, s, u, u)
        merge_top(w, 0, u, 0, s, 0)
        merge_top(s, 0, s, 0, u, 0, turn=4)
        merge_top(u, 0, u, 0, w, 0, turn=2)
    else:
        loop(4, lambda i: sort32(s, i * 32))
        loop(2, lambda i: merge64(s, i * 64, u))
        merge128(u, 0, s)
        merge_top(w, 0, s, 0, u, 0)
        merge_top(u, 0, u, 0, s, 0, turn=4)
        merge_top(s, 0, s, 0, u, 0, turn=2)
        merge_top(u, 0, u, 0, w, 0, turn=1)


def main_rows(chunk):
    return jnp.concatenate(
        [chunk[:, c * MAIN : (c + 1) * MAIN, :].reshape(-1, 128) for c in range(COLS)], axis=1
    )


def tail_rows(chunk):
    langs = chunk.shape[0]
    many, each = langs * TAIL, TAIL * COLS
    shape, total = (COLS, many, langs * each), langs * each
    col, row, at = (lax.broadcasted_iota(jnp.int32, shape, d) for d in range(3))
    from_row = lax.shift_right_logical(row, 2) * each + col * TAIL + (row & 3)
    picks = jnp.where(at == from_row, 1.0, 0.0).astype(jnp.bfloat16).reshape(total, total)
    flat = chunk[:, MAIN * COLS : SENT, :].reshape(total, 128)
    found = jnp.dot(picks, flat, preferred_element_type=jnp.float32).astype(jnp.bfloat16)
    return jnp.concatenate([found[c * many : (c + 1) * many, :] for c in range(COLS)], axis=1)


def first_kernel(chunk, own, far_in, out, far, rows, sem, *work):
    copy = pltpu.make_async_copy(far_in, far, sem)
    copy.start()
    rows[...] = main_rows(chunk)
    waited = []

    def partner():
        if not waited:
            copy.wait()
            waited.append(True)
        return far

    def emit(g, half, value):
        out[half * Q : (half + 1) * Q, :] = value

    leaders([(2, lambda: rows[...])], lambda: own, partner, *work, emit=emit, ahead=0)


def early_kernel(half0, half1, own, far, out, rows, *work):
    rows[0:128, :] = main_rows(half0)
    rows[128:256, :] = main_rows(half1)

    def emit(g, half, value):
        out[half * Q : (half + 1) * Q, :] = value

    leaders([(2, lambda: rows[...])], lambda: own, lambda: far, *work, emit=emit)


STEPS = 800.0
FLOOR = 32.5
LN2 = 0.6931471805599453


def coded(v):
    level = jnp.round(jnp.log(jnp.abs(v)) * (STEPS / LN2) + STEPS * FLOOR)
    level = jnp.clip(level, 0.0, 32767.0)
    return jnp.where(v < 0, -level, level)


def decoded(c):
    level = jnp.abs(c)
    v = jnp.where(level > 0, jnp.exp(level * (LN2 / STEPS) - FLOOR * LN2), 0.0)
    return jnp.where(c < 0, -v, v)


def boxed(box, main, tail):
    box[0:MAIN, :] = main
    box[MAIN:CAP, :] = tail
    box[CAP:ROWS, :] = jnp.zeros((ROWS - CAP, TOPK), jnp.float32)
    return coded(box[...]).astype(jnp.int32).astype(jnp.int16)


def middle_kernel(mine, cx0, cx1, cy0, cy1, own, far, r0, r1, out, rows, lists, box, *work):
    rows[0:128, :] = main_rows(cx1)
    rows[128:256, :] = main_rows(cy1)
    rows[256:320, :] = tail_rows(mine)
    for k, chunk in enumerate((cx0, cx1, cy0, cy1)):
        rows[320 + k * 32 : 352 + k * 32, :] = tail_rows(chunk)
    rows[448:512, :] = jnp.zeros((64, WIDTH), jnp.bfloat16)

    def emit(g, half, value):
        lists[g * 256 + half * Q : g * 256 + (half + 1) * Q, :] = value

    leaders(
        [(2, lambda: rows[0:256, :]), (2, lambda: rows[256:512, :])], lambda: own, lambda: far, *work, emit=emit
    )
    for k in range(3):
        for lang in range(LANGS):
            half, start = lang // 8, lang % 8 * MAIN
            if k == 0:
                main = r0[lang * MAIN : (lang + 1) * MAIN, :]
            else:
                start += (k - 1) * Q
                main = (r1, lists)[half][start : start + MAIN, :]
            start = 256 + k * 64 + lang * TAIL
            out[k, lang] = boxed(box.at[k], main, lists[start : start + TAIL, :])


def late_kernel(at, cd0, cd1, own, far, done, out, rows, last, box, *work):
    rows[0:128, :] = main_rows(cd0)
    rows[128:256, :] = main_rows(cd1)
    rows[256:288, :] = tail_rows(cd0)
    rows[288:320, :] = tail_rows(cd1)
    rows[320:384, :] = jnp.zeros((64, WIDTH), jnp.bfloat16)
    me = at[0]
    for k, owner in enumerate((me, me ^ 1, me ^ 2)):
        for lang in range(LANGS):
            out[lang, owner] = done[k, lang]

    def emit(g, half, value):
        last[g * 256 + half * Q : g * 256 + (half + 1) * Q, :] = value

    leaders(
        [(2, lambda: rows[0:256, :]), (1, lambda: rows[256:384, :])], lambda: own, lambda: far, *work, emit=emit
    )
    for lang in range(LANGS):
        tail = last[256 + lang * TAIL : 256 + (lang + 1) * TAIL, :]
        out[lang, me ^ 3] = boxed(box.at[lang % 4], last[lang * MAIN : (lang + 1) * MAIN, :], tail)


COST = 2 * 256 * 2048 * 768 * 8
VMEM = pl.BlockSpec(memory_space=pltpu.VMEM)
LIMIT = pltpu.CompilerParams(vmem_limit_bytes=14 << 20)
WORK = [pltpu.VMEM((64 * 8, 128), jnp.float32)] * 8 + [
    pltpu.VMEM((256 * 8, 128), jnp.float32),
    pltpu.VMEM((256 * 8, 128), jnp.float32),
    pltpu.VMEM((128 * 8, 128), jnp.float32),
]


def first(chunk, own, far):
    return pl.pallas_call(
        first_kernel,
        out_shape=(
            jax.ShapeDtypeStruct((256, TOPK), jnp.float32),
            jax.ShapeDtypeStruct((1024, WIDTH), jnp.bfloat16),
        ),
        in_specs=[VMEM, VMEM, pl.BlockSpec(memory_space=pl.ANY)],
        out_specs=(VMEM, VMEM),
        scratch_shapes=[pltpu.VMEM((256, WIDTH), jnp.bfloat16), pltpu.SemaphoreType.DMA] + WORK,
        compiler_params=LIMIT,
        cost_estimate=pl.CostEstimate(flops=COST, bytes_accessed=1 << 20, transcendentals=0),
        name="first",
    )(chunk, own, far)


def early(half0, half1, own, far):
    return pl.pallas_call(
        early_kernel,
        out_shape=jax.ShapeDtypeStruct((256, TOPK), jnp.float32),
        in_specs=[VMEM] * 4,
        out_specs=VMEM,
        scratch_shapes=[pltpu.VMEM((256, WIDTH), jnp.bfloat16)] + WORK,
        compiler_params=LIMIT,
        cost_estimate=pl.CostEstimate(flops=COST, bytes_accessed=1 << 20, transcendentals=0),
        name="early",
    )(half0, half1, own, far)


def middle(mine, halves, own, far, results):
    return pl.pallas_call(
        middle_kernel,
        out_shape=jax.ShapeDtypeStruct((3, LANGS, ROWS, TOPK), jnp.int16),
        in_specs=[VMEM] * 9,
        out_specs=VMEM,
        scratch_shapes=[
            pltpu.VMEM((512, WIDTH), jnp.bfloat16),
            pltpu.VMEM((512, TOPK), jnp.float32),
            pltpu.VMEM((3, ROWS, TOPK), jnp.float32),
        ]
        + WORK,
        compiler_params=LIMIT,
        cost_estimate=pl.CostEstimate(flops=COST * 2, bytes_accessed=1 << 20, transcendentals=0),
        name="middle",
    )(mine, *halves, own, far, *results)


def late(at, halves, own, far, done):
    return pl.pallas_call(
        late_kernel,
        out_shape=jax.ShapeDtypeStruct((LANGS, 4, ROWS, TOPK), jnp.int16),
        in_specs=[pl.BlockSpec(memory_space=pltpu.SMEM)] + [VMEM] * 5,
        out_specs=VMEM,
        scratch_shapes=[
            pltpu.VMEM((384, WIDTH), jnp.bfloat16),
            pltpu.VMEM((384, TOPK), jnp.float32),
            pltpu.VMEM((4, ROWS, TOPK), jnp.float32),
        ]
        + WORK,
        compiler_params=LIMIT,
        cost_estimate=pl.CostEstimate(flops=COST * 2, bytes_accessed=1 << 20, transcendentals=0),
        name="late",
    )(at, *halves, own, far, done)


def outbox_kernel(queries_in, routes_in, out, slots, queries, routes, sems):
    copies = (
        pltpu.make_async_copy(routes_in, routes, sems.at[0]),
        pltpu.make_async_copy(queries_in, queries, sems.at[1]),
    )
    for copy in copies:
        copy.start()
    copies[0].wait()
    along = jnp.broadcast_to(routes[...].astype(jnp.float32), (Q, Q))
    down = along.T
    before = lax.broadcasted_iota(jnp.int32, (Q, Q), 0) < lax.broadcasted_iota(jnp.int32, (Q, Q), 1)
    earlier = jnp.where(before & (along == down), 1.0, 0.0)
    rank = jnp.sum(earlier, axis=0, keepdims=True).astype(jnp.int32)
    lang = routes[...]
    slots[...] = lang * ROWS + rank
    main_at = jnp.where(rank < MAIN, lang * MAIN + rank, -1)
    hits = lax.broadcasted_iota(jnp.int32, (LANGS * MAIN, Q), 0) == jnp.broadcast_to(main_at, (LANGS * MAIN, Q))
    picks = jnp.where(hits, 1.0, 0.0).astype(jnp.bfloat16)
    each = TAIL * COLS
    tail_at = jnp.where(rank < MAIN, -1, lang * TAIL + rank - MAIN)
    shape = (LANGS, each, Q)
    of_lang, row = (lax.broadcasted_iota(jnp.int32, shape, d) for d in range(2))
    hits = of_lang * TAIL + (row & 3) == jnp.broadcast_to(tail_at.reshape(1, 1, Q), shape)
    tail_picks = [
        jnp.where(hits & (lax.shift_right_logical(row, 2) == c), 1.0, 0.0).astype(jnp.bfloat16).reshape(LANGS * each, Q)
        for c in range(COLS)
    ]
    copies[1].wait()
    x = queries[...].astype(jnp.float32)
    unit = (x * lax.rsqrt(jnp.mean(x * x, axis=1, keepdims=True) + epsilon)).astype(jnp.bfloat16)
    box = jnp.dot(picks, unit, preferred_element_type=jnp.float32).astype(jnp.bfloat16)
    for c in range(COLS):
        out[:, c * MAIN : (c + 1) * MAIN, :] = box[:, c * 128 : (c + 1) * 128].reshape(LANGS, MAIN, 128)
    tail = jnp.zeros((LANGS * each, 128), jnp.float32)
    for c in range(COLS):
        tail = tail + jnp.dot(tail_picks[c], unit[:, c * 128 : (c + 1) * 128], preferred_element_type=jnp.float32)
    out[:, MAIN * COLS : SENT, :] = tail.astype(jnp.bfloat16).reshape(LANGS, each, 128)


def outbox_of(queries, routes):
    return pl.pallas_call(
        outbox_kernel,
        out_shape=(
            jax.ShapeDtypeStruct((LANGS, SENT, 128), jnp.bfloat16),
            jax.ShapeDtypeStruct((1, Q), jnp.int32),
        ),
        in_specs=[pl.BlockSpec(memory_space=pltpu.HBM)] * 2,
        out_specs=(VMEM, VMEM),
        scratch_shapes=[
            pltpu.VMEM((Q, WIDTH), jnp.bfloat16),
            pltpu.VMEM((1, Q), jnp.int32),
            pltpu.SemaphoreType.DMA((2,)),
        ],
        compiler_params=pltpu.CompilerParams(vmem_limit_bytes=60 << 20),
        name="outbox",
    )(queries, routes)


def join_kernel(back, slots, out, a, b):
    total = LANGS * ROWS
    hits = lax.broadcasted_iota(jnp.int32, (total, Q), 0) == jnp.broadcast_to(slots[...], (total, Q))
    picks = jnp.where(hits, 1.0, 0.0)
    picks = jnp.concatenate([picks[i * Q : (i + 1) * Q, :].T for i in range(total // Q)], axis=1)
    picks = picks.astype(jnp.bfloat16)
    for k in range(4):
        code = back[:, k].astype(jnp.int32).astype(jnp.float32).reshape(total, TOPK)
        high = code.astype(jnp.bfloat16)
        low = (code - high.astype(jnp.float32)).astype(jnp.bfloat16)
        rows = jnp.dot(picks, high, preferred_element_type=jnp.float32) + jnp.dot(
            picks, low, preferred_element_type=jnp.float32
        )
        ranks = decoded(rows).T
        a[pl.ds(k, TOPK, stride=8), :] = ranks
        a[pl.ds(k + 4, TOPK, stride=8), :] = ranks
    merge_top(a, 0, a, 0, b, 0, turn=2)
    merge_top(b, 0, b, 0, a, 0, turn=1)
    out[...] = a[pl.ds(0, TOPK, stride=8), :].T


def join(back, slots):
    return pl.pallas_call(
        join_kernel,
        out_shape=jax.ShapeDtypeStruct((Q, TOPK), jnp.float32),
        in_specs=[VMEM] * 2,
        out_specs=VMEM,
        scratch_shapes=[pltpu.VMEM((128 * 8, 128), jnp.float32)] * 2,
        compiler_params=LIMIT,
        name="join",
    )(back, slots)


AXES = ("lang", "shard")


def moves(target):
    return [
        (lang * 8 + y * 4 + x, lang * 8 + ty * 4 + tx % 4)
        for lang in range(16)
        for y in range(2)
        for x in range(4)
        for ty, tx in (target(lang % 2, y, x),)
    ]


def pair(core, y, x):
    return y, x + (1 if (x + core) % 2 == 0 else -1)


def over_x(core, y, x):
    return y, x + 2


def over_y(core, y, x):
    return 1 - y, x


TEAMS = [
    [lang * 8 + y * 4 + odd + 2 * half for lang in range(16) for y in range(2) for half in range(2)]
    for odd in range(2)
]


def shards(queries, routes, corpus):
    far = lax.ppermute(corpus, AXES, moves(pair))
    outbox, slots = outbox_of(queries, routes.reshape(1, Q))
    mine = lax.all_to_all(outbox, "lang", split_axis=0, concat_axis=0, tiled=True)
    cx0, cy0, cx1, cy1 = (
        lax.ppermute(part, AXES, moves(over)) for part in (mine[:8], mine[8:]) for over in (over_x, over_y)
    )
    r0, far = first(mine, corpus, far)
    cx0, cy0, r0 = lax.optimization_barrier((cx0, cy0, r0))
    cd0 = lax.ppermute(cx0, AXES, moves(over_y))
    r1 = early(cx0, cy0, corpus, far)
    cx1, cy1, r1 = lax.optimization_barrier((cx1, cy1, r1))
    cd1 = lax.ppermute(cy1, AXES, moves(over_x))
    done = middle(mine, (cx0, cx1, cy0, cy1), corpus, far, (r0, r1))
    shard = lax.axis_index("shard")
    at = (lax.shift_right_logical(shard, 2) * 2 + (lax.shift_right_logical(shard, 1) & 1)).reshape(1)
    found = late(at, (cd0, cd1), corpus, far, done)
    back = lax.all_to_all(
        found.reshape(LANGS * 4, ROWS, TOPK), AXES, 0, 0, axis_index_groups=TEAMS, tiled=True
    )
    return join(back.reshape(LANGS, 4, ROWS, TOPK), slots)


def solution(mesh):
    placed = (P(AXES, None), P(AXES, None), P(AXES, None))
    return jax.shard_map(shards, mesh=mesh, in_specs=placed, out_specs=P(AXES, None), check_vma=False)
```

```python
import functools

import jax
import jax.numpy as jnp
from jax import lax
from jax.experimental import pallas as pl
from jax.experimental.pallas import tpu as pltpu
from jax.sharding import PartitionSpec as P

TOPK = 128
LANGS = 16
CAP = 20
ROWS = 24
MAIN = 16
TAIL = CAP - MAIN
Q = 128
WIDTH = 768
COLS = WIDTH // 128
SENT = CAP * COLS

epsilon = 1e-06


def batcher(n):
    pairs = []
    p = 1
    while p < n:
        k = p
        while k >= 1:
            for j in range(k % p, n - k, 2 * k):
                for i in range(min(k, n - j - k)):
                    if (i + j) // (2 * p) == (i + j + k) // (2 * p):
                        pairs.append((i + j, i + j + k))
            k //= 2
        p *= 2
    return pairs


SORT32 = batcher(32)
SORT16 = batcher(16)


def wire(ref, base, i):
    return ref[pl.ds(pl.multiple_of((base + i) * 8, 8), 8), :]


def put(ref, base, i, value):
    ref[pl.ds(pl.multiple_of((base + i) * 8, 8), 8), :] = value


def sort32(ref, base):
    v = [wire(ref, base, i) for i in range(32)]
    for i, j in SORT32:
        v[i], v[j] = jnp.maximum(v[i], v[j]), jnp.minimum(v[i], v[j])
    for i in range(32):
        put(ref, base, i, v[i])


def clean(v):
    n = len(v)
    step = n // 2
    while step:
        for i in range(n):
            if not i & step:
                v[i], v[i + step] = jnp.maximum(v[i], v[i + step]), jnp.minimum(v[i], v[i + step])
        step //= 2
    return v


def clean_at(ref, base):
    v = clean([wire(ref, base, i) for i in range(32)])
    for i in range(32):
        put(ref, base, i, v[i])


def merge64(src, base, dst):
    for op, at in ((jnp.maximum, 0), (jnp.minimum, 32)):
        v = clean([op(wire(src, base, i), wire(src, base, 63 - i)) for i in range(32)])
        for i in range(32):
            put(dst, base + at, i, v[i])


def merge128(src, base, dst):
    for op, at in ((jnp.maximum, 0), (jnp.minimum, 64)):
        v = []
        for i in range(32):
            a = op(wire(src, base, i), wire(src, base, 127 - i))
            b = op(wire(src, base, i + 32), wire(src, base, 95 - i))
            v.append(jnp.maximum(a, b))
            put(dst, base + at + 32, i, jnp.minimum(a, b))
        v = clean(v)
        for i in range(32):
            put(dst, base + at, i, v[i])
        clean_at(dst, base + at + 32)


def merge_top(a, a_base, b, b_base, dst, dst_base, turn=0):
    def other(i):
        value = wire(b, b_base, 127 - i)
        return pltpu.roll(value, turn, 0) if turn else value

    v = []
    for i in range(32):
        c = [jnp.maximum(wire(a, a_base, i + 32 * k), other(i + 32 * k)) for k in range(4)]
        f0, g0 = jnp.maximum(c[0], c[2]), jnp.minimum(c[0], c[2])
        f1, g1 = jnp.maximum(c[1], c[3]), jnp.minimum(c[1], c[3])
        v.append(jnp.maximum(f0, f1))
        put(dst, dst_base + 32, i, jnp.minimum(f0, f1))
        put(dst, dst_base + 64, i, jnp.maximum(g0, g1))
        put(dst, dst_base + 96, i, jnp.minimum(g0, g1))
    v = clean(v)
    for i in range(32):
        put(dst, dst_base, i, v[i])

    def rest(k, carry):
        clean_at(dst, dst_base + 32 + 32 * k)
        return carry

    lax.fori_loop(0, 3, rest, 0)


def loop(n, body):
    def step(i, carry):
        body(i)
        return carry

    lax.fori_loop(0, n, step, 0)


def wires_of(corpus, rows, parts, i, whole=False):
    blocks = rows.shape[0] // 128
    apart, nth, kind = (256, i, 0) if blocks == 2 else (128, i // 2, i % 2 * 4)
    starts = [(kind + k) * apart + nth * 64 for k in range(4)]
    scores = lax.dot_general(
        jnp.concatenate([corpus[at : at + 64, :] for at in starts], axis=0),
        rows,
        (((1,), (1,)), ((), ())),
        preferred_element_type=jnp.float32,
    )
    ref, at = (parts, nth * 512) if whole else (parts[nth], 0)
    for k in range(4):
        for half in range(blocks):
            place = pl.ds(at + (kind + k) * blocks + half, 64, stride=8)
            ref[place, :] = scores[k * 64 : (k + 1) * 64, half * 128 : (half + 1) * 128]


def score(corpus, rows, s):
    for i in range(4):
        wires_of(corpus, rows, s, i, whole=True)


def order(blocks, s, u, dst):
    loop(4 * blocks, lambda i: sort32(s, i * 32))
    loop(2 * blocks, lambda i: merge64(s, i * 64, u))
    if blocks == 1:
        merge128(u, 0, dst)
    else:
        loop(2, lambda i: merge128(u, i * 128, s))
        merge_top(s, 0, s, 128, dst, 0)


def network(v, pairs):
    for i, j in pairs:
        v[i], v[j] = jnp.maximum(v[i], v[j]), jnp.minimum(v[i], v[j])
    return v


def best16(ref, base):
    a = network([wire(ref, base, i) for i in range(16)], SORT16)
    b = network([wire(ref, base, i) for i in range(16, 32)], SORT16)
    return clean([jnp.maximum(a[i], b[15 - i]) for i in range(16)])


def shorten(src, base, dst, dst_base):
    a = best16(src, base)
    b = best16(src, base + 32)
    peak = jnp.maximum(a[15], b[15])
    high = clean([jnp.maximum(a[i], b[15 - i]) for i in range(16)])
    low = clean([jnp.minimum(a[i], b[15 - i]) for i in range(16)])
    for i in range(16):
        put(dst, dst_base, i, high[i])
        put(dst, dst_base, 16 + i, low[i])
    return peak


def best32(src, base, dst, dst_base):
    v = clean([jnp.maximum(wire(src, base, i), wire(src, base, 63 - i)) for i in range(32)])
    for i in range(32):
        put(dst, dst_base, i, v[i])
    return v[31]


def best64(src, dst, turn=0):
    def other(i):
        return pltpu.roll(wire(src, 0, 63 - i), turn, 0) if turn else wire(src, 0, 127 - i)

    v = []
    for i in range(32):
        a = jnp.maximum(wire(src, 0, i), other(i))
        b = jnp.maximum(wire(src, 0, i + 32), other(i + 32))
        v.append(jnp.maximum(a, b))
        put(dst, 32, i, jnp.minimum(a, b))
    v = clean(v)
    for i in range(32):
        put(dst, 0, i, v[i])
    clean_at(dst, 32)
    return wire(dst, 63, 0)


def merge_turned(src, dst, turn):
    for op, at in ((jnp.maximum, 0), (jnp.minimum, 64)):
        v = []
        for i in range(32):
            a = op(wire(src, 0, i), pltpu.roll(wire(src, 0, 63 - i), turn, 0))
            b = op(wire(src, 0, i + 32), pltpu.roll(wire(src, 0, 31 - i), turn, 0))
            v.append(jnp.maximum(a, b))
            put(dst, at + 32, i, jnp.minimum(a, b))
        v = clean(v)
        for i in range(32):
            put(dst, at, i, v[i])
        clean_at(dst, at + 32)


def leaders(groups, own, far, *work, emit, ahead=2):
    near_parts, far_parts, (s, u, w) = work[:4], work[4:8], work[8:]
    sides = (near_parts, far_parts)
    parts = [(g, side, i) for g in range(len(groups)) for side in range(2) for i in range(4)]

    def scored(k):
        if k < len(parts):
            g, side, i = parts[k]
            wires_of((own, far)[side](), groups[g][1](), sides[side], i)

    for k in range(ahead):
        scored(k)
    peak = None
    for k, (g, side, i) in enumerate(parts):
        scored(k + ahead)
        blocks = groups[g][0]
        if blocks == 2 or i % 2 == 1:
            nth = i if blocks == 2 else i // 2
            now = shorten(sides[side][nth], 0, u, side * 64 * blocks + nth * 32)
            peak = now if peak is None else jnp.maximum(peak, now)
        if side == 0 or i < 3:
            continue
        for j in range(2 * blocks):
            peak = jnp.maximum(peak, best32(u, j * 64, w, j * 32))
        if blocks == 2:
            loop(2, lambda j: merge64(w, j * 64, u))
            peak = jnp.maximum(peak, best64(u, w))
            turns = (4, 2)
        else:
            merge64(w, 0, u)
            peak = jnp.maximum(peak, best64(u, w, turn=4))
            turns = (2, 1)
        merge_turned(w, u, turns[0])
        merge_top(u, 0, u, 0, w, 0, turn=turns[1])
        for turn in (4, 2, 1)[: 4 - blocks]:
            peak = jnp.maximum(peak, pltpu.roll(peak, turn, 0))
        unsure = jnp.max(jnp.where(peak > wire(w, 127, 0), 1.0, 0.0)) > 0.0
        peak = None

        def give(g=g, blocks=blocks):
            for half in range(blocks):
                emit(g, half, w[pl.ds(half, TOPK, stride=8), :].T)

        give()

        @pl.when(unsure)
        def _(g=g, blocks=blocks, give=give):
            long_way(blocks, groups[g][1](), own(), far(), s, u, w)
            give()


def long_way(blocks, rows, own, far, s, u, w):
    score(own, rows, s)
    order(blocks, s, u, w)
    score(far, rows, s)
    if blocks == 2:
        order(blocks, s, u, u)
        merge_top(w, 0, u, 0, s, 0)
        merge_top(s, 0, s, 0, u, 0, turn=4)
        merge_top(u, 0, u, 0, w, 0, turn=2)
    else:
        loop(4, lambda i: sort32(s, i * 32))
        loop(2, lambda i: merge64(s, i * 64, u))
        merge128(u, 0, s)
        merge_top(w, 0, s, 0, u, 0)
        merge_top(u, 0, u, 0, s, 0, turn=4)
        merge_top(s, 0, s, 0, u, 0, turn=2)
        merge_top(u, 0, u, 0, w, 0, turn=1)


def main_rows(chunk):
    return jnp.concatenate(
        [chunk[:, c * MAIN : (c + 1) * MAIN, :].reshape(-1, 128) for c in range(COLS)], axis=1
    )


def tail_rows(chunk):
    langs = chunk.shape[0]
    many, each = langs * TAIL, TAIL * COLS
    shape, total = (COLS, many, langs * each), langs * each
    col, row, at = (lax.broadcasted_iota(jnp.int32, shape, d) for d in range(3))
    from_row = lax.shift_right_logical(row, 2) * each + col * TAIL + (row & 3)
    picks = jnp.where(at == from_row, 1.0, 0.0).astype(jnp.bfloat16).reshape(total, total)
    flat = chunk[:, MAIN * COLS : SENT, :].reshape(total, 128)
    found = jnp.dot(picks, flat, preferred_element_type=jnp.float32).astype(jnp.bfloat16)
    return jnp.concatenate([found[c * many : (c + 1) * many, :] for c in range(COLS)], axis=1)


def first_kernel(chunk, own, far_in, out, far, rows, sem, *work):
    copy = pltpu.make_async_copy(far_in, far, sem)
    copy.start()
    rows[...] = main_rows(chunk)
    waited = []

    def partner():
        if not waited:
            copy.wait()
            waited.append(True)
        return far

    def emit(g, half, value):
        out[half * Q : (half + 1) * Q, :] = value

    leaders([(2, lambda: rows[...])], lambda: own, partner, *work, emit=emit, ahead=0)


def early_kernel(half0, half1, own, far, out, rows, *work):
    rows[0:128, :] = main_rows(half0)
    rows[128:256, :] = main_rows(half1)

    def emit(g, half, value):
        out[half * Q : (half + 1) * Q, :] = value

    leaders([(2, lambda: rows[...])], lambda: own, lambda: far, *work, emit=emit)


STEPS = 800.0
FLOOR = 32.5
LN2 = 0.6931471805599453


def coded(v):
    level = jnp.round(jnp.log(jnp.abs(v)) * (STEPS / LN2) + STEPS * FLOOR)
    level = jnp.clip(level, 0.0, 32767.0)
    return jnp.where(v < 0, -level, level)


def decoded(c):
    level = jnp.abs(c)
    v = jnp.where(level > 0, jnp.exp(level * (LN2 / STEPS) - FLOOR * LN2), 0.0)
    return jnp.where(c < 0, -v, v)


def boxed(box, main, tail):
    box[0:MAIN, :] = main
    box[MAIN:CAP, :] = tail
    box[CAP:ROWS, :] = jnp.zeros((ROWS - CAP, TOPK), jnp.float32)
    return coded(box[...]).astype(jnp.int32).astype(jnp.int16)


def middle_kernel(mine, cx0, cx1, cy0, cy1, own, far, r0, r1, out, rows, lists, box, *work):
    rows[0:128, :] = main_rows(cx1)
    rows[128:256, :] = main_rows(cy1)
    rows[256:320, :] = tail_rows(mine)
    for k, chunk in enumerate((cx0, cx1, cy0, cy1)):
        rows[320 + k * 32 : 352 + k * 32, :] = tail_rows(chunk)
    rows[448:512, :] = jnp.zeros((64, WIDTH), jnp.bfloat16)

    def emit(g, half, value):
        lists[g * 256 + half * Q : g * 256 + (half + 1) * Q, :] = value

    leaders(
        [(2, lambda: rows[0:256, :]), (2, lambda: rows[256:512, :])], lambda: own, lambda: far, *work, emit=emit
    )
    for k in range(3):
        for lang in range(LANGS):
            half, start = lang // 8, lang % 8 * MAIN
            if k == 0:
                main = r0[lang * MAIN : (lang + 1) * MAIN, :]
            else:
                start += (k - 1) * Q
                main = (r1, lists)[half][start : start + MAIN, :]
            start = 256 + k * 64 + lang * TAIL
            out[k, lang] = boxed(box.at[k], main, lists[start : start + TAIL, :])


def late_kernel(at, cd0, cd1, own, far, done, out, rows, last, box, *work):
    rows[0:128, :] = main_rows(cd0)
    rows[128:256, :] = main_rows(cd1)
    rows[256:288, :] = tail_rows(cd0)
    rows[288:320, :] = tail_rows(cd1)
    rows[320:384, :] = jnp.zeros((64, WIDTH), jnp.bfloat16)
    me = at[0]
    for k, owner in enumerate((me, me ^ 2, me ^ 1)):
        for lang in range(LANGS):
            out[lang % 2, owner, lang // 2] = done[k, lang]

    def emit(g, half, value):
        last[g * 256 + half * Q : g * 256 + (half + 1) * Q, :] = value

    leaders(
        [(2, lambda: rows[0:256, :]), (1, lambda: rows[256:384, :])], lambda: own, lambda: far, *work, emit=emit
    )
    for lang in range(LANGS):
        tail = last[256 + lang * TAIL : 256 + (lang + 1) * TAIL, :]
        out[lang % 2, me ^ 3, lang // 2] = boxed(box.at[lang % 4], last[lang * MAIN : (lang + 1) * MAIN, :], tail)


COST = 2 * 256 * 2048 * 768 * 8
VMEM = pl.BlockSpec(memory_space=pltpu.VMEM)
LIMIT = pltpu.CompilerParams(vmem_limit_bytes=14 << 20)
WORK = [pltpu.VMEM((64 * 8, 128), jnp.float32)] * 8 + [
    pltpu.VMEM((256 * 8, 128), jnp.float32),
    pltpu.VMEM((256 * 8, 128), jnp.float32),
    pltpu.VMEM((128 * 8, 128), jnp.float32),
]


def first(chunk, own, far):
    return pl.pallas_call(
        first_kernel,
        out_shape=(
            jax.ShapeDtypeStruct((256, TOPK), jnp.float32),
            jax.ShapeDtypeStruct((1024, WIDTH), jnp.bfloat16),
        ),
        in_specs=[VMEM, VMEM, pl.BlockSpec(memory_space=pl.ANY)],
        out_specs=(VMEM, VMEM),
        scratch_shapes=[pltpu.VMEM((256, WIDTH), jnp.bfloat16), pltpu.SemaphoreType.DMA] + WORK,
        compiler_params=LIMIT,
        cost_estimate=pl.CostEstimate(flops=COST, bytes_accessed=1 << 20, transcendentals=0),
        name="first",
    )(chunk, own, far)


def early(half0, half1, own, far):
    return pl.pallas_call(
        early_kernel,
        out_shape=jax.ShapeDtypeStruct((256, TOPK), jnp.float32),
        in_specs=[VMEM] * 4,
        out_specs=VMEM,
        scratch_shapes=[pltpu.VMEM((256, WIDTH), jnp.bfloat16)] + WORK,
        compiler_params=LIMIT,
        cost_estimate=pl.CostEstimate(flops=COST, bytes_accessed=1 << 20, transcendentals=0),
        name="early",
    )(half0, half1, own, far)


def middle(mine, halves, own, far, results):
    return pl.pallas_call(
        middle_kernel,
        out_shape=jax.ShapeDtypeStruct((3, LANGS, ROWS, TOPK), jnp.int16),
        in_specs=[VMEM] * 9,
        out_specs=VMEM,
        scratch_shapes=[
            pltpu.VMEM((512, WIDTH), jnp.bfloat16),
            pltpu.VMEM((512, TOPK), jnp.float32),
            pltpu.VMEM((3, ROWS, TOPK), jnp.float32),
        ]
        + WORK,
        compiler_params=LIMIT,
        cost_estimate=pl.CostEstimate(flops=COST * 2, bytes_accessed=1 << 20, transcendentals=0),
        name="middle",
    )(mine, *halves, own, far, *results)


def late(at, halves, own, far, done):
    return pl.pallas_call(
        late_kernel,
        out_shape=jax.ShapeDtypeStruct((2, 4, LANGS // 2, ROWS, TOPK), jnp.int16),
        in_specs=[pl.BlockSpec(memory_space=pltpu.SMEM)] + [VMEM] * 5,
        out_specs=VMEM,
        scratch_shapes=[
            pltpu.VMEM((384, WIDTH), jnp.bfloat16),
            pltpu.VMEM((384, TOPK), jnp.float32),
            pltpu.VMEM((4, ROWS, TOPK), jnp.float32),
        ]
        + WORK,
        compiler_params=LIMIT,
        cost_estimate=pl.CostEstimate(flops=COST * 2, bytes_accessed=1 << 20, transcendentals=0),
        name="late",
    )(at, *halves, own, far, done)


def outbox_kernel(queries_in, routes_in, out, slots, queries, routes, sems):
    copies = (
        pltpu.make_async_copy(routes_in, routes, sems.at[0]),
        pltpu.make_async_copy(queries_in, queries, sems.at[1]),
    )
    for copy in copies:
        copy.start()
    copies[0].wait()
    along = jnp.broadcast_to(routes[...].astype(jnp.float32), (Q, Q))
    down = along.T
    before = lax.broadcasted_iota(jnp.int32, (Q, Q), 0) < lax.broadcasted_iota(jnp.int32, (Q, Q), 1)
    earlier = jnp.where(before & (along == down), 1.0, 0.0)
    rank = jnp.sum(earlier, axis=0, keepdims=True).astype(jnp.int32)
    lang = routes[...]
    slots[...] = ((lang & 1) * (LANGS // 2) + lax.shift_right_logical(lang, 1)) * ROWS + rank
    main_at = jnp.where(rank < MAIN, lang * MAIN + rank, -1)
    hits = lax.broadcasted_iota(jnp.int32, (LANGS * MAIN, Q), 0) == jnp.broadcast_to(main_at, (LANGS * MAIN, Q))
    picks = jnp.where(hits, 1.0, 0.0).astype(jnp.bfloat16)
    each = TAIL * COLS
    tail_at = jnp.where(rank < MAIN, -1, lang * TAIL + rank - MAIN)
    shape = (LANGS, each, Q)
    of_lang, row = (lax.broadcasted_iota(jnp.int32, shape, d) for d in range(2))
    hits = of_lang * TAIL + (row & 3) == jnp.broadcast_to(tail_at.reshape(1, 1, Q), shape)
    tail_picks = [
        jnp.where(hits & (lax.shift_right_logical(row, 2) == c), 1.0, 0.0).astype(jnp.bfloat16).reshape(LANGS * each, Q)
        for c in range(COLS)
    ]
    copies[1].wait()
    x = queries[...].astype(jnp.float32)
    unit = (x * lax.rsqrt(jnp.mean(x * x, axis=1, keepdims=True) + epsilon)).astype(jnp.bfloat16)
    box = jnp.dot(picks, unit, preferred_element_type=jnp.float32).astype(jnp.bfloat16)
    for c in range(COLS):
        out[:, c * MAIN : (c + 1) * MAIN, :] = box[:, c * 128 : (c + 1) * 128].reshape(LANGS, MAIN, 128)
    tail = jnp.zeros((LANGS * each, 128), jnp.float32)
    for c in range(COLS):
        tail = tail + jnp.dot(tail_picks[c], unit[:, c * 128 : (c + 1) * 128], preferred_element_type=jnp.float32)
    out[:, MAIN * COLS : SENT, :] = tail.astype(jnp.bfloat16).reshape(LANGS, each, 128)


def outbox_of(queries, routes):
    return pl.pallas_call(
        outbox_kernel,
        out_shape=(
            jax.ShapeDtypeStruct((LANGS, SENT, 128), jnp.bfloat16),
            jax.ShapeDtypeStruct((1, Q), jnp.int32),
        ),
        in_specs=[pl.BlockSpec(memory_space=pltpu.HBM)] * 2,
        out_specs=(VMEM, VMEM),
        scratch_shapes=[
            pltpu.VMEM((Q, WIDTH), jnp.bfloat16),
            pltpu.VMEM((1, Q), jnp.int32),
            pltpu.SemaphoreType.DMA((2,)),
        ],
        compiler_params=pltpu.CompilerParams(vmem_limit_bytes=60 << 20),
        name="outbox",
    )(queries, routes)


def join_kernel(back, slots, out, a, b):
    total = LANGS * ROWS
    hits = lax.broadcasted_iota(jnp.int32, (total, Q), 0) == jnp.broadcast_to(slots[...], (total, Q))
    picks = jnp.where(hits, 1.0, 0.0)
    picks = jnp.concatenate([picks[i * Q : (i + 1) * Q, :].T for i in range(total // Q)], axis=1)
    picks = picks.astype(jnp.bfloat16)
    for k in range(4):
        code = back[:, k].astype(jnp.int32).astype(jnp.float32).reshape(total, TOPK)
        high = code.astype(jnp.bfloat16)
        low = (code - high.astype(jnp.float32)).astype(jnp.bfloat16)
        rows = jnp.dot(picks, high, preferred_element_type=jnp.float32) + jnp.dot(
            picks, low, preferred_element_type=jnp.float32
        )
        ranks = decoded(rows).T
        a[pl.ds(k, TOPK, stride=8), :] = ranks
        a[pl.ds(k + 4, TOPK, stride=8), :] = ranks
    merge_top(a, 0, a, 0, b, 0, turn=2)
    merge_top(b, 0, b, 0, a, 0, turn=1)
    out[...] = a[pl.ds(0, TOPK, stride=8), :].T


def join(back, slots):
    return pl.pallas_call(
        join_kernel,
        out_shape=jax.ShapeDtypeStruct((Q, TOPK), jnp.float32),
        in_specs=[VMEM] * 2,
        out_specs=VMEM,
        scratch_shapes=[pltpu.VMEM((128 * 8, 128), jnp.float32)] * 2,
        compiler_params=LIMIT,
        name="join",
    )(back, slots)


AXES = ("lang", "shard")


def moves(target):
    return [
        (lang * 8 + y * 4 + x, lang * 8 + ty * 4 + tx % 4)
        for lang in range(16)
        for y in range(2)
        for x in range(4)
        for ty, tx in (target(lang % 2, y, x),)
    ]


def pair(core, y, x):
    return y, x + (1 if (x + core) % 2 == 0 else -1)


def over_x(core, y, x):
    return y, x + 2


def over_y(core, y, x):
    return 1 - y, x


TEAMS = [
    [
        (pair * 2 + core) * 8 + y * 4 + odd + 2 * half
        for core in range(2)
        for half in range(2)
        for y in range(2)
        for pair in range(8)
    ]
    for odd in range(2)
]


def shards(queries, routes, corpus):
    far = lax.ppermute(corpus, AXES, moves(pair))
    outbox, slots = outbox_of(queries, routes.reshape(1, Q))
    mine = lax.all_to_all(outbox, "lang", split_axis=0, concat_axis=0, tiled=True)
    cx0, cy0, cx1, cy1 = (
        lax.ppermute(part, AXES, moves(over)) for part in (mine[:8], mine[8:]) for over in (over_x, over_y)
    )
    r0, far = first(mine, corpus, far)
    cx0, cy0, r0 = lax.optimization_barrier((cx0, cy0, r0))
    cd0 = lax.ppermute(cx0, AXES, moves(over_y))
    r1 = early(cx0, cy0, corpus, far)
    cx1, cy1, r1 = lax.optimization_barrier((cx1, cy1, r1))
    cd1 = lax.ppermute(cy1, AXES, moves(over_x))
    done = middle(mine, (cx0, cx1, cy0, cy1), corpus, far, (r0, r1))
    shard = lax.axis_index("shard")
    at = (lax.shift_right_logical(shard, 2) + (shard & 2)).reshape(1)
    found = late(at, (cd0, cd1), corpus, far, done)
    back = lax.all_to_all(
        found.reshape(LANGS * 4, ROWS, TOPK), AXES, 0, 0, axis_index_groups=TEAMS, tiled=True
    )
    return join(back.reshape(2, 4, LANGS // 2, ROWS, TOPK), slots)


def solution(mesh):
    placed = (P(AXES, None), P(AXES, None), P(AXES, None))
    return jax.shard_map(shards, mesh=mesh, in_specs=placed, out_specs=P(AXES, None), check_vma=False)
```
